8 devices in a mesh: dp: 1 (over z), col: 2 (over y), row: 4 (over x, core).
Axes of the slice: x: 2, y: 2, z: 1, core: 2. Of those that a mesh axis runs over, the one named last changes fastest.
Arguments:
- hidden: bfloat16 [16, 1024, 2048], P(('dp', 'row'), None, 'col')
- ln1_gain: float32 [2048], P('col')
- ln1_bias: float32 [2048], P('col')
- w_qkv: bfloat16 [2048, 3, 24, 128], P('row', None, 'col')
- b_qkv: bfloat16 [3, 24, 128], P(None, 'col')
- w_out: bfloat16 [24, 128, 2048], P('row', None, 'col')
- b_out: bfloat16 [2048], P('col')
- ln2_gain: float32 [2048], P('col')
- ln2_bias: float32 [2048], P('col')
- w_up: bfloat16 [2048, 8192], P('row', 'col')
- b_up: bfloat16 [8192], P('col')
- w_down: bfloat16 [8192, 2048], P('row', 'col')
- b_down: bfloat16 [2048], P('col')
Outputs:
- output: bfloat16 [16, 1024, 2048], P(('dp', 'row'), None, 'col')
All inputs are finite; a program needn't handle non-finite values.
Results may differ from the reference program's by a relative error of at most 0.0090525.
Values are sent between devices in bfloat16 or wider.
A program may use at most 1 GiB of HBM per device.

```python
import jax
import jax.numpy as jnp
from jax import lax

D_MODEL = 2048
N_HEADS = 24
HEAD_DIM = 128
FF_DIM = 8192
N_SEQS = 16
SEQ_LEN = 1024
LN_EPS = 1e-5


def setup_inputs(seed: int = 0, part: int = 0) -> dict:
    root_key = jax.random.key(seed)
    shared = jax.random.split(root_key, 12)
    part_keys = jax.random.split(jax.random.fold_in(root_key, part), 2)
    width_attn = N_HEADS * HEAD_DIM

    def draw_normal(key_index, shape, scale):
        return scale * jax.random.normal(shared[key_index], shape, jnp.float32)

    tok_mean = jax.random.normal(part_keys[0], (N_SEQS, SEQ_LEN, 1), jnp.float32)
    hidden = tok_mean + jax.random.normal(part_keys[1], (N_SEQS, SEQ_LEN, D_MODEL), jnp.float32)
    return {
        'hidden': hidden.astype(jnp.bfloat16),
        'ln1_gain': 1.0 + draw_normal(0, (D_MODEL,), 0.3),
        'ln1_bias': draw_normal(1, (D_MODEL,), 0.3),
        'w_qkv': draw_normal(2, (D_MODEL, 3, N_HEADS, HEAD_DIM), 1.5 * D_MODEL ** -0.5).astype(jnp.bfloat16),
        'b_qkv': draw_normal(3, (3, N_HEADS, HEAD_DIM), 0.3).astype(jnp.bfloat16),
        'w_out': draw_normal(4, (N_HEADS, HEAD_DIM, D_MODEL), width_attn ** -0.5).astype(jnp.bfloat16),
        'b_out': draw_normal(5, (D_MODEL,), 0.3).astype(jnp.bfloat16),
        'ln2_gain': 1.0 + draw_normal(6, (D_MODEL,), 0.3),
        'ln2_bias': draw_normal(7, (D_MODEL,), 0.3),
        'w_up': draw_normal(8, (D_MODEL, FF_DIM), D_MODEL ** -0.5).astype(jnp.bfloat16),
        'b_up': draw_normal(9, (FF_DIM,), 0.5).astype(jnp.bfloat16),
        'w_down': draw_normal(10, (FF_DIM, D_MODEL), FF_DIM ** -0.5).astype(jnp.bfloat16),
        'b_down': draw_normal(11, (D_MODEL,), 0.3).astype(jnp.bfloat16),
    }


def layer_norm(values, ln_gain, ln_shift):
    values = values.astype(jnp.float32)
    row_mean = jnp.mean(values, axis=-1, keepdims=True)
    centered = values - row_mean
    row_var = jnp.mean(centered * centered, axis=-1, keepdims=True)
    return (centered * lax.rsqrt(row_var + LN_EPS) * ln_gain + ln_shift).astype(jnp.bfloat16)


def attend_one(seq_qkv):
    queries = seq_qkv[:, 0].astype(jnp.float32)
    key_vals = seq_qkv[:, 1].astype(jnp.float32)
    val_vals = seq_qkv[:, 2].astype(jnp.float32)
    scores = jnp.einsum('qhe,khe->hqk', queries, key_vals) * HEAD_DIM ** -0.5
    positions = jnp.arange(SEQ_LEN)
    causal = positions[:, None] >= positions[None, :]
    scores = jnp.where(causal, scores, -1e30)
    attn_probs = jax.nn.softmax(scores, axis=-1).astype(jnp.bfloat16).astype(jnp.float32)
    return jnp.einsum('hqk,khe->qhe', attn_probs, val_vals).astype(jnp.bfloat16)


def reference(hidden, ln1_gain, ln1_bias, w_qkv, b_qkv, w_out, b_out, ln2_gain, ln2_bias, w_up, b_up, w_down, b_down):
    width_attn = N_HEADS * HEAD_DIM
    flat_rows = hidden.reshape(N_SEQS * SEQ_LEN, D_MODEL)
    normed = layer_norm(flat_rows, ln1_gain, ln1_bias)
    qkv_proj = jnp.dot(normed, w_qkv.reshape(D_MODEL, 3 * width_attn), preferred_element_type=jnp.float32)
    qkv_proj = (qkv_proj + b_qkv.reshape(3 * width_attn).astype(jnp.float32)).astype(jnp.bfloat16)
    seq_qkv = qkv_proj.reshape(N_SEQS, SEQ_LEN, 3, N_HEADS, HEAD_DIM)
    attn_out = lax.map(attend_one, seq_qkv).reshape(N_SEQS * SEQ_LEN, width_attn)
    out_proj = jnp.dot(attn_out, w_out.reshape(width_attn, D_MODEL), preferred_element_type=jnp.float32)
    resid = (flat_rows.astype(jnp.float32) + out_proj + b_out.astype(jnp.float32)).astype(jnp.bfloat16)
    normed_two = layer_norm(resid, ln2_gain, ln2_bias)
    pre_act = jnp.dot(normed_two, w_up, preferred_element_type=jnp.float32) + b_up.astype(jnp.float32)
    act_bf = jax.nn.gelu(pre_act, approximate=True).astype(jnp.bfloat16)
    down_proj = jnp.dot(act_bf, w_down, preferred_element_type=jnp.float32)
    layer_out = (resid.astype(jnp.float32) + down_proj + b_down.astype(jnp.float32)).astype(jnp.bfloat16)
    return layer_out.reshape(N_SEQS, SEQ_LEN, D_MODEL)
```

```python
import functools

import jax
import jax.numpy as jnp
from jax import lax
from jax.experimental import pallas as pl
from jax.experimental.pallas import tpu as pltpu
from jax.sharding import PartitionSpec as P

LN_EPS = 1e-5
BF = jnp.bfloat16
F32 = jnp.float32
LOG2E = 1.4426950408889634


def attn_kernel(block, q_ref, k_ref, v_ref, o_ref):
    seq, size = q_ref.shape
    scale = size ** -0.5 * LOG2E
    tri = lax.broadcasted_iota(jnp.int32, (block, block), 0) >= lax.broadcasted_iota(jnp.int32, (block, block), 1)
    for i in range(seq // block):
        q = q_ref[i * block:(i + 1) * block, :]
        dn = (((1,), (1,)), ((), ()))
        diag = lax.dot_general(q, k_ref[i * block:(i + 1) * block, :], dn, preferred_element_type=F32)
        diag = jnp.where(tri, diag, -1e30)
        top = jnp.max(diag, axis=1, keepdims=True)
        if i:
            past = lax.dot_general(q, k_ref[:i * block, :], dn, preferred_element_type=F32)
            top = jnp.maximum(top, jnp.max(past, axis=1, keepdims=True))
        e_diag = jnp.exp2((diag - top) * scale)
        total = jnp.sum(e_diag, axis=1, keepdims=True)
        if i:
            e_past = jnp.exp2((past - top) * scale)
            total = total + jnp.sum(e_past, axis=1, keepdims=True)
        inv = 1.0 / total
        out = jnp.dot((e_diag * inv).astype(BF), v_ref[i * block:(i + 1) * block, :], preferred_element_type=F32)
        if i:
            out = out + jnp.dot((e_past * inv).astype(BF), v_ref[:i * block, :], preferred_element_type=F32)
        o_ref[i * block:(i + 1) * block, :] = out.astype(BF)


def attention(qkv, seqs, heads, size):
    tokens = qkv.shape[0]
    seq = tokens // seqs
    spec = lambda part: pl.BlockSpec((seq, size), lambda s, h, part=part: (s, part * heads + h))
    return pl.pallas_call(
        functools.partial(attn_kernel, 256),
        grid=(seqs, heads),
        in_specs=[spec(0), spec(1), spec(2)],
        out_specs=pl.BlockSpec((seq, size), lambda s, h: (s, h)),
        out_shape=jax.ShapeDtypeStruct((tokens, heads * size), BF),
        cost_estimate=pl.CostEstimate(flops=2 * 2 * tokens * seq * size * heads, bytes_accessed=8 * tokens * heads * size, transcendentals=tokens * seq * heads),
    )(qkv, qkv, qkv)


def layer_norm(values, gain, shift):
    values = values.astype(F32)
    mean = jnp.mean(values, axis=-1, keepdims=True)
    centered = values - mean
    var = jnp.mean(centered * centered, axis=-1, keepdims=True)
    return (centered * lax.rsqrt(var + LN_EPS) * gain + shift).astype(BF)


def solution(mesh):
    act_spec = P(('dp', 'row'), None, 'col')
    arg_specs = (act_spec, P('col'), P('col'), P('row', None, 'col', None), P(None, 'col', None), P('row', None, 'col'), P('col'), P('col'), P('col'), P('row', 'col'), P('col'), P('row', 'col'), P('col'))
    swap = [(0, 1), (1, 0)]

    def local_layer(hidden, ln1_gain, ln1_bias, w_qkv, b_qkv, w_out, b_out, ln2_gain, ln2_bias, w_up, b_up, w_down, b_down):
        col = lax.axis_index('col')
        seqs, seq_len, half = hidden.shape
        mine = seqs // 2
        tokens = mine * seq_len
        heads, size = w_qkv.shape[2], w_qkv.shape[3]

        def both(own, got, axis):
            return jnp.where(col == 0, jnp.concatenate([own, got], axis), jnp.concatenate([got, own], axis))

        def part(a, which):
            return lax.dynamic_slice_in_dim(a, which * mine, mine, 0)

        got = lax.ppermute(part(hidden, 1 - col), 'col', swap)
        x = both(part(hidden, col), got, 2).reshape(tokens, 2 * half)
        small = [ln1_gain, ln1_bias, ln2_gain, ln2_bias, b_out, b_down, b_qkv.reshape(-1), b_up]
        packed = jnp.concatenate([a.astype(F32) for a in small])[None]
        packed = both(packed, lax.ppermute(packed, 'col', swap), 0)
        params, at = [], 0
        for a in small:
            params.append(packed[:, at:at + a.size])
            at += a.size
        g1, s1, g2, s2, bo, bd, bq, bu = params

        def gather(w):
            full = lax.all_gather(w, ('col', 'row'), axis=0, tiled=False)
            return full.reshape(2, 4 * w.shape[0], w.shape[1])

        wq = gather(w_qkv.reshape(w_qkv.shape[0], -1))
        wo = gather(w_out.reshape(-1, half))
        wu = gather(w_up)
        wd = gather(w_down)

        u = layer_norm(x, g1.reshape(-1), s1.reshape(-1))
        outs = []
        for c in range(2):
            qkv = (jnp.dot(u, wq[c], preferred_element_type=F32) + bq[c]).astype(BF)
            outs.append(attention(qkv, mine, heads, size))
        o = jnp.concatenate(outs, axis=1)
        proj = jnp.concatenate([jnp.dot(o, wo[c], preferred_element_type=F32) for c in range(2)], axis=1)
        h = (x.astype(F32) + proj + bo.reshape(-1)).astype(BF)
        n2 = layer_norm(h, g2.reshape(-1), s2.reshape(-1))
        acts = [jax.nn.gelu(jnp.dot(n2, wu[c], preferred_element_type=F32) + bu[c], approximate=True).astype(BF) for c in range(2)]
        act = jnp.concatenate(acts, axis=1)
        ys = [(h[:, c * half:(c + 1) * half].astype(F32) + jnp.dot(act, wd[c], preferred_element_type=F32) + bd[c]).astype(BF).reshape(mine, seq_len, half) for c in range(2)]
        keep = jnp.where(col == 0, ys[0], ys[1])
        give = jnp.where(col == 0, ys[1], ys[0])
        return both(keep, lax.ppermute(give, 'col', swap), 0)

    return jax.shard_map(local_layer, mesh=mesh, in_specs=arg_specs, out_specs=act_spec, check_vma=False)
```

```python
import functools

import jax
import jax.numpy as jnp
from jax import lax
from jax.experimental import pallas as pl
from jax.experimental.pallas import tpu as pltpu
from jax.sharding import PartitionSpec as P

LN_EPS = 1e-5
BF = jnp.bfloat16
F32 = jnp.float32
LOG2E = 1.4426950408889634
MESH = pl.DeviceIdType.MESH
ANY = pl.BlockSpec(memory_space=pl.ANY)
VMEM_LIMIT = 63 * 1024 * 1024


class Grid:
    def __init__(self):
        self.c = lax.axis_index('col')
        self.r = lax.axis_index('row')
        self.oc = 1 - self.c
        x = self.r // 2
        k = self.r - 2 * x
        self.rp = 2 * x + 1 - k
        self.rx = 2 * (1 - x) + k
        self.rxp = 2 * (1 - x) + 1 - k
        self.P, self.X, self.Y = {'row': self.rp}, {'row': self.rx}, {'col': self.oc}

    def barrier(self):
        sem = pltpu.get_barrier_semaphore()
        for dev in (self.P, self.X, self.Y):
            pl.semaphore_signal(sem, inc=1, device_id=dev, device_id_type=MESH)
        pl.semaphore_wait(sem, 3)


def remote(src, dst, send, recv, dev):
    return pltpu.make_async_remote_copy(src_ref=src, dst_ref=dst, send_sem=send, recv_sem=recv, device_id=dev, device_id_type=MESH)


class Gather:
    def __init__(self, g, own, land, send, recv, via_x):
        self.g, self.own, self.land, self.send_sem, self.recv_sem, self.via_x = g, own, land, send, recv, via_x

    def desc(self, kind, j, via_x=None):
        g = self.g
        via_x = self.via_x if via_x is None else via_x
        if kind < 3:
            src, dst = self.own(j), self.land(g.c, g.r, j)
            dev = (g.X, g.Y, g.P)[kind]
        else:
            at = {3: (g.c, g.rx), 4: (g.oc, g.r), 5: (g.oc, g.rx), 6: (g.oc, g.r) if via_x else (g.c, g.rx)}[kind]
            src = dst = self.land(*at, j)
            dev = g.P if kind < 6 else (g.X if via_x else g.Y)
        return remote(src, dst, self.send_sem.at[kind, j], self.recv_sem.at[kind, j], dev)

    def start(self, kind, j, via_x=None):
        self.desc(kind, j, via_x).start()

    def arrive(self, kind, j):
        g = self.g
        at = [(g.c, g.rx), (g.oc, g.r), (g.c, g.rp), (g.c, g.rxp), (g.oc, g.rp), (g.oc, g.rxp), (g.oc, g.rx)][kind]
        ref = self.land(*at, j)
        remote(ref, ref, self.send_sem.at[kind, j], self.recv_sem.at[kind, j], g.P).wait_recv()

    def sent(self, kind, j):
        self.desc(kind, j).wait_send()


def chunked(total, body):
    lax.fori_loop(0, total, lambda j, carry: (body(j), carry)[1], 0)


def matmul_rows(a_ref, w_ref, tile, emit):
    depth = w_ref.shape[0] * w_ref.shape[1]

    def body(m):
        rows = pl.ds(pl.multiple_of(m * tile, tile), tile)
        w = w_ref[...].reshape(depth, w_ref.shape[2])
        emit(rows, jnp.dot(a_ref[rows, :], w, preferred_element_type=F32))

    chunked(a_ref.shape[0] // tile, body)


def norm_rows(parts, gains, shifts):
    parts = [p.astype(F32) for p in parts]
    width = sum(p.shape[1] for p in parts)
    mean = sum(jnp.sum(p, axis=1, keepdims=True) for p in parts) / width
    parts = [p - mean for p in parts]
    var = sum(jnp.sum(p * p, axis=1, keepdims=True) for p in parts) / width
    inv = lax.rsqrt(var + LN_EPS)
    return [(p * inv * gn + sh).astype(BF) for p, gn, sh in zip(parts, gains, shifts)]


def qkv_kernel(offs, hid, pk, wq, xland, wland, qkv, pk2, u, xbuf, wbuf, obuf, pkv, gs, gr, hs, hr, ps, pr, ls, ws, os):
    g = Grid()
    g.barrier()
    seqs, seq, half = hid.shape
    piece = 512
    per = seq // piece
    pieces = (seqs // 2) * per
    units = 4
    chunk = units * 128
    n = wq.shape[0] // units

    def own(j):
        return wq.at[pl.ds(j * units, units)]

    def land(cc, rr, j):
        return wland.at[cc, rr, pl.ds(j * units, units)]

    gat = Gather(g, own, land, gs, gr, True)

    def small():
        return remote(pk, pkv, ps, pr, g.Y)

    def hidden(p):
        s, q = p // per, p % per
        return remote(hid.at[g.oc * (seqs // 2) + s, pl.ds(q * piece, piece)], xland.at[s, pl.ds(q * piece, piece)], hs.at[p], hr.at[p], g.Y)

    small().start()
    for p in range(pieces):
        hidden(p).start()

    @functools.partial(chunked, n)
    def _(j):
        gat.start(0, j)
        gat.start(2, j)

    @functools.partial(chunked, n)
    def _(j):
        gat.start(1, j)

    small().wait_recv()
    pk2[g.c] = pk[...]
    pk2[g.oc] = pkv[...]

    def vec(name, cc, size, start=0):
        return pk2[cc, :, pl.ds(offs[name] + start, size)]

    def mine(p):
        s, q = p // per, p % per
        return pltpu.make_async_copy(hid.at[g.c * (seqs // 2) + s, pl.ds(q * piece, piece)], xbuf.at[p % 2, 0], ls.at[p % 2, 0])

    def theirs(p):
        s, q = p // per, p % per
        return pltpu.make_async_copy(xland.at[s, pl.ds(q * piece, piece)], xbuf.at[p % 2, 1], ls.at[p % 2, 1])

    gains = [vec('g1', cc, half) for cc in (g.c, g.oc)]
    shifts = [vec('s1', cc, half) for cc in (g.c, g.oc)]
    for p in range(pieces):
        mine(p).start()
        hidden(p).wait_recv()
        theirs(p).start()
        mine(p).wait()
        theirs(p).wait()
        sub = 64

        @functools.partial(chunked, piece // sub)
        def _(i):
            rows = pl.ds(pl.multiple_of(i * sub, sub), sub)
            res = norm_rows([xbuf[p % 2, 0, rows, :], xbuf[p % 2, 1, rows, :]], gains, shifts)
            to = pl.ds(pl.multiple_of(p * piece + i * sub, sub), sub)
            for cc, val in zip((g.c, g.oc), res):
                u[to, pl.ds(pl.multiple_of(cc * half, half), half)] = val

    def load_own(j, go):
        for i in range(units):
            for idx, rr in enumerate((g.r, g.rp, g.rx, g.rxp)):
                src = wq.at[j * units + i] if idx == 0 else wland.at[g.c, rr, j * units + i]
                go(pltpu.make_async_copy(src, wbuf.at[0, rr, :, pl.ds(i * 128, 128)], ws.at[0, i, idx]))

    def load_other(j, go):
        for i in range(units):
            go(pltpu.make_async_copy(wland.at[g.oc, :, j * units + i], wbuf.at[1, :, :, pl.ds(i * 128, 128)], ws.at[1, i, 0]))

    def out(slot, cc, j):
        return pltpu.make_async_copy(obuf.at[slot], qkv.at[:, pl.ds(pl.multiple_of(cc * (n * chunk) + j * chunk, chunk), chunk)], os.at[slot])

    def compute(slot, cc, j):
        @pl.when(j > 0)
        def _():
            out(slot, cc, j - 1).wait()

        bias = vec('bq', cc, chunk, pl.multiple_of(j * chunk, chunk))

        def emit(rows, val):
            obuf[slot, rows, :] = (val + bias).astype(BF)

        matmul_rows(u, wbuf.at[slot], 512, emit)
        out(slot, cc, j).start()

    begin, finish = (lambda d: d.start()), (lambda d: d.wait())

    @functools.partial(chunked, n + 3)
    def _(t):
        @pl.when(t < n)
        def _():
            gat.arrive(0, t)
            gat.start(3, t)
            gat.arrive(1, t)
            gat.start(4, t)
            gat.start(6, t)

        @pl.when((t >= 1) & (t <= n))
        def _():
            gat.arrive(6, t - 1)
            gat.start(5, t - 1)

        @pl.when(t < n)
        def _():
            gat.arrive(2, t)
            gat.arrive(3, t)
            load_own(t, begin)

        @pl.when(t >= 3)
        def _():
            load_other(t - 3, finish)
            compute(1, g.oc, t - 3)

        @pl.when((t >= 2) & (t < n + 2))
        def _():
            gat.arrive(4, t - 2)
            gat.arrive(5, t - 2)
            load_other(t - 2, begin)

        @pl.when(t < n)
        def _():
            load_own(t, finish)
            compute(0, g.c, t)

    out(0, g.c, n - 1).wait()
    out(1, g.oc, n - 1).wait()
    small().wait_send()
    for p in range(pieces):
        hidden(p).wait_send()

    @functools.partial(chunked, n)
    def _(j):
        for kind in range(7):
            gat.sent(kind, j)


def qkv_call(hidden, packed, wq, offs):
    seqs, seq, half = hidden.shape
    tokens = seqs // 2 * seq
    n = wq.shape[0] // 4
    dma = pltpu.SemaphoreType.DMA
    return pl.pallas_call(
        functools.partial(qkv_kernel, offs),
        in_specs=[ANY, pl.BlockSpec(memory_space=pltpu.VMEM), ANY],
        out_specs=[ANY, ANY, ANY, pl.BlockSpec(memory_space=pltpu.VMEM)],
        out_shape=[
            jax.ShapeDtypeStruct((seqs // 2, seq, half), BF),
            jax.ShapeDtypeStruct((2, 4) + wq.shape, BF),
            jax.ShapeDtypeStruct((tokens, 2 * wq.shape[0] * 128), BF),
            jax.ShapeDtypeStruct((2,) + packed.shape, F32),
        ],
        scratch_shapes=[
            pltpu.VMEM((tokens, 2 * half), BF),
            pltpu.VMEM((2, 2, 512, half), BF),
            pltpu.VMEM((2, 4, wq.shape[1], 512), BF),
            pltpu.VMEM((2, tokens, 512), BF),
            pltpu.VMEM(packed.shape, F32),
            dma((7, n)), dma((7, n)), dma((4,)), dma((4,)), dma, dma, dma((2, 2)), dma((2, 4, 4)), dma((2,)),
        ],
        compiler_params=pltpu.CompilerParams(collective_id=1, has_side_effects=True, vmem_limit_bytes=VMEM_LIMIT),
        name='qkv',
    )(hidden, packed, wq)


def attn_kernel(block, q_ref, k_ref, v_ref, o_ref):
    seq, size = q_ref.shape
    scale = size ** -0.5 * LOG2E
    tri = lax.broadcasted_iota(jnp.int32, (block, block), 0) >= lax.broadcasted_iota(jnp.int32, (block, block), 1)
    for i in range(seq // block):
        q = q_ref[i * block:(i + 1) * block, :]
        dn = (((1,), (1,)), ((), ()))
        diag = lax.dot_general(q, k_ref[i * block:(i + 1) * block, :], dn, preferred_element_type=F32)
        diag = jnp.where(tri, diag, -1e30)
        top = jnp.max(diag, axis=1, keepdims=True)
        if i:
            past = lax.dot_general(q, k_ref[:i * block, :], dn, preferred_element_type=F32)
            top = jnp.maximum(top, jnp.max(past, axis=1, keepdims=True))
        e_diag = jnp.exp2((diag - top) * scale)
        total = jnp.sum(e_diag, axis=1, keepdims=True)
        if i:
            e_past = jnp.exp2((past - top) * scale)
            total = total + jnp.sum(e_past, axis=1, keepdims=True)
        inv = 1.0 / total
        out = jnp.dot((e_diag * inv).astype(BF), v_ref[i * block:(i + 1) * block, :], preferred_element_type=F32)
        if i:
            out = out + jnp.dot((e_past * inv).astype(BF), v_ref[:i * block, :], preferred_element_type=F32)
        o_ref[i * block:(i + 1) * block, :] = out.astype(BF)


def attention(qkv, seqs, heads, size):
    tokens = qkv.shape[0]
    seq = tokens // seqs
    spec = lambda part: pl.BlockSpec((seq, size), lambda s, h: (s, (h // heads) * 3 * heads + part * heads + h % heads))
    return pl.pallas_call(
        functools.partial(attn_kernel, 256),
        grid=(seqs, 2 * heads),
        in_specs=[spec(0), spec(1), spec(2)],
        out_specs=pl.BlockSpec((seq, size), lambda s, h: (s, h)),
        out_shape=jax.ShapeDtypeStruct((tokens, 2 * heads * size), BF),
        cost_estimate=pl.CostEstimate(flops=8 * tokens * seq * size * heads, bytes_accessed=16 * tokens * heads * size, transcendentals=2 * tokens * seq * heads),
        name='attn',
    )(qkv, qkv, qkv)


def layer_norm(values, gain, shift):
    values = values.astype(F32)
    mean = jnp.mean(values, axis=-1, keepdims=True)
    centered = values - mean
    var = jnp.mean(centered * centered, axis=-1, keepdims=True)
    return (centered * lax.rsqrt(var + LN_EPS) * gain + shift).astype(BF)


def solution(mesh):
    act_spec = P(('dp', 'row'), None, 'col')
    arg_specs = (act_spec, P('col'), P('col'), P('row', None, 'col', None), P(None, 'col', None), P('row', None, 'col'), P('col'), P('col'), P('col'), P('row', 'col'), P('col'), P('row', 'col'), P('col'))
    swap = [(0, 1), (1, 0)]

    def local_layer(hidden, ln1_gain, ln1_bias, w_qkv, b_qkv, w_out, b_out, ln2_gain, ln2_bias, w_up, b_up, w_down, b_down):
        col = lax.axis_index('col')
        seqs, seq_len, half = hidden.shape
        mine = seqs // 2
        tokens = mine * seq_len
        heads, size = w_qkv.shape[2], w_qkv.shape[3]

        def both(own, got, axis):
            return jnp.where(col == 0, jnp.concatenate([own, got], axis), jnp.concatenate([got, own], axis))

        small = {'g1': ln1_gain, 's1': ln1_bias, 'g2': ln2_gain, 's2': ln2_bias, 'bo': b_out, 'bd': b_down, 'bq': b_qkv, 'bu': b_up}
        offs, at = {}, 0
        for name, a in small.items():
            offs[name], at = at, at + a.size
        packed = jnp.concatenate([a.reshape(-1).astype(F32) for a in small.values()])[None]
        wq = jnp.transpose(w_qkv, (1, 2, 0, 3)).reshape(3 * heads, w_qkv.shape[0], size)
        got, _, qkv, pk2 = qkv_call(hidden, packed, wq, offs)
        pk2 = pk2[:, 0]
        g2, s2, bo, bd, bu = (pk2[:, offs[k]:offs[k] + small[k].size] for k in ('g2', 's2', 'bo', 'bd', 'bu'))

        x = both(lax.dynamic_slice_in_dim(hidden, col * mine, mine, 0), got, 2).reshape(tokens, 2 * half)

        def gather(w):
            full = lax.all_gather(w, ('col', 'row'), axis=0, tiled=False)
            return full.reshape(2, 4 * w.shape[0], w.shape[1])

        wo = gather(w_out.reshape(-1, half))
        wu = gather(w_up)
        wd = gather(w_down)

        o = attention(qkv, mine, heads, size)
        proj = jnp.concatenate([jnp.dot(o, wo[c], preferred_element_type=F32) for c in range(2)], axis=1)
        h = (x.astype(F32) + proj + bo.reshape(-1)).astype(BF)
        n2 = layer_norm(h, g2.reshape(-1), s2.reshape(-1))
        acts = [jax.nn.gelu(jnp.dot(n2, wu[c], preferred_element_type=F32) + bu[c], approximate=True).astype(BF) for c in range(2)]
        act = jnp.concatenate(acts, axis=1)
        ys = [(h[:, c * half:(c + 1) * half].astype(F32) + jnp.dot(act, wd[c], preferred_element_type=F32) + bd[c]).astype(BF).reshape(mine, seq_len, half) for c in range(2)]
        keep = jnp.where(col == 0, ys[0], ys[1])
        give = jnp.where(col == 0, ys[1], ys[0])
        return both(keep, lax.ppermute(give, 'col', swap), 0)

    return jax.shard_map(local_layer, mesh=mesh, in_specs=arg_specs, out_specs=act_spec, check_vma=False)
```

```python
import functools

import jax
import jax.numpy as jnp
from jax import lax
from jax.experimental import pallas as pl
from jax.experimental.pallas import tpu as pltpu
from jax.sharding import PartitionSpec as P

LN_EPS = 1e-5
BF = jnp.bfloat16
F32 = jnp.float32
LOG2E = 1.4426950408889634
MESH = pl.DeviceIdType.MESH
ANY = pl.BlockSpec(memory_space=pl.ANY)
VMEM_LIMIT = 63 * 1024 * 1024


class Grid:
    def __init__(self):
        self.c = lax.axis_index('col')
        self.r = lax.axis_index('row')
        self.oc = 1 - self.c
        x = self.r // 2
        k = self.r - 2 * x
        self.rp = 2 * x + 1 - k
        self.rx = 2 * (1 - x) + k
        self.rxp = 2 * (1 - x) + 1 - k
        self.P, self.X, self.Y = {'row': self.rp}, {'row': self.rx}, {'col': self.oc}

    def barrier(self):
        sem = pltpu.get_barrier_semaphore()
        for dev in (self.P, self.X, self.Y):
            pl.semaphore_signal(sem, inc=1, device_id=dev, device_id_type=MESH)
        pl.semaphore_wait(sem, 3)


def remote(src, dst, send, recv, dev):
    return pltpu.make_async_remote_copy(src_ref=src, dst_ref=dst, send_sem=send, recv_sem=recv, device_id=dev, device_id_type=MESH)


class Gather:
    def __init__(self, g, own, land, send, recv, via_x):
        self.g, self.own, self.land, self.send_sem, self.recv_sem, self.via_x = g, own, land, send, recv, via_x

    def desc(self, kind, j, via_x=True):
        g = self.g
        if kind < 3:
            src, dst = self.own(j), self.land(g.c, g.r, j)
            dev = (g.X, g.Y, g.P)[kind]
        else:
            at = {3: (g.c, g.rx), 4: (g.oc, g.r), 5: (g.oc, g.rx), 6: (g.oc, g.r) if via_x else (g.c, g.rx)}[kind]
            src = dst = self.land(*at, j)
            dev = g.P if kind < 6 else (g.X if via_x else g.Y)
        return remote(src, dst, self.send_sem.at[kind, j], self.recv_sem.at[kind, j], dev)

    def routed(self, j, act):
        via = self.via_x(j)
        if via is True:
            act(self.desc(6, j))
            return

        @pl.when(via)
        def _():
            act(self.desc(6, j))

        @pl.when(jnp.logical_not(via))
        def _():
            act(self.desc(6, j, False))

    def start(self, kind, j):
        if kind == 6:
            self.routed(j, lambda d: d.start())
        else:
            self.desc(kind, j).start()

    def arrive(self, kind, j):
        g = self.g
        at = [(g.c, g.rx), (g.oc, g.r), (g.c, g.rp), (g.c, g.rxp), (g.oc, g.rp), (g.oc, g.rxp), (g.oc, g.rx)][kind]
        ref = self.land(*at, j)
        remote(ref, ref, self.send_sem.at[kind, j], self.recv_sem.at[kind, j], g.P).wait_recv()

    def drain(self, n):
        @functools.partial(chunked, n)
        def _(j):
            for kind in range(6):
                self.desc(kind, j).wait_send()
            self.routed(j, lambda d: d.wait_send())


def chunked(total, body):
    lax.fori_loop(0, total, lambda j, carry: (body(j), carry)[1], 0)


def matmul_rows(a_ref, w_ref, tile, emit):
    depth = w_ref.shape[0] * w_ref.shape[1]

    def body(m):
        rows = pl.ds(pl.multiple_of(m * tile, tile), tile)
        w = w_ref[...].reshape(depth, w_ref.shape[2])
        emit(rows, jnp.dot(a_ref[rows, :], w, preferred_element_type=F32))

    chunked(a_ref.shape[0] // tile, body)


def norm_rows(parts, gains, shifts):
    parts = [p.astype(F32) for p in parts]
    width = sum(p.shape[1] for p in parts)
    mean = sum(jnp.sum(p, axis=1, keepdims=True) for p in parts) / width
    parts = [p - mean for p in parts]
    var = sum(jnp.sum(p * p, axis=1, keepdims=True) for p in parts) / width
    inv = lax.rsqrt(var + LN_EPS)
    return [(p * inv * gn + sh).astype(BF) for p, gn, sh in zip(parts, gains, shifts)]


BEGIN, FINISH = (lambda d: d.start()), (lambda d: d.wait())


def consume(gat, n, load_own, load_other, compute):
    g = gat.g

    @functools.partial(chunked, n + 3)
    def _(t):
        @pl.when(t < n)
        def _():
            gat.arrive(0, t)
            gat.start(3, t)
            gat.arrive(1, t)
            gat.start(4, t)
            gat.start(6, t)

        @pl.when((t >= 1) & (t <= n))
        def _():
            gat.arrive(6, t - 1)
            gat.start(5, t - 1)

        @pl.when(t < n)
        def _():
            gat.arrive(2, t)
            gat.arrive(3, t)
            load_own(t, BEGIN)

        @pl.when(t >= 3)
        def _():
            load_other(t - 3, FINISH)
            compute(1, g.oc, t - 3)

        @pl.when((t >= 2) & (t < n + 2))
        def _():
            gat.arrive(4, t - 2)
            gat.arrive(5, t - 2)
            load_other(t - 2, BEGIN)

        @pl.when(t < n)
        def _():
            load_own(t, FINISH)
            compute(0, g.c, t)


def qkv_kernel(offs, hid, pk, wq, xland, wland, qkv, pk2, u, xbuf, wbuf, obuf, pkv, gs, gr, hs, hr, ps, pr, ls, ws, os):
    g = Grid()
    g.barrier()
    seqs, seq, half = hid.shape
    piece = 512
    per = seq // piece
    pieces = (seqs // 2) * per
    units = 4
    chunk = units * 128
    n = wq.shape[0] // units

    def own(j):
        return wq.at[pl.ds(j * units, units)]

    def land(cc, rr, j):
        return wland.at[cc, rr, pl.ds(j * units, units)]

    gat = Gather(g, own, land, gs, gr, lambda j: True)

    def small():
        return remote(pk, pkv, ps, pr, g.Y)

    def hidden(p):
        s, q = p // per, p % per
        return remote(hid.at[g.oc * (seqs // 2) + s, pl.ds(q * piece, piece)], xland.at[s, pl.ds(q * piece, piece)], hs.at[p], hr.at[p], g.Y)

    small().start()
    for p in range(pieces):
        hidden(p).start()

    @functools.partial(chunked, n)
    def _(j):
        gat.start(0, j)
        gat.start(2, j)

    @functools.partial(chunked, n)
    def _(j):
        gat.start(1, j)

    small().wait_recv()
    pk2[g.c] = pk[...]
    pk2[g.oc] = pkv[...]

    def vec(name, cc, size, start=0):
        return pk2[cc, :, pl.ds(offs[name] + start, size)]

    def mine(p):
        s, q = p // per, p % per
        return pltpu.make_async_copy(hid.at[g.c * (seqs // 2) + s, pl.ds(q * piece, piece)], xbuf.at[p % 2, 0], ls.at[p % 2, 0])

    def theirs(p):
        s, q = p // per, p % per
        return pltpu.make_async_copy(xland.at[s, pl.ds(q * piece, piece)], xbuf.at[p % 2, 1], ls.at[p % 2, 1])

    gains = [vec('g1', cc, half) for cc in (g.c, g.oc)]
    shifts = [vec('s1', cc, half) for cc in (g.c, g.oc)]
    for p in range(pieces):
        mine(p).start()
        hidden(p).wait_recv()
        theirs(p).start()
        mine(p).wait()
        theirs(p).wait()
        sub = 64

        @functools.partial(chunked, piece // sub)
        def _(i):
            rows = pl.ds(pl.multiple_of(i * sub, sub), sub)
            res = norm_rows([xbuf[p % 2, 0, rows, :], xbuf[p % 2, 1, rows, :]], gains, shifts)
            to = pl.ds(pl.multiple_of(p * piece + i * sub, sub), sub)
            for cc, val in zip((g.c, g.oc), res):
                u[to, pl.ds(pl.multiple_of(cc * half, half), half)] = val

    def load_own(j, go):
        for i in range(units):
            for idx, rr in enumerate((g.r, g.rp, g.rx, g.rxp)):
                src = wq.at[j * units + i] if idx == 0 else wland.at[g.c, rr, j * units + i]
                go(pltpu.make_async_copy(src, wbuf.at[0, rr, :, pl.ds(i * 128, 128)], ws.at[0, i, idx]))

    def load_other(j, go):
        for i in range(units):
            go(pltpu.make_async_copy(wland.at[g.oc, :, j * units + i], wbuf.at[1, :, :, pl.ds(i * 128, 128)], ws.at[1, i, 0]))

    def out(slot, cc, j):
        return pltpu.make_async_copy(obuf.at[slot], qkv.at[:, pl.ds(pl.multiple_of(cc * (n * chunk) + j * chunk, chunk), chunk)], os.at[slot])

    def compute(slot, cc, j):
        @pl.when(j > 0)
        def _():
            out(slot, cc, j - 1).wait()

        bias = vec('bq', cc, chunk, pl.multiple_of(j * chunk, chunk))

        def emit(rows, val):
            obuf[slot, rows, :] = (val + bias).astype(BF)

        matmul_rows(u, wbuf.at[slot], 512, emit)
        out(slot, cc, j).start()

    consume(gat, n, load_own, load_other, compute)
    out(0, g.c, n - 1).wait()
    out(1, g.oc, n - 1).wait()
    small().wait_send()
    for p in range(pieces):
        hidden(p).wait_send()

    gat.drain(n)


def qkv_call(hidden, packed, wq, offs):
    seqs, seq, half = hidden.shape
    tokens = seqs // 2 * seq
    n = wq.shape[0] // 4
    dma = pltpu.SemaphoreType.DMA
    return pl.pallas_call(
        functools.partial(qkv_kernel, offs),
        in_specs=[ANY, pl.BlockSpec(memory_space=pltpu.VMEM), ANY],
        out_specs=[ANY, ANY, ANY, pl.BlockSpec(memory_space=pltpu.VMEM)],
        out_shape=[
            jax.ShapeDtypeStruct((seqs // 2, seq, half), BF),
            jax.ShapeDtypeStruct((2, 4) + wq.shape, BF),
            jax.ShapeDtypeStruct((tokens, 2 * wq.shape[0] * 128), BF),
            jax.ShapeDtypeStruct((2,) + packed.shape, F32),
        ],
        scratch_shapes=[
            pltpu.VMEM((tokens, 2 * half), BF),
            pltpu.VMEM((2, 2, 512, half), BF),
            pltpu.VMEM((2, 4, wq.shape[1], 512), BF),
            pltpu.VMEM((2, tokens, 512), BF),
            pltpu.VMEM(packed.shape, F32),
            dma((7, n)), dma((7, n)), dma((4,)), dma((4,)), dma, dma, dma((2, 2)), dma((2, 4, 4)), dma((2,)),
        ],
        compiler_params=pltpu.CompilerParams(collective_id=1, has_side_effects=True, vmem_limit_bytes=VMEM_LIMIT),
        name='qkv',
    )(hidden, packed, wq)


def attn_head(block, q_ref, k_ref, v_ref, o_ref):
    seq, size = q_ref.shape
    scale = size ** -0.5 * LOG2E
    tri = lax.broadcasted_iota(jnp.int32, (block, block), 0) >= lax.broadcasted_iota(jnp.int32, (block, block), 1)
    for i in range(seq // block):
        q = q_ref[i * block:(i + 1) * block, :]
        dn = (((1,), (1,)), ((), ()))
        diag = lax.dot_general(q, k_ref[i * block:(i + 1) * block, :], dn, preferred_element_type=F32)
        diag = jnp.where(tri, diag, -1e30)
        top = jnp.max(diag, axis=1, keepdims=True)
        if i:
            past = lax.dot_general(q, k_ref[:i * block, :], dn, preferred_element_type=F32)
            top = jnp.maximum(top, jnp.max(past, axis=1, keepdims=True))
        e_diag = jnp.exp2((diag - top) * scale)
        total = jnp.sum(e_diag, axis=1, keepdims=True)
        if i:
            e_past = jnp.exp2((past - top) * scale)
            total = total + jnp.sum(e_past, axis=1, keepdims=True)
        inv = 1.0 / total
        out = jnp.dot((e_diag * inv).astype(BF), v_ref[i * block:(i + 1) * block, :], preferred_element_type=F32)
        if i:
            out = out + jnp.dot((e_past * inv).astype(BF), v_ref[:i * block, :], preferred_element_type=F32)
        o_ref[i * block:(i + 1) * block, :] = out.astype(BF)


def columns(own_ref, wland, width):
    def cols(j):
        return pl.ds(pl.multiple_of(j * width, width), width)

    return (lambda j: own_ref.at[:, cols(j)]), (lambda cc, rr, j: wland.at[cc, rr, :, cols(j)])


def shard_loads(g, own, land_all, land, buf, sems, rel, j):
    if rel == 0:
        srcs = [own(j)] + [land(g.c, rr, j) for rr in (g.rp, g.rx, g.rxp)]
        return [pltpu.make_async_copy(s, buf.at[rr], sems.at[i]) for i, (s, rr) in enumerate(zip(srcs, (g.r, g.rp, g.rx, g.rxp)))]
    return [pltpu.make_async_copy(land_all(g.oc, j), buf, sems.at[0])]


def attn_kernel(n, q_ref, k_ref, v_ref, w, o_ref, wland, gs, gr):
    step = pl.program_id(0) * pl.num_programs(1) + pl.program_id(1)
    steps = pl.num_programs(0) * pl.num_programs(1)
    g = Grid()
    own, land = columns(w, wland, w.shape[1] // n)
    gat = Gather(g, own, land, gs, gr, lambda j: j == 0)

    @pl.when(step == 0)
    def _():
        g.barrier()
        for j in range(n):
            for kind in range(3):
                gat.start(kind, j)

    for j, when in enumerate((14, 28)):
        @pl.when(step == when)
        def _():
            gat.arrive(0, j)
            gat.start(3, j)
            gat.arrive(1, j)
            gat.start(4, j)
            relay = gat.desc(6, j, j == 0)
            relay.start()

    @pl.when(step == 42)
    def _():
        for j in range(n):
            gat.arrive(6, j)
            gat.start(5, j)

    attn_head(256, q_ref, k_ref, v_ref, o_ref)

    @pl.when(step == steps - 1)
    def _():
        for j in range(n):
            for kind in range(2, 6):
                gat.arrive(kind, j)
            for kind in range(6):
                gat.desc(kind, j).wait_send()
            gat.desc(6, j, j == 0).wait_send()


def attn_call(qkv, w, seqs, heads, size):
    tokens = qkv.shape[0]
    seq = tokens // seqs
    n = 2
    spec = lambda part: pl.BlockSpec((seq, size), lambda s, h: (s, (h // heads) * 3 * heads + part * heads + h % heads))
    dma = pltpu.SemaphoreType.DMA
    return pl.pallas_call(
        functools.partial(attn_kernel, n),
        grid=(seqs, 2 * heads),
        in_specs=[spec(0), spec(1), spec(2), ANY],
        out_specs=[pl.BlockSpec((seq, size), lambda s, h: (s, h)), ANY],
        out_shape=[jax.ShapeDtypeStruct((tokens, 2 * heads * size), BF), jax.ShapeDtypeStruct((2, 4) + w.shape, BF)],
        scratch_shapes=[dma((7, n)), dma((7, n))],
        compiler_params=pltpu.CompilerParams(collective_id=2, has_side_effects=True, vmem_limit_bytes=VMEM_LIMIT),
        name='attn',
    )(qkv, qkv, qkv, w)


def up_kernel(offs, o, hid, xland, wo, woland, wu, pk2, h, act, wuland, ob, wob, xb, hb, ab, wbuf, obuf, gs, gr, ol, wl, xl, hl, ws, os):
    g = Grid()
    g.barrier()
    seqs, seq, half = hid.shape
    width = 512
    n = wu.shape[1] // width
    own, land = columns(wu, wuland, width)
    gat = Gather(g, own, land, gs, gr, lambda j: j % 2 == 0)

    @functools.partial(chunked, n)
    def _(j):
        for kind in range(3):
            gat.start(kind, j)

    def vec(name, cc, size, start=0):
        return pk2[cc, :, pl.ds(offs[name] + start, size)]

    own_o, land_o = columns(wo, woland, width)
    per = half // width

    def fetch(q, act_on):
        slot = q % 2
        rel, j = q // per, q % per
        cols = pl.ds(j * width, width)
        copies = shard_loads(g, own_o, lambda cc, j: woland.at[cc, :, :, cols], land_o, wob.at[slot], wl.at[slot], rel, j)
        for s in range(seqs // 2):
            src = hid.at[g.c * (seqs // 2) + s, :, cols] if rel == 0 else xland.at[s, :, cols]
            copies.append(pltpu.make_async_copy(src, xb.at[slot, pl.ds(s * seq, seq)], xl.at[slot, s]))
        for copy in copies:
            act_on(copy)

    load_o = pltpu.make_async_copy(o, ob, ol)
    load_o.start()
    fetch(0, BEGIN)
    load_o.wait()
    for q in range(2 * per):
        slot = q % 2
        if q + 1 < 2 * per:
            fetch(q + 1, BEGIN)
        fetch(q, FINISH)
        cc = g.c if q < per else g.oc
        bias = vec('bo', cc, width, (q % per) * width)
        at = pl.ds(pl.multiple_of(cc * half + (q % per) * width, width), width)

        def emit(rows, val):
            hb[rows, at] = (xb[slot, rows, :].astype(F32) + val + bias).astype(BF)

        matmul_rows(ob, wob.at[slot], 256, emit)

    store_h = pltpu.make_async_copy(hb, h, hl)
    store_h.start()

    gains = [vec('g2', cc, half) for cc in range(2)]
    shifts = [vec('s2', cc, half) for cc in range(2)]
    sub = 64

    @functools.partial(chunked, hb.shape[0] // sub)
    def _(i):
        rows = pl.ds(pl.multiple_of(i * sub, sub), sub)
        res = norm_rows([hb[rows, :half], hb[rows, half:]], gains, shifts)
        ab[rows, :half] = res[0]
        ab[rows, half:] = res[1]

    def cols_of(j):
        return pl.ds(pl.multiple_of(j * width, width), width)

    def load(rel, j, act_on):
        for copy in shard_loads(g, own, lambda cc, j: wuland.at[cc, :, :, cols_of(j)], land, wbuf.at[rel], ws.at[rel], rel, j):
            act_on(copy)

    def out(slot, cc, j):
        return pltpu.make_async_copy(obuf.at[slot], act.at[:, pl.ds(pl.multiple_of(cc * (n * width) + j * width, width), width)], os.at[slot])

    def compute(slot, cc, j):
        @pl.when(j > 0)
        def _():
            out(slot, cc, j - 1).wait()

        bias = vec('bu', cc, width, pl.multiple_of(j * width, width))

        def emit(rows, val):
            obuf[slot, rows, :] = jax.nn.gelu(val + bias, approximate=True).astype(BF)

        matmul_rows(ab, wbuf.at[slot], 256, emit)
        out(slot, cc, j).start()

    consume(gat, n, functools.partial(load, 0), functools.partial(load, 1), compute)
    out(0, g.c, n - 1).wait()
    out(1, g.oc, n - 1).wait()
    store_h.wait()
    gat.drain(n)


def up_call(o, hidden, got, wo, wo_land, wu, pk2, offs):
    tokens = o.shape[0]
    half = hidden.shape[2]
    n = wu.shape[1] // 512
    dma = pltpu.SemaphoreType.DMA
    return pl.pallas_call(
        functools.partial(up_kernel, offs),
        in_specs=[ANY] * 6 + [pl.BlockSpec(memory_space=pltpu.VMEM)],
        out_specs=[ANY] * 3,
        out_shape=[
            jax.ShapeDtypeStruct((tokens, 2 * half), BF),
            jax.ShapeDtypeStruct((tokens, 2 * wu.shape[1]), BF),
            jax.ShapeDtypeStruct((2, 4) + wu.shape, BF),
        ],
        scratch_shapes=[
            pltpu.VMEM(o.shape, BF),
            pltpu.VMEM((2, 4, wo.shape[0], 512), BF),
            pltpu.VMEM((2, tokens, 512), BF),
            pltpu.VMEM((tokens, 2 * half), BF),
            pltpu.VMEM((tokens, 2 * half), BF),
            pltpu.VMEM((2, 4, wu.shape[0], 512), BF),
            pltpu.VMEM((2, tokens, 512), BF),
            dma((7, n)), dma((7, n)), dma, dma((2, 4)), dma((2, 2)), dma, dma((2, 4)), dma((2,)),
        ],
        compiler_params=pltpu.CompilerParams(collective_id=3, has_side_effects=True, vmem_limit_bytes=VMEM_LIMIT),
        name='up',
    )(o, hidden, got, wo, wo_land, wu, pk2)


def down_kernel(offs, act, h, w, pk2, out, wland, ab, wbuf, hb, obuf, gs, gr, al, ws, hl, os, ps, pr):
    g = Grid()
    g.barrier()
    seqs, seq, half = out.shape
    mine = seqs // 2
    width = 256
    n = half // width
    own, land = columns(w, wland, width)
    gat = Gather(g, own, land, gs, gr, lambda j: True)

    gat.start(0, 0)
    for j in range(n):
        gat.start(1, j)
        gat.start(2, j)
    parts = ab.shape[1] // al.shape[0]
    loads = [pltpu.make_async_copy(act.at[:, pl.ds(i * parts, parts)], ab.at[:, pl.ds(i * parts, parts)], al.at[i]) for i in range(al.shape[0])]
    for load in loads:
        load.start()

    def cols(j):
        return pl.ds(pl.multiple_of(j * width, width), width)

    def fetch(rel, j, act_on):
        copies = shard_loads(g, own, lambda cc, j: wland.at[cc, :, :, cols(j)], land, wbuf.at[rel], ws.at[rel], rel, j)
        cc = g.oc if rel else g.c
        copies.append(pltpu.make_async_copy(h.at[:, pl.ds(pl.multiple_of(cc * half + j * width, width), width)], hb.at[rel], hl.at[rel]))
        for copy in copies:
            act_on(copy)

    def keep(s, j):
        return pltpu.make_async_copy(obuf.at[0, pl.ds(s * seq, seq)], out.at[g.c * mine + s, :, cols(j)], os.at[s])

    def give(s, j):
        return remote(obuf.at[1, pl.ds(s * seq, seq)], out.at[g.c * mine + s, :, cols(j)], ps.at[s, j], pr.at[s, j], g.Y)

    def compute(rel, j):
        fetch(rel, j, BEGIN)
        bias = pk2[g.oc if rel else g.c, :, pl.ds(pl.multiple_of(offs['bd'] + j * width, width), width)]

        @pl.when(j > 0)
        def _():
            for s in range(mine):
                if rel:
                    give(s, j - 1).wait_send()
                else:
                    keep(s, j - 1).wait()

        fetch(rel, j, FINISH)

        def emit(rows, val):
            obuf[rel, rows, :] = (hb[rel, rows, :].astype(F32) + val + bias).astype(BF)

        matmul_rows(ab, wbuf.at[rel], 512, emit)
        for s in range(mine):
            (give if rel else keep)(s, j).start()

    @functools.partial(chunked, 2 * n)
    def _(t):
        @pl.when(t < n)
        def _():
            gat.arrive(1, t)
            gat.start(4, t)
            gat.start(6, t)

        @pl.when(t == 0)
        def _():
            gat.arrive(0, 0)
            gat.start(3, 0)

        @pl.when(t == n - 1)
        def _():
            for j in range(1, n):
                gat.start(0, j)

        @pl.when((t >= 1) & (t <= n))
        def _():
            gat.arrive(6, t - 1)
            gat.start(5, t - 1)

        @pl.when(t == 1)
        def _():
            for load in loads:
                load.wait()

        @pl.when((t >= 2) & (t < n + 2))
        def _():
            gat.arrive(4, t - 2)
            gat.arrive(5, t - 2)
            compute(1, t - 2)

        @pl.when(t > n)
        def _():
            gat.arrive(0, t - n)
            gat.start(3, t - n)

        @pl.when((t == 1) | (t > n))
        def _():
            j = jnp.maximum(t - n, 0)
            gat.arrive(2, j)
            gat.arrive(3, j)
            compute(0, j)

    for s in range(mine):
        keep(s, n - 1).wait()
        give(s, n - 1).wait_send()
        for j in range(n):
            got = out.at[g.oc * mine + s, :, cols(j)]
            remote(got, got, ps.at[s, j], pr.at[s, j], g.Y).wait_recv()
    gat.drain(n)


def down_call(act, h, w, pk2, offs, seqs):
    tokens = act.shape[0]
    half = w.shape[1]
    n = half // 256
    dma = pltpu.SemaphoreType.DMA
    return pl.pallas_call(
        functools.partial(down_kernel, offs),
        in_specs=[ANY] * 3 + [pl.BlockSpec(memory_space=pltpu.VMEM)],
        out_specs=[ANY] * 2,
        out_shape=[jax.ShapeDtypeStruct((seqs, 2 * tokens // seqs, half), BF), jax.ShapeDtypeStruct((2, 4) + w.shape, BF)],
        scratch_shapes=[
            pltpu.VMEM(act.shape, BF),
            pltpu.VMEM((2, 4, w.shape[0], 256), BF),
            pltpu.VMEM((2, tokens, 256), BF),
            pltpu.VMEM((2, tokens, 256), BF),
            dma((7, n)), dma((7, n)), dma((8,)), dma((2, 4)), dma((2,)), dma((2,)), dma((2, n)), dma((2, n)),
        ],
        compiler_params=pltpu.CompilerParams(collective_id=4, has_side_effects=True, vmem_limit_bytes=VMEM_LIMIT),
        name='down',
    )(act, h, w, pk2)


def solution(mesh):
    act_spec = P(('dp', 'row'), None, 'col')
    arg_specs = (act_spec, P('col'), P('col'), P('row', None, 'col', None), P(None, 'col', None), P('row', None, 'col'), P('col'), P('col'), P('col'), P('row', 'col'), P('col'), P('row', 'col'), P('col'))

    def local_layer(hidden, ln1_gain, ln1_bias, w_qkv, b_qkv, w_out, b_out, ln2_gain, ln2_bias, w_up, b_up, w_down, b_down):
        seqs, _, half = hidden.shape
        heads, size = w_qkv.shape[2], w_qkv.shape[3]
        small = {'g1': ln1_gain, 's1': ln1_bias, 'g2': ln2_gain, 's2': ln2_bias, 'bo': b_out, 'bd': b_down, 'bq': b_qkv, 'bu': b_up}
        offs, at = {}, 0
        for name, a in small.items():
            offs[name], at = at, at + a.size
        packed = jnp.concatenate([a.reshape(-1).astype(F32) for a in small.values()])[None]
        wq = jnp.transpose(w_qkv, (1, 2, 0, 3)).reshape(3 * heads, w_qkv.shape[0], size)
        wo = w_out.reshape(-1, half)
        got, _, qkv, pk2 = qkv_call(hidden, packed, wq, offs)
        o, wo_land = attn_call(qkv, wo, seqs // 2, heads, size)
        h, act, _ = up_call(o, hidden, got, wo, wo_land, w_up, pk2, offs)
        return down_call(act, h, w_down, pk2, offs, seqs)[0]

    return jax.shard_map(local_layer, mesh=mesh, in_specs=arg_specs, out_specs=act_spec, check_vma=False)
```

```python
import functools

import jax
import jax.numpy as jnp
from jax import lax
from jax.experimental import pallas as pl
from jax.experimental.pallas import tpu as pltpu
from jax.sharding import PartitionSpec as P

LN_EPS = 1e-5
BF = jnp.bfloat16
F32 = jnp.float32
LOG2E = 1.4426950408889634
MESH = pl.DeviceIdType.MESH
ANY = pl.BlockSpec(memory_space=pl.ANY)
VMEM_LIMIT = 63 * 1024 * 1024


class Grid:
    def __init__(self):
        self.c = lax.axis_index('col')
        self.r = lax.axis_index('row')
        self.oc = 1 - self.c
        x = self.r // 2
        k = self.r - 2 * x
        self.rp = 2 * x + 1 - k
        self.rx = 2 * (1 - x) + k
        self.rxp = 2 * (1 - x) + 1 - k
        self.P, self.X, self.Y = {'row': self.rp}, {'row': self.rx}, {'col': self.oc}

    def barrier(self):
        sem = pltpu.get_barrier_semaphore()
        for dev in (self.P, self.X, self.Y):
            pl.semaphore_signal(sem, inc=1, device_id=dev, device_id_type=MESH)
        pl.semaphore_wait(sem, 3)


def remote(src, dst, send, recv, dev):
    return pltpu.make_async_remote_copy(src_ref=src, dst_ref=dst, send_sem=send, recv_sem=recv, device_id=dev, device_id_type=MESH)


class Gather:
    def __init__(self, g, own, land, send, recv, via_x):
        self.g, self.own, self.land, self.send_sem, self.recv_sem, self.via_x = g, own, land, send, recv, via_x

    def desc(self, kind, j, via_x=True):
        g = self.g
        if kind < 3:
            src, dst = self.own(j), self.land(g.c, g.r, j)
            dev = (g.X, g.Y, g.P)[kind]
        else:
            at = {3: (g.c, g.rx), 4: (g.oc, g.r), 5: (g.oc, g.rx), 6: (g.oc, g.r) if via_x else (g.c, g.rx)}[kind]
            src = dst = self.land(*at, j)
            dev = g.P if kind < 6 else (g.X if via_x else g.Y)
        return remote(src, dst, self.send_sem.at[kind, j], self.recv_sem.at[kind, j], dev)

    def routed(self, j, act):
        via = self.via_x(j)
        if isinstance(via, bool):
            act(self.desc(6, j, via))
            return

        @pl.when(via)
        def _():
            act(self.desc(6, j))

        @pl.when(jnp.logical_not(via))
        def _():
            act(self.desc(6, j, False))

    def start(self, kind, j):
        if kind == 6:
            self.routed(j, lambda d: d.start())
        else:
            self.desc(kind, j).start()

    def arrive(self, kind, j):
        g = self.g
        at = [(g.c, g.rx), (g.oc, g.r), (g.c, g.rp), (g.c, g.rxp), (g.oc, g.rp), (g.oc, g.rxp), (g.oc, g.rx)][kind]
        ref = self.land(*at, j)
        remote(ref, ref, self.send_sem.at[kind, j], self.recv_sem.at[kind, j], g.P).wait_recv()

    def drain(self, kinds, lo, hi):
        @functools.partial(chunked, hi - lo)
        def _(i):
            for kind in kinds:
                if kind == 6:
                    self.routed(lo + i, lambda d: d.wait_send())
                else:
                    self.desc(kind, lo + i).wait_send()


def chunked(total, body):
    lax.fori_loop(0, total, lambda j, carry: (body(j), carry)[1], 0)


def matmul_rows(a_ref, w_ref, tile, emit):
    depth = w_ref.shape[0] * w_ref.shape[1]

    def body(m):
        rows = pl.ds(pl.multiple_of(m * tile, tile), tile)
        w = w_ref[...].reshape(depth, w_ref.shape[2])
        emit(rows, jnp.dot(a_ref[rows, :], w, preferred_element_type=F32))

    chunked(a_ref.shape[0] // tile, body)


def norm_rows(parts, gains, shifts):
    parts = [p.astype(F32) for p in parts]
    width = sum(p.shape[1] for p in parts)
    mean = sum(jnp.sum(p, axis=1, keepdims=True) for p in parts) / width
    parts = [p - mean for p in parts]
    var = sum(jnp.sum(p * p, axis=1, keepdims=True) for p in parts) / width
    inv = lax.rsqrt(var + LN_EPS)
    return [(p * inv * gn + sh).astype(BF) for p, gn, sh in zip(parts, gains, shifts)]


BEGIN, FINISH = (lambda d: d.start()), (lambda d: d.wait())


def consume(gat, n, load_own, load_other, compute, last):
    g = gat.g

    @functools.partial(chunked, n + 3)
    def _(t):
        @pl.when(t < n)
        def _():
            gat.arrive(0, t)
            gat.start(3, t)
            gat.arrive(1, t)
            gat.start(4, t)
            gat.start(6, t)

        @pl.when(t == n - 1)
        def _():
            last()

        @pl.when((t >= 1) & (t <= n))
        def _():
            gat.arrive(6, t - 1)
            gat.start(5, t - 1)

        @pl.when(t < n)
        def _():
            gat.arrive(2, t)
            gat.arrive(3, t)
            load_own(t, BEGIN)

        @pl.when(t >= 3)
        def _():
            load_other(t - 3, FINISH)
            compute(1, g.oc, t - 3)

        @pl.when((t >= 2) & (t < n + 2))
        def _():
            gat.arrive(4, t - 2)
            gat.arrive(5, t - 2)
            load_other(t - 2, BEGIN)

        @pl.when(t < n)
        def _():
            load_own(t, FINISH)
            compute(0, g.c, t)


def columns(own_ref, wland, width):
    def cols(j):
        return pl.ds(pl.multiple_of(j * width, width), width)

    return (lambda j: own_ref.at[:, cols(j)]), (lambda cc, rr, j: wland.at[cc, rr, :, cols(j)])


def shard_loads(g, own, land_all, land, buf, sems, rel, j):
    if rel == 0:
        srcs = [own(j)] + [land(g.c, rr, j) for rr in (g.rp, g.rx, g.rxp)]
        return [pltpu.make_async_copy(s, buf.at[rr], sems.at[i]) for i, (s, rr) in enumerate(zip(srcs, (g.r, g.rp, g.rx, g.rxp)))]
    return [pltpu.make_async_copy(land_all(g.oc, j), buf, sems.at[0])]


def qkv_kernel(offs, hid, pk, wq, wo, xland, wland, qkv, pk2, woland, u, xbuf, wbuf, obuf, pkv, gs, gr, es, er, hs, hr, ps, pr, ls, ws, os):
    g = Grid()
    g.barrier()
    seqs, seq, half = hid.shape
    piece = 512
    per = seq // piece
    pieces = (seqs // 2) * per
    units = 4
    chunk = units * 128
    n = wq.shape[0] // units

    def own(j):
        return wq.at[pl.ds(j * units, units)]

    def land(cc, rr, j):
        return wland.at[cc, rr, pl.ds(j * units, units)]

    gat = Gather(g, own, land, gs, gr, lambda j: True)

    def small():
        return remote(pk, pkv, ps, pr, g.Y)

    def hidden(p):
        s, q = p // per, p % per
        return remote(hid.at[g.oc * (seqs // 2) + s, pl.ds(q * piece, piece)], xland.at[s, pl.ds(q * piece, piece)], hs.at[p], hr.at[p], g.Y)

    small().start()
    for p in range(pieces):
        hidden(p).start()

    @functools.partial(chunked, n)
    def _(j):
        gat.start(0, j)
        gat.start(2, j)

    @functools.partial(chunked, n)
    def _(j):
        gat.start(1, j)

    nxt = Gather(g, *columns(wo, woland, 512), es, er, None)
    nxt.start(1, 0)
    nxt.start(2, 0)

    small().wait_recv()
    pk2[g.c] = pk[...]
    pk2[g.oc] = pkv[...]

    def vec(name, cc, size, start=0):
        return pk2[cc, :, pl.ds(offs[name] + start, size)]

    def mine(p):
        s, q = p // per, p % per
        return pltpu.make_async_copy(hid.at[g.c * (seqs // 2) + s, pl.ds(q * piece, piece)], xbuf.at[p % 2, 0], ls.at[p % 2, 0])

    def theirs(p):
        s, q = p // per, p % per
        return pltpu.make_async_copy(xland.at[s, pl.ds(q * piece, piece)], xbuf.at[p % 2, 1], ls.at[p % 2, 1])

    gains = [vec('g1', cc, half) for cc in (g.c, g.oc)]
    shifts = [vec('s1', cc, half) for cc in (g.c, g.oc)]
    for p in range(pieces):
        mine(p).start()
        hidden(p).wait_recv()
        theirs(p).start()
        mine(p).wait()
        theirs(p).wait()
        sub = 64

        @functools.partial(chunked, piece // sub)
        def _(i):
            rows = pl.ds(pl.multiple_of(i * sub, sub), sub)
            res = norm_rows([xbuf[p % 2, 0, rows, :], xbuf[p % 2, 1, rows, :]], gains, shifts)
            to = pl.ds(pl.multiple_of(p * piece + i * sub, sub), sub)
            for cc, val in zip((g.c, g.oc), res):
                u[to, pl.ds(pl.multiple_of(cc * half, half), half)] = val

    def load_own(j, go):
        for i in range(units):
            for idx, rr in enumerate((g.r, g.rp, g.rx, g.rxp)):
                src = wq.at[j * units + i] if idx == 0 else wland.at[g.c, rr, j * units + i]
                go(pltpu.make_async_copy(src, wbuf.at[0, rr, :, pl.ds(i * 128, 128)], ws.at[0, i, idx]))

    def load_other(j, go):
        for i in range(units):
            go(pltpu.make_async_copy(wland.at[g.oc, :, j * units + i], wbuf.at[1, :, :, pl.ds(i * 128, 128)], ws.at[1, i, 0]))

    def out(slot, cc, j):
        return pltpu.make_async_copy(obuf.at[slot], qkv.at[:, pl.ds(pl.multiple_of(cc * (n * chunk) + j * chunk, chunk), chunk)], os.at[slot])

    def compute(slot, cc, j):
        @pl.when(j > 0)
        def _():
            out(slot, cc, j - 1).wait()

        bias = vec('bq', cc, chunk, pl.multiple_of(j * chunk, chunk))

        def emit(rows, val):
            obuf[slot, rows, :] = (val + bias).astype(BF)

        matmul_rows(u, wbuf.at[slot], 1024, emit)
        out(slot, cc, j).start()

    consume(gat, n, load_own, load_other, compute, lambda: nxt.start(0, 0))
    out(0, g.c, n - 1).wait()
    out(1, g.oc, n - 1).wait()
    small().wait_send()
    for p in range(pieces):
        hidden(p).wait_send()

    gat.drain(range(7), 0, n)
    for kind in range(3):
        nxt.arrive(kind, 0)
    nxt.drain(range(3), 0, 1)


def qkv_call(hidden, packed, wq, wo, offs):
    seqs, seq, half = hidden.shape
    tokens = seqs // 2 * seq
    n = wq.shape[0] // 4
    dma = pltpu.SemaphoreType.DMA
    return pl.pallas_call(
        functools.partial(qkv_kernel, offs),
        in_specs=[ANY, pl.BlockSpec(memory_space=pltpu.VMEM), ANY, ANY],
        out_specs=[ANY, ANY, ANY, pl.BlockSpec(memory_space=pltpu.VMEM), ANY],
        out_shape=[
            jax.ShapeDtypeStruct((seqs // 2, seq, half), BF),
            jax.ShapeDtypeStruct((2, 4) + wq.shape, BF),
            jax.ShapeDtypeStruct((tokens, 2 * wq.shape[0] * 128), BF),
            jax.ShapeDtypeStruct((2,) + packed.shape, F32),
            jax.ShapeDtypeStruct((2, 4) + wo.shape, BF),
        ],
        scratch_shapes=[
            pltpu.VMEM((tokens, 2 * half), BF),
            pltpu.VMEM((2, 2, 512, half), BF),
            pltpu.VMEM((2, 4, wq.shape[1], 512), BF),
            pltpu.VMEM((2, tokens, 512), BF),
            pltpu.VMEM(packed.shape, F32),
            dma((7, n)), dma((7, n)), dma((3, 1)), dma((3, 1)), dma((4,)), dma((4,)), dma, dma, dma((2, 2)), dma((2, 4, 4)), dma((2,)),
        ],
        compiler_params=pltpu.CompilerParams(collective_id=1, has_side_effects=True, vmem_limit_bytes=VMEM_LIMIT),
        name='qkv',
    )(hidden, packed, wq, wo)


def attn_head(block, q_ref, k_ref, v_ref, o_ref):
    seq, size = q_ref.shape
    scale = size ** -0.5 * LOG2E
    tri = lax.broadcasted_iota(jnp.int32, (block, block), 0) >= lax.broadcasted_iota(jnp.int32, (block, block), 1)
    for i in range(seq // block):
        q = q_ref[i * block:(i + 1) * block, :]
        dn = (((1,), (1,)), ((), ()))
        diag = lax.dot_general(q, k_ref[i * block:(i + 1) * block, :], dn, preferred_element_type=F32)
        diag = jnp.where(tri, diag, -1e30)
        top = jnp.max(diag, axis=1, keepdims=True)
        if i:
            past = lax.dot_general(q, k_ref[:i * block, :], dn, preferred_element_type=F32)
            top = jnp.maximum(top, jnp.max(past, axis=1, keepdims=True))
        e_diag = jnp.exp2((diag - top) * scale)
        total = jnp.sum(e_diag, axis=1, keepdims=True)
        if i:
            e_past = jnp.exp2((past - top) * scale)
            total = total + jnp.sum(e_past, axis=1, keepdims=True)
        inv = 1.0 / total
        out = jnp.dot((e_diag * inv).astype(BF), v_ref[i * block:(i + 1) * block, :], preferred_element_type=F32)
        if i:
            out = out + jnp.dot((e_past * inv).astype(BF), v_ref[:i * block, :], preferred_element_type=F32)
        o_ref[i * block:(i + 1) * block, :] = out.astype(BF)


def attn_kernel(ahead, q_ref, k_ref, v_ref, w, wu, woin, o_ref, wland, wuland, gs, gr, us, ur):
    step = pl.program_id(0) * pl.num_programs(1) + pl.program_id(1)
    steps = pl.num_programs(0) * pl.num_programs(1)
    g = Grid()
    gat = Gather(g, *columns(w, wland, 512), gs, gr, lambda j: j == 0)
    nxt = Gather(g, *columns(wu, wuland, 512), us, ur, lambda j: j % 2 == 0)

    def at(when):
        return pl.when(step == when)

    def relay(gather, j):
        gather.arrive(0, j)
        gather.start(3, j)
        gather.arrive(1, j)
        gather.start(4, j)
        gather.start(6, j)

    def push(gather, j):
        gather.arrive(6, j)
        gather.start(5, j)

    @at(0)
    def _():
        g.barrier()
        gat.start(6, 0)
        gat.start(3, 0)
        gat.start(4, 0)
        for kind in range(3):
            gat.start(kind, 1)
        for j in range(ahead):
            for kind in range(3):
                nxt.start(kind, j)

    @at(9)
    def _():
        push(gat, 0)

    @at(16)
    def _():
        relay(gat, 1)

    for j, when in zip(range(ahead), (20, 25, 31, 36)):
        @at(when)
        def _():
            relay(nxt, j)

    @at(41)
    def _():
        push(gat, 1)
        for j in range(2):
            push(nxt, j)

    attn_head(256, q_ref, k_ref, v_ref, o_ref)

    @at(steps - 1)
    def _():
        for j in range(2, ahead):
            push(nxt, j)
        for kind in range(3, 6):
            gat.arrive(kind, 0)
        for kind in range(2, 6):
            gat.arrive(kind, 1)
            for j in range(ahead):
                nxt.arrive(kind, j)
        gat.drain(range(3, 6), 0, 1)
        gat.drain(range(6), 1, 2)
        for j in range(2):
            gat.routed(j, lambda d: d.wait_send())
        nxt.drain(range(7), 0, ahead)


AHEAD = 4


def attn_call(qkv, w, wo_land, wu, seqs, heads, size):
    tokens = qkv.shape[0]
    seq = tokens // seqs
    spec = lambda part: pl.BlockSpec((seq, size), lambda s, h: (s, (h // heads) * 3 * heads + part * heads + h % heads))
    dma = pltpu.SemaphoreType.DMA
    return pl.pallas_call(
        functools.partial(attn_kernel, AHEAD),
        grid=(seqs, 2 * heads),
        in_specs=[spec(0), spec(1), spec(2), ANY, ANY, ANY],
        out_specs=[pl.BlockSpec((seq, size), lambda s, h: (s, h)), ANY, ANY],
        out_shape=[
            jax.ShapeDtypeStruct((tokens, 2 * heads * size), BF),
            jax.ShapeDtypeStruct(wo_land.shape, BF),
            jax.ShapeDtypeStruct((2, 4) + wu.shape, BF),
        ],
        scratch_shapes=[dma((7, 2)), dma((7, 2)), dma((7, AHEAD)), dma((7, AHEAD))],
        input_output_aliases={5: 1},
        compiler_params=pltpu.CompilerParams(collective_id=2, has_side_effects=True, vmem_limit_bytes=VMEM_LIMIT),
        name='attn',
    )(qkv, qkv, qkv, w, wu, wo_land)


def up_kernel(offs, ahead, o, hid, xland, wo, woland, wu, pk2, wd, wuin, h, act, wuland, wdland, ob, wob, xb, hb, ab, wbuf, obuf, gs, gr, ds, dr, ol, wl, xl, hl, ws, os):
    g = Grid()
    g.barrier()
    seqs, seq, half = hid.shape
    width = 512
    n = wu.shape[1] // width
    own, land = columns(wu, wuland, width)
    gat = Gather(g, own, land, gs, gr, lambda j: j % 2 == 0)
    nxt = Gather(g, *columns(wd, wdland, 256), ds, dr, lambda j: True)

    for j in range(ahead, n):
        for kind in range(3):
            gat.start(kind, j)

    def relay(j):
        gat.arrive(0, j)
        gat.start(3, j)
        gat.arrive(1, j)
        gat.start(4, j)
        gat.start(6, j)

    def vec(name, cc, size, start=0):
        return pk2[cc, :, pl.ds(offs[name] + start, size)]

    own_o, land_o = columns(wo, woland, width)
    per = half // width

    def fetch(q, act_on):
        slot = q % 2
        rel, j = q // per, q % per
        cols = pl.ds(j * width, width)
        copies = shard_loads(g, own_o, lambda cc, j: woland.at[cc, :, :, cols], land_o, wob.at[slot], wl.at[slot], rel, j)
        for s in range(seqs // 2):
            src = hid.at[g.c * (seqs // 2) + s, :, cols] if rel == 0 else xland.at[s, :, cols]
            copies.append(pltpu.make_async_copy(src, xb.at[slot, pl.ds(s * seq, seq)], xl.at[slot, s]))
        for copy in copies:
            act_on(copy)

    load_o = pltpu.make_async_copy(o, ob, ol)
    load_o.start()
    fetch(0, BEGIN)
    load_o.wait()
    for q in range(2 * per):
        slot = q % 2
        if q + 1 < 2 * per:
            fetch(q + 1, BEGIN)
        fetch(q, FINISH)
        cc = g.c if q < per else g.oc
        bias = vec('bo', cc, width, (q % per) * width)
        at = pl.ds(pl.multiple_of(cc * half + (q % per) * width, width), width)

        def emit(rows, val):
            hb[rows, at] = (xb[slot, rows, :].astype(F32) + val + bias).astype(BF)

        matmul_rows(ob, wob.at[slot], 512, emit)
        if q in (0, 1, 3):
            relay(ahead + (0, 1, 1, 2)[q])

    store_h = pltpu.make_async_copy(hb, h, hl)
    store_h.start()

    gains = [vec('g2', cc, half) for cc in range(2)]
    shifts = [vec('s2', cc, half) for cc in range(2)]
    sub = 64

    @functools.partial(chunked, hb.shape[0] // sub)
    def _(i):
        rows = pl.ds(pl.multiple_of(i * sub, sub), sub)
        res = norm_rows([hb[rows, :half], hb[rows, half:]], gains, shifts)
        ab[rows, :half] = res[0]
        ab[rows, half:] = res[1]

    def cols_of(j):
        return pl.ds(pl.multiple_of(j * width, width), width)

    def load(rel, j, act_on):
        for copy in shard_loads(g, own, lambda cc, j: wuland.at[cc, :, :, cols_of(j)], land, wbuf.at[rel], ws.at[rel], rel, j):
            act_on(copy)

    def out(slot, cc, j):
        return pltpu.make_async_copy(obuf.at[slot], act.at[:, pl.ds(pl.multiple_of(cc * (n * width) + j * width, width), width)], os.at[slot])

    def compute(slot, cc, j):
        @pl.when(j > 0)
        def _():
            out(slot, cc, j - 1).wait()

        bias = vec('bu', cc, width, pl.multiple_of(j * width, width))

        def emit(rows, val):
            obuf[slot, rows, :] = jax.nn.gelu(val + bias, approximate=True).astype(BF)

        matmul_rows(ab, wbuf.at[slot], 1024, emit)
        out(slot, cc, j).start()

    for j in range(ahead + 3, n):
        relay(j)
    for kind, count in ((0, DOWN_X), (1, DOWN_Y), (2, wd.shape[1] // 256)):
        for j in range(count):
            nxt.start(kind, j)
    load(0, 0, BEGIN)
    load(1, 0, BEGIN)

    @functools.partial(chunked, n)
    def _(t):
        @pl.when((t >= 1) & (t <= (n - ahead) // 2))
        def _():
            for i in range(2):
                j = ahead + 2 * (t - 1) + i
                gat.arrive(6, j)
                gat.start(5, j)

        load(0, t, FINISH)
        compute(0, g.c, t)

        @pl.when(t == 4)
        def _():
            nxt.arrive(1, 0)
            nxt.start(4, 0)
            nxt.start(6, 0)
            nxt.arrive(0, 0)
            nxt.start(3, 0)

        @pl.when(t + 1 >= ahead)
        def _():
            @pl.when(t + 1 < n)
            def _():
                gat.arrive(2, t + 1)
                gat.arrive(3, t + 1)

        @pl.when(t + 1 < n)
        def _():
            load(0, t + 1, BEGIN)

        load(1, t, FINISH)
        compute(1, g.oc, t)

        @pl.when(t + 1 >= ahead)
        def _():
            @pl.when(t + 1 < n)
            def _():
                gat.arrive(4, t + 1)
                gat.arrive(5, t + 1)

        @pl.when(t + 1 < n)
        def _():
            load(1, t + 1, BEGIN)

    out(0, g.c, n - 1).wait()
    out(1, g.oc, n - 1).wait()
    store_h.wait()
    gat.drain(range(7), ahead, n)
    nxt.arrive(6, 0)
    nxt.start(5, 0)
    for kind, lo, hi in ((0, 1, DOWN_X), (1, 1, DOWN_Y), (2, 0, wd.shape[1] // 256), (3, 0, 1), (4, 0, 1), (5, 0, 1)):
        for j in range(lo, hi):
            nxt.arrive(kind, j)
    for kind, hi in ((0, DOWN_X), (1, DOWN_Y), (2, wd.shape[1] // 256), (3, 1), (4, 1), (5, 1), (6, 1)):
        nxt.drain((kind,), 0, hi)


DOWN_X, DOWN_Y = 2, 3


def up_call(o, hidden, got, wo, wo_land, wu, wu_land, wd, pk2, offs):
    tokens = o.shape[0]
    half = hidden.shape[2]
    n = wu.shape[1] // 512
    dma = pltpu.SemaphoreType.DMA
    return pl.pallas_call(
        functools.partial(up_kernel, offs, AHEAD),
        in_specs=[ANY] * 6 + [pl.BlockSpec(memory_space=pltpu.VMEM), ANY, ANY],
        out_specs=[ANY] * 4,
        out_shape=[
            jax.ShapeDtypeStruct((tokens, 2 * half), BF),
            jax.ShapeDtypeStruct((tokens, 2 * wu.shape[1]), BF),
            jax.ShapeDtypeStruct(wu_land.shape, BF),
            jax.ShapeDtypeStruct((2, 4) + wd.shape, BF),
        ],
        input_output_aliases={8: 2},
        scratch_shapes=[
            pltpu.VMEM(o.shape, BF),
            pltpu.VMEM((2, 4, wo.shape[0], 512), BF),
            pltpu.VMEM((2, tokens, 512), BF),
            pltpu.VMEM((tokens, 2 * half), BF),
            pltpu.VMEM((tokens, 2 * half), BF),
            pltpu.VMEM((2, 4, wu.shape[0], 512), BF),
            pltpu.VMEM((2, tokens, 512), BF),
            dma((7, n)), dma((7, n)), dma((7, 4)), dma((7, 4)), dma, dma((2, 4)), dma((2, 2)), dma, dma((2, 4)), dma((2,)),
        ],
        compiler_params=pltpu.CompilerParams(collective_id=3, has_side_effects=True, vmem_limit_bytes=VMEM_LIMIT),
        name='up',
    )(o, hidden, got, wo, wo_land, wu, pk2, wd, wu_land)


def down_kernel(offs, act, h, w, pk2, win, out, wland, ab, wbuf, hb, obuf, kbuf, gs, gr, al, ws, hl, os, ps, pr):
    g = Grid()
    g.barrier()
    seqs, seq, half = out.shape
    mine = seqs // 2
    width = 256
    n = half // width
    own, land = columns(w, wland, width)
    gat = Gather(g, own, land, gs, gr, lambda j: True)

    for j in range(1, DOWN_Y):
        gat.start(6, j)
        gat.start(4, j)
    for j in range(1, DOWN_X):
        gat.start(3, j)
    for j in range(DOWN_Y, n):
        gat.start(1, j)
    parts = ab.shape[1] // al.shape[0]
    loads = [pltpu.make_async_copy(act.at[:, pl.ds(i * parts, parts)], ab.at[:, pl.ds(i * parts, parts)], al.at[i]) for i in range(al.shape[0])]
    for load in loads:
        load.start()

    def cols(j):
        return pl.ds(pl.multiple_of(j * width, width), width)

    def fetch(rel, j, act_on):
        copies = shard_loads(g, own, lambda cc, j: wland.at[cc, :, :, cols(j)], land, wbuf.at[rel], ws.at[rel], rel, j)
        cc = g.oc if rel else g.c
        copies.append(pltpu.make_async_copy(h.at[:, pl.ds(pl.multiple_of(cc * half + j * width, width), width)], hb.at[rel], hl.at[rel]))
        for copy in copies:
            act_on(copy)

    def keep(s, j):
        return pltpu.make_async_copy(kbuf.at[pl.ds(s * seq, seq)], out.at[g.c * mine + s, :, cols(j)], os.at[s])

    def give(s, j):
        return remote(obuf.at[j, pl.ds(s * seq, seq)], out.at[g.c * mine + s, :, cols(j)], ps.at[s, j], pr.at[s, j], g.Y)

    def compute(rel, j):
        bias = pk2[g.oc if rel else g.c, :, pl.ds(pl.multiple_of(offs['bd'] + j * width, width), width)]

        if not rel:
            @pl.when(j > 0)
            def _():
                for s in range(mine):
                    keep(s, j - 1).wait()

        fetch(rel, j, FINISH)

        def emit(rows, val):
            val = (hb[rel, rows, :].astype(F32) + val + bias).astype(BF)
            if rel:
                obuf[j, rows, :] = val
            else:
                kbuf[rows, :] = val

        matmul_rows(ab, wbuf.at[rel], 1024, emit)
        for s in range(mine):
            (give if rel else keep)(s, j).start()

    fetch(1, 0, BEGIN)
    fetch(0, 0, BEGIN)
    for load in loads:
        load.wait()

    @functools.partial(chunked, n + 1)
    def _(t):
        @pl.when(t == 1)
        def _():
            for j in range(DOWN_Y, n):
                gat.arrive(1, j)
                gat.start(4, j)
                gat.start(6, j)
            for j in range(DOWN_X, n):
                gat.start(0, j)

        @pl.when((t >= 1) & (t < n))
        def _():
            gat.arrive(6, t)
            gat.start(5, t)
            gat.arrive(4, t)
            gat.arrive(5, t)
            fetch(1, t, BEGIN)

        @pl.when(t == 1)
        def _():
            gat.arrive(3, 1)
            fetch(0, 1, BEGIN)

        @pl.when(t < n)
        def _():
            compute(1, t)

        @pl.when(t >= n - 1)
        def _():
            gat.arrive(0, t - 1)
            gat.start(3, t - 1)
            gat.arrive(3, t - 1)
            fetch(0, t - 1, BEGIN)

        @pl.when(t != 2)
        def _():
            compute(0, jnp.where(t > 2, t - 1, t))

    for s in range(mine):
        keep(s, n - 1).wait()
        for j in range(n):
            give(s, j).wait_send()
            got = out.at[g.oc * mine + s, :, cols(j)]
            remote(got, got, ps.at[s, j], pr.at[s, j], g.Y).wait_recv()
    for kind, lo in ((0, DOWN_X), (1, DOWN_Y), (3, 1), (4, 1), (5, 1), (6, 1)):
        gat.drain((kind,), lo, n)


def down_call(act, h, w, w_land, pk2, offs, seqs):
    tokens = act.shape[0]
    half = w.shape[1]
    n = half // 256
    dma = pltpu.SemaphoreType.DMA
    return pl.pallas_call(
        functools.partial(down_kernel, offs),
        in_specs=[ANY] * 3 + [pl.BlockSpec(memory_space=pltpu.VMEM), ANY],
        out_specs=[ANY] * 2,
        input_output_aliases={4: 1},
        out_shape=[jax.ShapeDtypeStruct((seqs, 2 * tokens // seqs, half), BF), jax.ShapeDtypeStruct((2, 4) + w.shape, BF)],
        scratch_shapes=[
            pltpu.VMEM(act.shape, BF),
            pltpu.VMEM((2, 4, w.shape[0], 256), BF),
            pltpu.VMEM((2, tokens, 256), BF),
            pltpu.VMEM((n, tokens, 256), BF),
            pltpu.VMEM((tokens, 256), BF),
            dma((7, n)), dma((7, n)), dma((8,)), dma((2, 4)), dma((2,)), dma((2,)), dma((2, n)), dma((2, n)),
        ],
        compiler_params=pltpu.CompilerParams(collective_id=4, has_side_effects=True, vmem_limit_bytes=VMEM_LIMIT),
        name='down',
    )(act, h, w, pk2, w_land)


def solution(mesh):
    act_spec = P(('dp', 'row'), None, 'col')
    arg_specs = (act_spec, P('col'), P('col'), P('row', None, 'col', None), P(None, 'col', None), P('row', None, 'col'), P('col'), P('col'), P('col'), P('row', 'col'), P('col'), P('row', 'col'), P('col'))

    def local_layer(hidden, ln1_gain, ln1_bias, w_qkv, b_qkv, w_out, b_out, ln2_gain, ln2_bias, w_up, b_up, w_down, b_down):
        seqs, _, half = hidden.shape
        heads, size = w_qkv.shape[2], w_qkv.shape[3]
        small = {'g1': ln1_gain, 's1': ln1_bias, 'g2': ln2_gain, 's2': ln2_bias, 'bo': b_out, 'bd': b_down, 'bq': b_qkv, 'bu': b_up}
        offs, at = {}, 0
        for name, a in small.items():
            offs[name], at = at, at + a.size
        packed = jnp.concatenate([a.reshape(-1).astype(F32) for a in small.values()])[None]
        wq = jnp.transpose(w_qkv, (1, 2, 0, 3)).reshape(3 * heads, w_qkv.shape[0], size)
        wo = w_out.reshape(-1, half)
        got, _, qkv, pk2, wo_land = qkv_call(hidden, packed, wq, wo, offs)
        o, wo_land, wu_land = attn_call(qkv, wo, wo_land, w_up, seqs // 2, heads, size)
        h, act, _, wd_land = up_call(o, hidden, got, wo, wo_land, w_up, wu_land, w_down, pk2, offs)
        return down_call(act, h, w_down, wd_land, pk2, offs, seqs)[0]

    return jax.shard_map(local_layer, mesh=mesh, in_specs=arg_specs, out_specs=act_spec, check_vma=False)
```

```python
import functools

import jax
import jax.numpy as jnp
from jax import lax
from jax.experimental import pallas as pl
from jax.experimental.pallas import tpu as pltpu
from jax.sharding import PartitionSpec as P

LN_EPS = 1e-5
BF = jnp.bfloat16
F32 = jnp.float32
LOG2E = 1.4426950408889634
MESH = pl.DeviceIdType.MESH
ANY = pl.BlockSpec(memory_space=pl.ANY)
VMEM_LIMIT = 63 * 1024 * 1024


class Grid:
    def __init__(self):
        self.c = lax.axis_index('col')
        self.r = lax.axis_index('row')
        self.oc = 1 - self.c
        x = self.r // 2
        k = self.r - 2 * x
        self.rp = 2 * x + 1 - k
        self.rx = 2 * (1 - x) + k
        self.rxp = 2 * (1 - x) + 1 - k
        self.P, self.X, self.Y = {'row': self.rp}, {'row': self.rx}, {'col': self.oc}

    def barrier(self):
        sem = pltpu.get_barrier_semaphore()
        for dev in (self.P, self.X, self.Y):
            pl.semaphore_signal(sem, inc=1, device_id=dev, device_id_type=MESH)
        pl.semaphore_wait(sem, 3)


def remote(src, dst, send, recv, dev):
    return pltpu.make_async_remote_copy(src_ref=src, dst_ref=dst, send_sem=send, recv_sem=recv, device_id=dev, device_id_type=MESH)


class Gather:
    def __init__(self, g, own, land, send, recv, via_x):
        self.g, self.own, self.land, self.send_sem, self.recv_sem, self.via_x = g, own, land, send, recv, via_x

    def desc(self, kind, j, via_x=True):
        g = self.g
        if kind < 3:
            src, dst = self.own(j), self.land(g.c, g.r, j)
            dev = (g.X, g.Y, g.P)[kind]
        else:
            at = {3: (g.c, g.rx), 4: (g.oc, g.r), 5: (g.oc, g.rx), 6: (g.oc, g.r) if via_x else (g.c, g.rx)}[kind]
            src = dst = self.land(*at, j)
            dev = g.P if kind < 6 else (g.X if via_x else g.Y)
        return remote(src, dst, self.send_sem.at[kind, j], self.recv_sem.at[kind, j], dev)

    def routed(self, j, act):
        via = self.via_x(j)
        if isinstance(via, bool):
            act(self.desc(6, j, via))
            return

        @pl.when(via)
        def _():
            act(self.desc(6, j))

        @pl.when(jnp.logical_not(via))
        def _():
            act(self.desc(6, j, False))

    def start(self, kind, j):
        if kind == 6:
            self.routed(j, lambda d: d.start())
        else:
            self.desc(kind, j).start()

    def arrive(self, kind, j):
        g = self.g
        at = [(g.c, g.rx), (g.oc, g.r), (g.c, g.rp), (g.c, g.rxp), (g.oc, g.rp), (g.oc, g.rxp), (g.oc, g.rx)][kind]
        ref = self.land(*at, j)
        remote(ref, ref, self.send_sem.at[kind, j], self.recv_sem.at[kind, j], g.P).wait_recv()

    def drain(self, kinds, lo, hi):
        @functools.partial(chunked, hi - lo)
        def _(i):
            for kind in kinds:
                if kind == 6:
                    self.routed(lo + i, lambda d: d.wait_send())
                else:
                    self.desc(kind, lo + i).wait_send()

    def relay(self, j):
        self.arrive(0, j)
        self.start(3, j)
        self.arrive(1, j)
        self.start(4, j)
        self.start(6, j)

    def push(self, j):
        self.arrive(6, j)
        self.start(5, j)


def chunked(total, body):
    lax.fori_loop(0, total, lambda j, carry: (body(j), carry)[1], 0)


def matmul_rows(a_ref, w_ref, tile, emit):
    depth = w_ref.shape[0] * w_ref.shape[1]

    def body(m):
        rows = pl.ds(pl.multiple_of(m * tile, tile), tile)
        w = w_ref[...].reshape(depth, w_ref.shape[2])
        emit(rows, jnp.dot(a_ref[rows, :], w, preferred_element_type=F32))

    chunked(a_ref.shape[0] // tile, body)


def norm_rows(parts, gains, shifts):
    parts = [p.astype(F32) for p in parts]
    width = sum(p.shape[1] for p in parts)
    mean = sum(jnp.sum(p, axis=1, keepdims=True) for p in parts) / width
    parts = [p - mean for p in parts]
    var = sum(jnp.sum(p * p, axis=1, keepdims=True) for p in parts) / width
    inv = lax.rsqrt(var + LN_EPS)
    return [(p * inv * gn + sh).astype(BF) for p, gn, sh in zip(parts, gains, shifts)]


def columns(own_ref, wland, width):
    def cols(j):
        return pl.ds(pl.multiple_of(j * width, width), width)

    return (lambda j: own_ref.at[:, cols(j)]), (lambda cc, rr, j: wland.at[cc, rr, :, cols(j)])


def shard_loads(g, own, land_all, land, buf, sems, rel, j):
    if rel == 0:
        srcs = [own(j)] + [land(g.c, rr, j) for rr in (g.rp, g.rx, g.rxp)]
        return [pltpu.make_async_copy(s, buf.at[rr], sems.at[i]) for i, (s, rr) in enumerate(zip(srcs, (g.r, g.rp, g.rx, g.rxp)))]
    return [pltpu.make_async_copy(land_all(g.oc, j), buf, sems.at[0])]


def attn_head(block, q_ref, k_ref, v_ref, o_ref):
    seq, size = q_ref.shape
    scale = size ** -0.5 * LOG2E
    tri = lax.broadcasted_iota(jnp.int32, (block, block), 0) >= lax.broadcasted_iota(jnp.int32, (block, block), 1)
    for i in range(seq // block):
        q = q_ref[i * block:(i + 1) * block, :]
        dn = (((1,), (1,)), ((), ()))
        diag = lax.dot_general(q, k_ref[i * block:(i + 1) * block, :], dn, preferred_element_type=F32)
        diag = jnp.where(tri, diag, -1e30)
        top = jnp.max(diag, axis=1, keepdims=True)
        if i:
            past = lax.dot_general(q, k_ref[:i * block, :], dn, preferred_element_type=F32)
            top = jnp.maximum(top, jnp.max(past, axis=1, keepdims=True))
        e_diag = jnp.exp2((diag - top) * scale)
        total = jnp.sum(e_diag, axis=1, keepdims=True)
        if i:
            e_past = jnp.exp2((past - top) * scale)
            total = total + jnp.sum(e_past, axis=1, keepdims=True)
        inv = 1.0 / total
        out = jnp.dot((e_diag * inv).astype(BF), v_ref[i * block:(i + 1) * block, :], preferred_element_type=F32)
        if i:
            out = out + jnp.dot((e_past * inv).astype(BF), v_ref[:i * block, :], preferred_element_type=F32)
        o_ref[i * block:(i + 1) * block, :] = out.astype(BF)


BEGIN, FINISH = (lambda d: d.start()), (lambda d: d.wait())
WIDE, SLIM, LANES, PIECE = 512, 256, 128, 512
DOWN_X = 2


def aligned(start, size):
    return pl.ds(pl.multiple_of(start, size), size)


def layer_kernel(offs, hid, pk, wq, wo, wu, wd, out, xland, qkv, qland, oland, uland, dland, hb, ab, pk2,
                 qs, qr, os, oo, us, ur, ds, dr, hs, hr, ps, pr, ls, ws, st, al, gs, gr, ks):
    g = Grid()
    g.barrier()
    seqs, seq, half = hid.shape
    mine = seqs // 2
    tokens = mine * seq
    units = WIDE // LANES
    qgat = Gather(g, lambda j: wq.at[pl.ds(j * units, units)], lambda cc, rr, j: qland.at[cc, rr, pl.ds(j * units, units)], qs, qr, lambda j: True)
    ogat = Gather(g, *columns(wo, oland, WIDE), os, oo, lambda j: j == 0)
    ugat = Gather(g, *columns(wu, uland, WIDE), us, ur, lambda j: j % 2 == 0)
    dgat = Gather(g, *columns(wd, dland, SLIM), ds, dr, lambda j: True)
    nq, no, nu, nd = wq.shape[0] // units, wo.shape[1] // WIDE, wu.shape[1] // WIDE, wd.shape[1] // SLIM
    per = seq // PIECE
    pieces = mine * per

    def vec(name, cc, size, start=0):
        return pk2[cc, :, pl.ds(offs[name] + start, size)]

    def small():
        return remote(pk, pk2.at[g.c], ps, pr, g.Y)

    def span(p):
        return p // per, pl.ds(p % per * PIECE, PIECE)

    def hidden(p):
        s, rows = span(p)
        return remote(hid.at[g.oc * mine + s, rows], xland.at[s, rows], hs.at[p], hr.at[p], g.Y)

    small().start()
    for p in range(pieces):
        hidden(p).start()
    for kind in (0, 2, 1):
        @functools.partial(chunked, nq)
        def _(j):
            qgat.start(kind, j)
    for j in range(no):
        ogat.start(1, j)
    for j in range(2):
        ugat.start(1, j)

    def qkv_phase(xbuf, wbuf, obuf):
        pk2[g.c] = pk[...]
        small().wait_recv()
        gains = [vec('g1', cc, half) for cc in (g.c, g.oc)]
        shifts = [vec('s1', cc, half) for cc in (g.c, g.oc)]
        for p in range(pieces):
            s, rows = span(p)
            loads = [pltpu.make_async_copy(src, xbuf.at[i], ls.at[i]) for i, src in enumerate((hid.at[g.c * mine + s, rows], xland.at[s, rows]))]
            loads[0].start()
            hidden(p).wait_recv()
            loads[1].start()
            for load in loads:
                load.wait()
            sub = 64

            @functools.partial(chunked, PIECE // sub)
            def _(i):
                rows = aligned(i * sub, sub)
                res = norm_rows([xbuf[0, rows, :], xbuf[1, rows, :]], gains, shifts)
                for cc, val in zip((g.c, g.oc), res):
                    ab[aligned(p * PIECE + i * sub, sub), aligned(cc * half, half)] = val

        def load_own(j, act_on):
            for i in range(units):
                for idx, rr in enumerate((g.r, g.rp, g.rx, g.rxp)):
                    src = qland.at[g.c, rr, j * units + i] if idx else wq.at[j * units + i]
                    act_on(pltpu.make_async_copy(src, wbuf.at[0, rr, :, pl.ds(i * LANES, LANES)], ws.at[0, i, idx]))

        def load_other(j, act_on):
            for i in range(units):
                act_on(pltpu.make_async_copy(qland.at[g.oc, :, j * units + i], wbuf.at[1, :, :, pl.ds(i * LANES, LANES)], ws.at[1, i, 0]))

        def save(slot, cc, j):
            return pltpu.make_async_copy(obuf.at[slot], qkv.at[:, aligned((cc * nq + j) * WIDE, WIDE)], st.at[slot])

        def compute(slot, cc, j):
            @pl.when(j > 0)
            def _():
                save(slot, cc, j - 1).wait()

            bias = vec('bq', cc, WIDE, pl.multiple_of(j * WIDE, WIDE))

            def emit(rows, val):
                obuf[slot, rows, :] = (val + bias).astype(BF)

            matmul_rows(ab, wbuf.at[slot], 1024, emit)
            save(slot, cc, j).start()

        @functools.partial(chunked, nq + 3)
        def _(t):
            @pl.when(t < nq)
            def _():
                qgat.relay(t)

            @pl.when(t == nq - 1)
            def _():
                for j in range(no):
                    ogat.start(0, j)

            @pl.when((t >= 1) & (t <= nq))
            def _():
                qgat.push(t - 1)

            @pl.when(t < nq)
            def _():
                qgat.arrive(2, t)
                qgat.arrive(3, t)
                load_own(t, BEGIN)

            @pl.when(t >= 3)
            def _():
                load_other(t - 3, FINISH)
                compute(1, g.oc, t - 3)

            @pl.when((t >= 2) & (t < nq + 2))
            def _():
                qgat.arrive(4, t - 2)
                qgat.arrive(5, t - 2)
                load_other(t - 2, BEGIN)

            @pl.when(t < nq)
            def _():
                load_own(t, FINISH)
                compute(0, g.c, t)

        for slot, cc in enumerate((g.c, g.oc)):
            save(slot, cc, nq - 1).wait()

    pl.run_scoped(
        qkv_phase,
        pltpu.VMEM((2, PIECE, half), BF),
        pltpu.VMEM((2, 4, wq.shape[1], WIDE), BF),
        pltpu.VMEM((2, tokens, WIDE), BF),
    )

    heads = wq.shape[0] // 3

    def attend(ob, abuf, wob, xb):
        def first():
            ogat.relay(0)
            for j in range(no):
                ogat.start(2, j)
            for j in range(nu):
                ugat.start(0, j)
                ugat.start(2, j)

        def second():
            ogat.relay(1)
            for j in range(2, nu):
                ugat.start(1, j)

        events = {0: first, 7: second, 14: lambda: ogat.push(0), 19: lambda: ogat.push(1)}
        for j in range(nu - 2):
            events[20 + 5 * j] = functools.partial(ugat.relay, j)
        steps = mine * 2 * heads

        def block(step, act_on):
            s, h = step // (2 * heads), step % (2 * heads)
            base = (h // heads) * 3 * heads + h % heads
            for i in range(3):
                src = qkv.at[aligned(s * seq, seq), aligned((base + i * heads) * LANES, LANES)]
                act_on(pltpu.make_async_copy(src, abuf.at[step % 2, i], al.at[step % 2, i]))

        block(0, BEGIN)

        @functools.partial(chunked, steps)
        def _(step):
            for at, act in events.items():
                pl.when(step == at)(act)

            @pl.when(step + 1 < steps)
            def _():
                block(step + 1, BEGIN)

            block(step, FINISH)
            s, h = step // (2 * heads), step % (2 * heads)
            attn_head(256, *(abuf.at[step % 2, i] for i in range(3)), ob.at[aligned(s * seq, seq), aligned(h * LANES, LANES)])

        for j in range(no):
            for kind in range(2, 6):
                ogat.arrive(kind, j)
        parts = half // WIDE

        def fetch(i, act_on):
            slot, rel, j = i % 2, i // parts, i % parts
            at = pl.ds(j * WIDE, WIDE)
            copies = shard_loads(g, ogat.own, lambda cc, j: oland.at[cc, :, :, at], ogat.land, wob.at[slot], ws.at[slot, 0], rel, j)
            for s in range(mine):
                src = xland.at[s, :, at] if rel else hid.at[g.c * mine + s, :, at]
                copies.append(pltpu.make_async_copy(src, xb.at[slot, pl.ds(s * seq, seq)], ws.at[slot, 1, s]))
            for copy in copies:
                act_on(copy)

        fetch(0, BEGIN)
        for i in range(2 * parts):
            slot = i % 2
            if i + 1 < 2 * parts:
                fetch(i + 1, BEGIN)
            fetch(i, FINISH)
            cc = g.oc if i >= parts else g.c
            bias = vec('bo', cc, WIDE, i % parts * WIDE)
            at = aligned(cc * half + i % parts * WIDE, WIDE)

            def emit(rows, val):
                hb[rows, at] = (xb[slot, rows, :].astype(F32) + val + bias).astype(BF)

            matmul_rows(ob, wob.at[slot], 512, emit)
            if i < 2:
                ugat.relay(nu - 2 + i)
            if i == 1:
                for j in range(nd):
                    dgat.start(1, j)
                    dgat.start(2, j)
                for j in range(DOWN_X):
                    dgat.start(0, j)

    pl.run_scoped(
        attend,
        pltpu.VMEM((tokens, 2 * heads * LANES), BF),
        pltpu.VMEM((2, 3, seq, LANES), BF),
        pltpu.VMEM((2, 4, wo.shape[0], WIDE), BF),
        pltpu.VMEM((2, tokens, WIDE), BF),
    )

    gains = [vec('g2', cc, half) for cc in range(2)]
    shifts = [vec('s2', cc, half) for cc in range(2)]

    @functools.partial(chunked, tokens // 64)
    def _(i):
        rows = aligned(i * 64, 64)
        ab[rows, :half], ab[rows, half:] = norm_rows([hb[rows, :half], hb[rows, half:]], gains, shifts)

    def mlp(act):
        def load(gat, land, width, wbuf, rel, j, act_on):
            whole = lambda cc, j: land.at[cc, :, :, aligned(j * width, width)]
            for copy in shard_loads(g, gat.own, whole, gat.land, wbuf.at[rel], ws.at[rel, 0], rel, j):
                act_on(copy)

        def up(wbuf):
            fetch = functools.partial(load, ugat, uland, WIDE, wbuf)

            def compute(rel, j):
                cc = g.oc if rel else g.c
                bias = vec('bu', cc, WIDE, pl.multiple_of(j * WIDE, WIDE))
                at = aligned((cc * nu + j) * WIDE, WIDE)

                def emit(rows, val):
                    act[rows, at] = jax.nn.gelu(val + bias, approximate=True).astype(BF)

                fetch(rel, j, FINISH)
                matmul_rows(ab, wbuf.at[rel], 1024, emit)

            def ready(rel, j):
                for kind in ((4, 5) if rel else (2, 3)):
                    ugat.arrive(kind, j)
                fetch(rel, j, BEGIN)

            for j in range(4):
                ugat.push(j)
            for rel in range(2):
                ready(rel, 0)

            @functools.partial(chunked, nu)
            def _(t):
                @pl.when((t >= 1) & (t <= 2))
                def _():
                    for i in range(2):
                        ugat.push(2 + 2 * t + i)

                @pl.when((t == 4) | (t == 6))
                def _():
                    dgat.relay((t - 4) // 2)

                for rel in range(2):
                    compute(rel, t)

                    @pl.when(t + 1 < nu)
                    def _():
                        ready(rel, t + 1)

        pl.run_scoped(up, pltpu.VMEM((2, 4, wu.shape[0], WIDE), BF))

        def down(wbuf):
            fetch = functools.partial(load, dgat, dland, SLIM, wbuf)

            def place(rel, s, j):
                src = ab.at[pl.ds(s * seq, seq), aligned((rel * nd + j) * SLIM, SLIM)]
                dst = out.at[g.c * mine + s, :, aligned(j * SLIM, SLIM)]
                return remote(src, dst, gs.at[s, j], gr.at[s, j], g.Y) if rel else pltpu.make_async_copy(src, dst, ks.at[s, j])

            def compute(rel, j):
                cc = g.oc if rel else g.c
                bias = vec('bd', cc, SLIM, pl.multiple_of(j * SLIM, SLIM))
                fetch(rel, j, FINISH)

                def emit(rows, val):
                    base = hb[rows, aligned(cc * half + j * SLIM, SLIM)].astype(F32)
                    ab[rows, aligned((rel * nd + j) * SLIM, SLIM)] = (base + val + bias).astype(BF)

                matmul_rows(act, wbuf.at[rel], 1024, emit)
                for s in range(mine):
                    place(rel, s, j).start()

            def ready(rel, j):
                for kind in ((4, 5) if rel else (2, 3)):
                    dgat.arrive(kind, j)
                fetch(rel, j, BEGIN)

            def pass_on(j):
                dgat.arrive(1, j)
                dgat.start(4, j)
                dgat.start(6, j)

            @functools.partial(chunked, nd + 1)
            def _(t):
                @pl.when(t < nd)
                def _():
                    dgat.push(t)

                @pl.when(t < DOWN_X)
                def _():
                    ready(0, t)

                @pl.when(t < DOWN_X)
                def _():
                    pass_on(t + DOWN_X)

                @pl.when(t == 1)
                def _():
                    for j in range(DOWN_X, nd):
                        dgat.start(0, j)

                @pl.when(t < nd)
                def _():
                    ready(1, t)
                    compute(1, t)

                @pl.when(t >= nd - 1)
                def _():
                    dgat.arrive(0, t - 1)
                    dgat.start(3, t - 1)
                    ready(0, t - 1)

                @pl.when(t != 2)
                def _():
                    compute(0, jnp.where(t > 2, t - 1, t))

            for s in range(mine):
                for j in range(nd):
                    place(0, s, j).wait()
                    place(1, s, j).wait_send()
                    got = out.at[g.oc * mine + s, :, aligned(j * SLIM, SLIM)]
                    remote(got, got, gs.at[s, j], gr.at[s, j], g.Y).wait_recv()

        pl.run_scoped(down, pltpu.VMEM((2, 4, wd.shape[0], SLIM), BF))

    pl.run_scoped(mlp, pltpu.VMEM((tokens, 2 * wu.shape[1]), BF))
    small().wait_send()
    for p in range(pieces):
        hidden(p).wait_send()
    for gat, count in ((qgat, nq), (ogat, no), (ugat, nu), (dgat, nd)):
        gat.drain(range(7), 0, count)


def layer_call(hidden, packed, wq, wo, wu, wd, offs):
    seqs, seq, half = hidden.shape
    mine = seqs // 2
    tokens = mine * seq
    nq, no, nu, nd = wq.shape[0] * LANES // WIDE, wo.shape[1] // WIDE, wu.shape[1] // WIDE, wd.shape[1] // SLIM
    dma = pltpu.SemaphoreType.DMA
    shape = lambda *dims: jax.ShapeDtypeStruct(dims, BF)
    sems = [dma((7, n)) for n in (nq, no, nu, nd) for _ in 'sr']
    sems += [dma((tokens // PIECE,))] * 2 + [dma, dma, dma((2,)), dma((2, 4, 4)), dma((2,)), dma((2, 3))] + [dma((mine, nd))] * 3
    return pl.pallas_call(
        functools.partial(layer_kernel, offs),
        in_specs=[ANY, pl.BlockSpec(memory_space=pltpu.VMEM)] + [ANY] * 4,
        out_specs=[ANY] * 7,
        out_shape=[shape(*hidden.shape), shape(mine, seq, half), shape(tokens, 2 * wq.shape[0] * LANES)] + [shape(2, 4, *w.shape) for w in (wq, wo, wu, wd)],
        scratch_shapes=[pltpu.VMEM((tokens, 2 * half), BF), pltpu.VMEM((tokens, 2 * half), BF), pltpu.VMEM((2,) + packed.shape, F32)] + sems,
        compiler_params=pltpu.CompilerParams(collective_id=1, has_side_effects=True, vmem_limit_bytes=VMEM_LIMIT),
        name='layer',
    )(hidden, packed, wq, wo, wu, wd)[0]


def solution(mesh):
    act_spec = P(('dp', 'row'), None, 'col')
    arg_specs = (act_spec, P('col'), P('col'), P('row', None, 'col', None), P(None, 'col', None), P('row', None, 'col'), P('col'), P('col'), P('col'), P('row', 'col'), P('col'), P('row', 'col'), P('col'))

    def local_layer(hidden, ln1_gain, ln1_bias, w_qkv, b_qkv, w_out, b_out, ln2_gain, ln2_bias, w_up, b_up, w_down, b_down):
        seqs, _, half = hidden.shape
        heads, size = w_qkv.shape[2], w_qkv.shape[3]
        small = {'g1': ln1_gain, 's1': ln1_bias, 'g2': ln2_gain, 's2': ln2_bias, 'bo': b_out, 'bd': b_down, 'bq': b_qkv, 'bu': b_up}
        offs, at = {}, 0
        for name, a in small.items():
            offs[name], at = at, at + a.size
        packed = jnp.concatenate([a.reshape(-1).astype(F32) for a in small.values()])[None]
        wq = jnp.transpose(w_qkv, (1, 2, 0, 3)).reshape(3 * heads, w_qkv.shape[0], size)
        wo = w_out.reshape(-1, half)
        return layer_call(hidden, packed, wq, wo, w_up, w_down, offs)

    return jax.shard_map(local_layer, mesh=mesh, in_specs=arg_specs, out_specs=act_spec, check_vma=False)
```

```python
import functools

import jax
import jax.numpy as jnp
from jax import lax
from jax.experimental import pallas as pl
from jax.experimental.pallas import tpu as pltpu
from jax.sharding import PartitionSpec as P

LN_EPS = 1e-5
BF = jnp.bfloat16
F32 = jnp.float32
LOG2E = 1.4426950408889634
MESH = pl.DeviceIdType.MESH
ANY = pl.BlockSpec(memory_space=pl.ANY)
VMEM_LIMIT = 63 * 1024 * 1024


class Grid:
    def __init__(self):
        self.c = lax.axis_index('col')
        self.r = lax.axis_index('row')
        self.oc = 1 - self.c
        x = self.r // 2
        k = self.r - 2 * x
        self.rp = 2 * x + 1 - k
        self.rx = 2 * (1 - x) + k
        self.rxp = 2 * (1 - x) + 1 - k
        self.P, self.X, self.Y = {'row': self.rp}, {'row': self.rx}, {'col': self.oc}

    def barrier(self):
        sem = pltpu.get_barrier_semaphore()
        for dev in (self.P, self.X, self.Y):
            pl.semaphore_signal(sem, inc=1, device_id=dev, device_id_type=MESH)
        pl.semaphore_wait(sem, 3)


def remote(src, dst, send, recv, dev):
    return pltpu.make_async_remote_copy(src_ref=src, dst_ref=dst, send_sem=send, recv_sem=recv, device_id=dev, device_id_type=MESH)


class Gather:
    def __init__(self, g, own, land, send, recv, via_x):
        self.g, self.own, self.land, self.send_sem, self.recv_sem, self.via_x = g, own, land, send, recv, via_x

    def desc(self, kind, j, via_x=True):
        g = self.g
        if kind < 3:
            src, dst = self.own(j), self.land(g.c, g.r, j)
            dev = (g.X, g.Y, g.P)[kind]
        else:
            at = {3: (g.c, g.rx), 4: (g.oc, g.r), 5: (g.oc, g.rx), 6: (g.oc, g.r) if via_x else (g.c, g.rx)}[kind]
            src = dst = self.land(*at, j)
            dev = g.P if kind < 6 else (g.X if via_x else g.Y)
        return remote(src, dst, self.send_sem.at[kind, j], self.recv_sem.at[kind, j], dev)

    def routed(self, j, act):
        via = self.via_x(j)
        if isinstance(via, bool):
            act(self.desc(6, j, via))
            return

        @pl.when(via)
        def _():
            act(self.desc(6, j))

        @pl.when(jnp.logical_not(via))
        def _():
            act(self.desc(6, j, False))

    def start(self, kind, j):
        if kind == 6:
            self.routed(j, lambda d: d.start())
        else:
            self.desc(kind, j).start()

    def arrive(self, kind, j):
        g = self.g
        at = [(g.c, g.rx), (g.oc, g.r), (g.c, g.rp), (g.c, g.rxp), (g.oc, g.rp), (g.oc, g.rxp), (g.oc, g.rx)][kind]
        ref = self.land(*at, j)
        remote(ref, ref, self.send_sem.at[kind, j], self.recv_sem.at[kind, j], g.P).wait_recv()

    def drain(self, kinds, lo, hi):
        @functools.partial(chunked, hi - lo)
        def _(i):
            for kind in kinds:
                if kind == 6:
                    self.routed(lo + i, lambda d: d.wait_send())
                else:
                    self.desc(kind, lo + i).wait_send()

    def relay(self, j):
        self.arrive(0, j)
        self.start(3, j)
        self.arrive(1, j)
        self.start(4, j)
        self.start(6, j)

    def push(self, j):
        self.arrive(6, j)
        self.start(5, j)


def chunked(total, body):
    lax.fori_loop(0, total, lambda j, carry: (body(j), carry)[1], 0)


def matmul_rows(a_ref, w_ref, tile, emit):
    depth = w_ref.shape[0] * w_ref.shape[1]

    def body(m):
        rows = pl.ds(pl.multiple_of(m * tile, tile), tile)
        w = w_ref[...].reshape(depth, w_ref.shape[2])
        emit(rows, jnp.dot(a_ref[rows, :], w, preferred_element_type=F32))

    chunked(a_ref.shape[0] // tile, body)


def norm_rows(parts, gains, shifts):
    parts = [p.astype(F32) for p in parts]
    width = sum(p.shape[1] for p in parts)
    mean = sum(jnp.sum(p, axis=1, keepdims=True) for p in parts) / width
    parts = [p - mean for p in parts]
    var = sum(jnp.sum(p * p, axis=1, keepdims=True) for p in parts) / width
    inv = lax.rsqrt(var + LN_EPS)
    return [(p * inv * gn + sh).astype(BF) for p, gn, sh in zip(parts, gains, shifts)]


def columns(own_ref, wland, width):
    def cols(j):
        return pl.ds(pl.multiple_of(j * width, width), width)

    return (lambda j: own_ref.at[:, cols(j)]), (lambda cc, rr, j: wland.at[cc, rr, :, cols(j)])


def shard_loads(g, own, land_all, land, buf, sems, rel, j):
    if rel == 0:
        srcs = [own(j)] + [land(g.c, rr, j) for rr in (g.rp, g.rx, g.rxp)]
        return [pltpu.make_async_copy(s, buf.at[rr], sems.at[i]) for i, (s, rr) in enumerate(zip(srcs, (g.r, g.rp, g.rx, g.rxp)))]
    return [pltpu.make_async_copy(land_all(g.oc, j), buf, sems.at[0])]


def attn_head(block, q_ref, k_ref, v_ref, o_ref):
    seq, size = q_ref.shape
    scale = size ** -0.5 * LOG2E
    tri = lax.broadcasted_iota(jnp.int32, (block, block), 0) >= lax.broadcasted_iota(jnp.int32, (block, block), 1)

    def scores(i):
        q = q_ref[i * block:(i + 1) * block, :]
        dot = lambda k: lax.dot_general(q, k, (((1,), (1,)), ((), ())), preferred_element_type=F32)
        diag = jnp.where(tri, dot(k_ref[i * block:(i + 1) * block, :]), -1e30)
        return [dot(k_ref[:i * block, :]), diag] if i else [diag]

    def probs(parts):
        top = functools.reduce(jnp.maximum, [jnp.max(s, axis=1, keepdims=True) for s in parts])
        parts = [jnp.exp2((s - top) * scale) for s in parts]
        inv = 1.0 / sum(jnp.sum(e, axis=1, keepdims=True) for e in parts)
        return jnp.concatenate([(e * inv).astype(BF) for e in parts], axis=1)

    def finish(i, p):
        o_ref[i * block:(i + 1) * block, :] = jnp.dot(p, v_ref[:(i + 1) * block, :], preferred_element_type=F32).astype(BF)

    count = seq // block
    ahead, before = scores(0), None
    for i in range(count):
        now, ahead = ahead, scores(i + 1) if i + 1 < count else None
        now = probs(now)
        if i:
            finish(i - 1, before)
        before = now
    finish(count - 1, before)


BEGIN, FINISH = (lambda d: d.start()), (lambda d: d.wait())
WIDE, SLIM, LANES, PIECE = 512, 256, 128, 512
DOWN_X = 2


def aligned(start, size):
    return pl.ds(pl.multiple_of(start, size), size)


def layer_kernel(offs, g1, s1, g2, s2, bo, bd, bq, bu, hid, wq, wo, wu, wd, out, xland, qkv, qland, oland, uland, dland, hb, pk, pk2,
                 qs, qr, os, oo, us, ur, ds, dr, hs, hr, ps, pr, ls, ws, st, al, gs, gr, ks):
    g = Grid()
    for ref, start in zip((g1, s1, g2, s2, bo, bd, bq, bu), offs.values()):
        if len(ref.shape) == 1:
            pk[0, pl.ds(start, ref.shape[0])] = ref[...].astype(F32)
            continue
        for i in range(ref.shape[0]):
            for j in range(ref.shape[1]):
                pk[0, pl.ds(start + (i * ref.shape[1] + j) * LANES, LANES)] = ref[i, j, :].astype(F32)
    g.barrier()
    seqs, seq, half = hid.shape
    mine = seqs // 2
    tokens = mine * seq
    units = WIDE // LANES
    qgat = Gather(g, lambda j: wq.at[pl.ds(j * units, units)], lambda cc, rr, j: qland.at[cc, rr, pl.ds(j * units, units)], qs, qr, lambda j: True)
    ogat = Gather(g, *columns(wo, oland, WIDE), os, oo, lambda j: j == 0)
    ugat = Gather(g, *columns(wu, uland, WIDE), us, ur, lambda j: (j % 2 == 0) & (j < 5))
    dgat = Gather(g, *columns(wd, dland, SLIM), ds, dr, lambda j: True)
    nq, no, nu, nd = wq.shape[0] // units, wo.shape[1] // WIDE, wu.shape[1] // WIDE, wd.shape[1] // SLIM
    per = seq // PIECE
    pieces = mine * per

    def vec(name, cc, size, start=0):
        return pk2[cc, :, pl.ds(offs[name] + start, size)]

    def small():
        return remote(pk, pk2.at[g.c], ps, pr, g.Y)

    def span(p):
        return p // per, pl.ds(p % per * PIECE, PIECE)

    def hidden(p):
        s, rows = span(p)
        return remote(hid.at[g.oc * mine + s, rows], xland.at[s, rows], hs.at[p], hr.at[p], g.Y)

    small().start()
    for p in range(pieces):
        hidden(p).start()
    for kind in (0, 2, 1):
        @functools.partial(chunked, nq)
        def _(j):
            qgat.start(kind, j)
    for j in range(no):
        ogat.start(1, j)
    for j in range(2):
        ugat.start(1, j)

    def qkv_phase(xbuf, wbuf, obuf, ab):
        pk2[g.c] = pk[...]
        small().wait_recv()
        gains = [vec('g1', cc, half) for cc in (g.c, g.oc)]
        shifts = [vec('s1', cc, half) for cc in (g.c, g.oc)]
        for p in range(pieces):
            s, rows = span(p)
            loads = [pltpu.make_async_copy(src, xbuf.at[i], ls.at[i]) for i, src in enumerate((hid.at[g.c * mine + s, rows], xland.at[s, rows]))]
            loads[0].start()
            hidden(p).wait_recv()
            loads[1].start()
            for load in loads:
                load.wait()
            sub = 64

            @functools.partial(chunked, PIECE // sub)
            def _(i):
                rows = aligned(i * sub, sub)
                res = norm_rows([xbuf[0, rows, :], xbuf[1, rows, :]], gains, shifts)
                for cc, val in zip((g.c, g.oc), res):
                    ab[aligned(p * PIECE + i * sub, sub), aligned(cc * half, half)] = val

        def load_own(j, act_on):
            for i in range(units):
                for idx, rr in enumerate((g.r, g.rp, g.rx, g.rxp)):
                    src = qland.at[g.c, rr, j * units + i] if idx else wq.at[j * units + i]
                    act_on(pltpu.make_async_copy(src, wbuf.at[0, rr, :, pl.ds(i * LANES, LANES)], ws.at[0, i, idx]))

        def load_other(j, act_on):
            for i in range(units):
                act_on(pltpu.make_async_copy(qland.at[g.oc, :, j * units + i], wbuf.at[1, :, :, pl.ds(i * LANES, LANES)], ws.at[1, i, 0]))

        def save(slot, cc, j):
            return pltpu.make_async_copy(obuf.at[slot], qkv.at[:, aligned((cc * nq + j) * WIDE, WIDE)], st.at[slot])

        def compute(slot, cc, j):
            @pl.when(j > 0)
            def _():
                save(slot, cc, j - 1).wait()

            bias = vec('bq', cc, WIDE, pl.multiple_of(j * WIDE, WIDE))

            def emit(rows, val):
                obuf[slot, rows, :] = (val + bias).astype(BF)

            matmul_rows(ab, wbuf.at[slot], 1024, emit)
            save(slot, cc, j).start()

        @functools.partial(chunked, nq + 3)
        def _(t):
            @pl.when(t < nq)
            def _():
                qgat.relay(t)

            @pl.when(t == nq - 1)
            def _():
                for j in range(no):
                    ogat.start(0, j)

            @pl.when((t >= 1) & (t <= nq))
            def _():
                qgat.push(t - 1)

            @pl.when(t < nq)
            def _():
                qgat.arrive(2, t)
                qgat.arrive(3, t)
                load_own(t, BEGIN)

            @pl.when(t >= 3)
            def _():
                load_other(t - 3, FINISH)
                compute(1, g.oc, t - 3)

            @pl.when((t >= 2) & (t < nq + 2))
            def _():
                qgat.arrive(4, t - 2)
                qgat.arrive(5, t - 2)
                load_other(t - 2, BEGIN)

            @pl.when(t < nq)
            def _():
                load_own(t, FINISH)
                compute(0, g.c, t)

        for slot, cc in enumerate((g.c, g.oc)):
            save(slot, cc, nq - 1).wait()

    pl.run_scoped(
        qkv_phase,
        pltpu.VMEM((2, PIECE, half), BF),
        pltpu.VMEM((2, 4, wq.shape[1], WIDE), BF),
        pltpu.VMEM((2, tokens, WIDE), BF),
        pltpu.VMEM((tokens, 2 * half), BF),
    )

    heads = wq.shape[0] // 3

    def attend(ob, abuf, wob, xb):
        def first():
            ogat.relay(0)
            for j in range(no):
                ogat.start(2, j)
            for j in range(nu):
                ugat.start(0, j)
                ugat.start(2, j)

        def second():
            ogat.relay(1)
            for j in range(2, nu):
                ugat.start(1, j)

        events = {0: first, 9: second, 23: lambda: ogat.push(0), 32: lambda: ogat.push(1)}
        for j, at in enumerate((34, 43)):
            events[at] = functools.partial(ugat.relay, j)
        steps = mine * 2 * heads

        def block(step, act_on):
            s, h = step // (2 * heads), step % (2 * heads)
            base = (h // heads) * 3 * heads + h % heads
            for i in range(3):
                src = qkv.at[aligned(s * seq, seq), aligned((base + i * heads) * LANES, LANES)]
                act_on(pltpu.make_async_copy(src, abuf.at[step % 2, i], al.at[step % 2, i]))

        block(0, BEGIN)

        @functools.partial(chunked, steps)
        def _(step):
            for at, act in events.items():
                pl.when(step == at)(act)

            @pl.when(step + 1 < steps)
            def _():
                block(step + 1, BEGIN)

            block(step, FINISH)
            s, h = step // (2 * heads), step % (2 * heads)
            attn_head(256, *(abuf.at[step % 2, i] for i in range(3)), ob.at[aligned(s * seq, seq), aligned(h * LANES, LANES)])

        for j in range(no):
            for kind in range(2, 6):
                ogat.arrive(kind, j)
        parts = half // WIDE

        def fetch(i, act_on):
            slot, rel, j = i % 2, i // parts, i % parts
            at = pl.ds(j * WIDE, WIDE)
            copies = shard_loads(g, ogat.own, lambda cc, j: oland.at[cc, :, :, at], ogat.land, wob.at[slot], ws.at[slot, 0], rel, j)
            for s in range(mine):
                src = xland.at[s, :, at] if rel else hid.at[g.c * mine + s, :, at]
                copies.append(pltpu.make_async_copy(src, xb.at[slot, pl.ds(s * seq, seq)], ws.at[slot, 1, s]))
            for copy in copies:
                act_on(copy)

        fetch(0, BEGIN)
        for i in range(2 * parts):
            slot = i % 2
            if i + 1 < 2 * parts:
                fetch(i + 1, BEGIN)
            fetch(i, FINISH)
            cc = g.oc if i >= parts else g.c
            bias = vec('bo', cc, WIDE, i % parts * WIDE)
            at = aligned(cc * half + i % parts * WIDE, WIDE)

            def emit(rows, val):
                hb[rows, at] = (xb[slot, rows, :].astype(F32) + val + bias).astype(BF)

            matmul_rows(ob, wob.at[slot], 512, emit)
            ugat.relay(2 + i)

    pl.run_scoped(
        attend,
        pltpu.VMEM((tokens, 2 * heads * LANES), BF),
        pltpu.VMEM((2, 3, seq, LANES), BF),
        pltpu.VMEM((2, 4, wo.shape[0], WIDE), BF),
        pltpu.VMEM((2, tokens, WIDE), BF),
    )

    def mlp(act):
        def load(gat, land, width, wbuf, rel, j, act_on):
            whole = lambda cc, j: land.at[cc, :, :, aligned(j * width, width)]
            for copy in shard_loads(g, gat.own, whole, gat.land, wbuf.at[rel], ws.at[rel, 0], rel, j):
                act_on(copy)

        def up(wbuf, ab):
            gains = [vec('g2', cc, half) for cc in range(2)]
            shifts = [vec('s2', cc, half) for cc in range(2)]

            @functools.partial(chunked, tokens // 64)
            def _(i):
                rows = aligned(i * 64, 64)
                ab[rows, :half], ab[rows, half:] = norm_rows([hb[rows, :half], hb[rows, half:]], gains, shifts)

            fetch = functools.partial(load, ugat, uland, WIDE, wbuf)

            def compute(rel, j):
                cc = g.oc if rel else g.c
                bias = vec('bu', cc, WIDE, pl.multiple_of(j * WIDE, WIDE))
                at = aligned((cc * nu + j) * WIDE, WIDE)

                def emit(rows, val):
                    act[rows, at] = jax.nn.gelu(val + bias, approximate=True).astype(BF)

                fetch(rel, j, FINISH)
                matmul_rows(ab, wbuf.at[rel], 1024, emit)

            def ready(rel, j):
                for kind in ((4, 5) if rel else (2, 3)):
                    ugat.arrive(kind, j)
                fetch(rel, j, BEGIN)

            ugat.relay(nu - 2)
            ready(0, 0)

            @functools.partial(chunked, nu + 1)
            def _(t):
                @pl.when(t < nu)
                def _():
                    compute(0, t)

                @pl.when(t == 0)
                def _():
                    ugat.relay(nu - 1)
                    for j in range(nd):
                        dgat.start(1, j)
                        dgat.start(2, j)
                    for j in range(DOWN_X):
                        dgat.start(0, j)

                @pl.when(t + 1 < nu)
                def _():
                    ready(0, t + 1)

                @pl.when((t >= 1) & (t <= nu // 2))
                def _():
                    ugat.push(2 * t - 2)
                    ugat.push(2 * t - 1)

                @pl.when(t == 1)
                def _():
                    ready(1, 0)

                @pl.when((t == 6) | (t == 8))
                def _():
                    dgat.relay((t - 6) // 2)

                @pl.when(t >= 1)
                def _():
                    compute(1, t - 1)

                @pl.when((t >= 1) & (t < nu))
                def _():
                    ready(1, t)

        pl.run_scoped(up, pltpu.VMEM((2, 4, wu.shape[0], WIDE), BF), pltpu.VMEM((tokens, 2 * half), BF))

        def down(wbuf, acc):
            depth = wd.shape[0]
            fetch = functools.partial(load, dgat, dland, SLIM, wbuf, 1)

            def spot(rel, j):
                return aligned((g.oc if rel else g.c) * half + j * SLIM, SLIM)

            def place(rel, s, j):
                src = hb.at[pl.ds(s * seq, seq), spot(rel, j)]
                dst = out.at[g.c * mine + s, :, aligned(j * SLIM, SLIM)]
                return remote(src, dst, gs.at[s, j], gr.at[s, j], g.Y) if rel else pltpu.make_async_copy(src, dst, ks.at[s, j])

            def finish(rel, j):
                cc = g.oc if rel else g.c
                bias = vec('bd', cc, SLIM, pl.multiple_of(j * SLIM, SLIM))

                def emit(rows, val):
                    hb[rows, spot(rel, j)] = (hb[rows, spot(rel, j)].astype(F32) + val + bias).astype(BF)

                return emit

            def send(rel, j):
                for s in range(mine):
                    place(rel, s, j).start()

            def other(j):
                fetch(j, FINISH)
                matmul_rows(act, wbuf.at[1], 1024, finish(1, j))
                send(1, j)

            def shard(rr, j, act_on):
                src = dland.at[g.c, rr, :, aligned(j * SLIM, SLIM)]
                act_on(pltpu.make_async_copy(src, wbuf.at[0, rr], ws.at[0, 1, rr]))

            def mine_shard(j, act_on):
                act_on(pltpu.make_async_copy(dgat.own(j), wbuf.at[0, g.r], ws.at[0, 1, g.r]))
                shard(g.rp, j, act_on)

            def product(rr, count, emit):
                matmul_rows(act.at[:, aligned(rr * depth, count * depth)], wbuf.at[0, pl.ds(rr, count)], 1024, emit)

            def near(j):
                mine_shard(j, FINISH)

                def emit(rows, val):
                    acc[rows, :] = val

                product(g.r // 2 * 2, 2, emit)

                @pl.when(j + 1 < nd)
                def _():
                    dgat.arrive(2, j + 1)
                    mine_shard(j + 1, BEGIN)

            def far(j):
                @pl.when(j >= DOWN_X)
                def _():
                    dgat.arrive(0, j)
                    dgat.start(3, j)

                shard(g.rx, j, BEGIN)
                shard(g.rx, j, FINISH)

                def emit(rows, val):
                    acc[rows, :] += val

                dgat.arrive(3, j)
                shard(g.rxp, j, BEGIN)
                product(g.rx, 1, emit)
                shard(g.rxp, j, FINISH)
                last = finish(0, j)
                product(g.rxp, 1, lambda rows, val: last(rows, acc[rows, :] + val))
                send(0, j)

            def pass_on(j):
                dgat.arrive(1, j)
                dgat.start(4, j)
                dgat.start(6, j)

            dgat.arrive(2, 0)
            mine_shard(0, BEGIN)

            @functools.partial(chunked, nd + 1)
            def _(t):
                @pl.when(t < nd)
                def _():
                    dgat.push(t)

                @pl.when(t < DOWN_X)
                def _():
                    pass_on(t + DOWN_X)

                @pl.when(t == 1)
                def _():
                    for j in range(DOWN_X, nd):
                        dgat.start(0, j)

                @pl.when(t < nd)
                def _():
                    for kind in (4, 5):
                        dgat.arrive(kind, t)
                    fetch(t, BEGIN)
                    other(t)

                @pl.when(t <= DOWN_X)
                def _():
                    near(t)

                @pl.when(t != DOWN_X)
                def _():
                    far(jnp.where(t > DOWN_X, t - 1, t))

                @pl.when(t == nd - 1)
                def _():
                    near(nd - 1)

            for s in range(mine):
                for j in range(nd):
                    place(0, s, j).wait()
                    place(1, s, j).wait_send()
                    got = out.at[g.oc * mine + s, :, aligned(j * SLIM, SLIM)]
                    remote(got, got, gs.at[s, j], gr.at[s, j], g.Y).wait_recv()

        pl.run_scoped(down, pltpu.VMEM((2, 4, wd.shape[0], SLIM), BF), pltpu.VMEM((tokens, SLIM), F32))

    pl.run_scoped(mlp, pltpu.VMEM((tokens, 2 * wu.shape[1]), BF))
    small().wait_send()
    for p in range(pieces):
        hidden(p).wait_send()
    for gat, count in ((qgat, nq), (ogat, no), (ugat, nu), (dgat, nd)):
        gat.drain(range(7), 0, count)


def layer_call(small, hidden, wq, wo, wu, wd, offs):
    seqs, seq, half = hidden.shape
    mine = seqs // 2
    tokens = mine * seq
    nq, no, nu, nd = wq.shape[0] * LANES // WIDE, wo.shape[1] // WIDE, wu.shape[1] // WIDE, wd.shape[1] // SLIM
    total = sum(a.size for a in small)
    dma = pltpu.SemaphoreType.DMA
    shape = lambda *dims: jax.ShapeDtypeStruct(dims, BF)
    sems = [dma((7, n)) for n in (nq, no, nu, nd) for _ in 'sr']
    sems += [dma((tokens // PIECE,))] * 2 + [dma, dma, dma((2,)), dma((2, 4, 4)), dma((2,)), dma((2, 3))] + [dma((mine, nd))] * 3
    return pl.pallas_call(
        functools.partial(layer_kernel, offs),
        in_specs=[pl.BlockSpec(memory_space=pltpu.VMEM)] * len(small) + [ANY] * 5,
        out_specs=[ANY] * 7,
        out_shape=[shape(*hidden.shape), shape(mine, seq, half), shape(tokens, 2 * wq.shape[0] * LANES)] + [shape(2, 4, *w.shape) for w in (wq, wo, wu, wd)],
        scratch_shapes=[pltpu.VMEM((tokens, 2 * half), BF), pltpu.VMEM((1, total), F32), pltpu.VMEM((2, 1, total), F32)] + sems,
        compiler_params=pltpu.CompilerParams(collective_id=1, has_side_effects=True, vmem_limit_bytes=VMEM_LIMIT),
        name='layer',
    )(*small, hidden, wq, wo, wu, wd)[0]


def solution(mesh):
    act_spec = P(('dp', 'row'), None, 'col')
    arg_specs = (act_spec, P('col'), P('col'), P('row', None, 'col', None), P(None, 'col', None), P('row', None, 'col'), P('col'), P('col'), P('col'), P('row', 'col'), P('col'), P('row', 'col'), P('col'))

    def local_layer(hidden, ln1_gain, ln1_bias, w_qkv, b_qkv, w_out, b_out, ln2_gain, ln2_bias, w_up, b_up, w_down, b_down):
        seqs, _, half = hidden.shape
        heads, size = w_qkv.shape[2], w_qkv.shape[3]
        small = {'g1': ln1_gain, 's1': ln1_bias, 'g2': ln2_gain, 's2': ln2_bias, 'bo': b_out, 'bd': b_down, 'bq': b_qkv, 'bu': b_up}
        offs, at = {}, 0
        for name, a in small.items():
            offs[name], at = at, at + a.size
        wq = jnp.transpose(w_qkv, (1, 2, 0, 3)).reshape(3 * heads, w_qkv.shape[0], size)
        wo = w_out.reshape(-1, half)
        return layer_call(list(small.values()), hidden, wq, wo, w_up, w_down, offs)

    return jax.shard_map(local_layer, mesh=mesh, in_specs=arg_specs, out_specs=act_spec, check_vma=False)
```

```python
import functools

import jax
import jax.numpy as jnp
from jax import lax
from jax.experimental import pallas as pl
from jax.experimental.pallas import tpu as pltpu
from jax.sharding import PartitionSpec as P

LN_EPS = 1e-5
BF = jnp.bfloat16
F32 = jnp.float32
LOG2E = 1.4426950408889634
MESH = pl.DeviceIdType.MESH
ANY = pl.BlockSpec(memory_space=pl.ANY)
VMEM_LIMIT = 63 * 1024 * 1024


class Grid:
    def __init__(self):
        self.c = lax.axis_index('col')
        self.r = lax.axis_index('row')
        self.oc = 1 - self.c
        x = self.r // 2
        k = self.r - 2 * x
        self.rp = 2 * x + 1 - k
        self.rx = 2 * (1 - x) + k
        self.rxp = 2 * (1 - x) + 1 - k
        self.P, self.X, self.Y = {'row': self.rp}, {'row': self.rx}, {'col': self.oc}

    def barrier(self):
        sem = pltpu.get_barrier_semaphore()
        for dev in (self.P, self.X, self.Y):
            pl.semaphore_signal(sem, inc=1, device_id=dev, device_id_type=MESH)
        pl.semaphore_wait(sem, 3)


def remote(src, dst, send, recv, dev):
    return pltpu.make_async_remote_copy(src_ref=src, dst_ref=dst, send_sem=send, recv_sem=recv, device_id=dev, device_id_type=MESH)


class Gather:
    def __init__(self, g, own, land, send, recv, via_x, split=None):
        self.split = split
        self.g, self.own, self.land, self.send_sem, self.recv_sem, self.via_x = g, own, land, send, recv, via_x

    def desc(self, kind, j, via_x=True):
        g = self.g
        if kind < 3:
            src, dst = self.own(j), self.land(g.c, g.r, j)
            dev = (g.X, g.Y, g.P)[kind]
        else:
            at = {3: (g.c, g.rx), 4: (g.oc, g.r), 5: (g.oc, g.rx), 6: (g.oc, g.r) if via_x else (g.c, g.rx)}[kind]
            src = dst = self.land(*at, j)
            dev = g.P if kind < 6 else (g.X if via_x else g.Y)
        return remote(src, dst, self.send_sem.at[kind, j], self.recv_sem.at[kind, j], dev)

    def routed(self, j, act):
        via = self.via_x(j)
        if isinstance(via, bool) and self.split is None:
            act(self.desc(6, j, via))
            return

        @pl.when(via)
        def _():
            act(self.desc(6, j))

        @pl.when(jnp.logical_not(via) & (j != self.split[0]) if self.split else jnp.logical_not(via))
        def _():
            act(self.desc(6, j, False))

        if self.split:
            @pl.when(j == self.split[0])
            def _():
                for copy in self.shares():
                    act(copy)

    def shares(self, arriving=False):
        g, (j, rows, sems) = self.g, self.split
        copies = []
        for i, dev in enumerate((g.X, g.Y)):
            cut = pl.ds(0, rows) if i == 0 else pl.ds(rows, self.own(j).shape[0] - rows)
            at = (g.oc, g.rx) if arriving else ((g.oc, g.r) if i == 0 else (g.c, g.rx))
            ref = self.land(*at, j).at[cut]
            copies.append(remote(ref, ref, sems.at[0, i], sems.at[1, i], dev))
        return copies

    def start(self, kind, j):
        if kind == 6:
            self.routed(j, lambda d: d.start())
        else:
            self.desc(kind, j).start()

    def arrive(self, kind, j):
        g = self.g
        at = [(g.c, g.rx), (g.oc, g.r), (g.c, g.rp), (g.c, g.rxp), (g.oc, g.rp), (g.oc, g.rxp), (g.oc, g.rx)][kind]
        ref = self.land(*at, j)
        copy = remote(ref, ref, self.send_sem.at[kind, j], self.recv_sem.at[kind, j], g.P)
        if kind < 6 or not self.split:
            copy.wait_recv()
            return

        @pl.when(j != self.split[0])
        def _():
            copy.wait_recv()

        @pl.when(j == self.split[0])
        def _():
            for part in self.shares(True):
                part.wait_recv()

    def drain(self, kinds, lo, hi):
        @functools.partial(chunked, hi - lo)
        def _(i):
            for kind in kinds:
                if kind == 6:
                    self.routed(lo + i, lambda d: d.wait_send())
                else:
                    self.desc(kind, lo + i).wait_send()

    def relay(self, j):
        self.arrive(0, j)
        self.start(3, j)
        self.arrive(1, j)
        self.start(4, j)
        self.start(6, j)

    def push(self, j):
        self.arrive(6, j)
        self.start(5, j)


def chunked(total, body):
    lax.fori_loop(0, total, lambda j, carry: (body(j), carry)[1], 0)


def matmul_rows(a_ref, w_ref, tile, emit):
    depth = w_ref.shape[0] * w_ref.shape[1]

    def body(m):
        rows = pl.ds(pl.multiple_of(m * tile, tile), tile)
        w = w_ref[...].reshape(depth, w_ref.shape[2])
        emit(rows, jnp.dot(a_ref[rows, :], w, preferred_element_type=F32))

    chunked(a_ref.shape[0] // tile, body)


def norm_rows(parts, gains, shifts):
    parts = [p.astype(F32) for p in parts]
    width = sum(p.shape[1] for p in parts)
    mean = sum(jnp.sum(p, axis=1, keepdims=True) for p in parts) / width
    parts = [p - mean for p in parts]
    var = sum(jnp.sum(p * p, axis=1, keepdims=True) for p in parts) / width
    inv = lax.rsqrt(var + LN_EPS)
    return [(p * inv * gn + sh).astype(BF) for p, gn, sh in zip(parts, gains, shifts)]


def columns(own_ref, wland, width):
    def cols(j):
        return pl.ds(pl.multiple_of(j * width, width), width)

    return (lambda j: own_ref.at[:, cols(j)]), (lambda cc, rr, j: wland.at[cc, rr, :, cols(j)])


def shard_loads(g, own, land_all, land, buf, sems, rel, j):
    if rel == 0:
        srcs = [own(j)] + [land(g.c, rr, j) for rr in (g.rp, g.rx, g.rxp)]
        return [pltpu.make_async_copy(s, buf.at[rr], sems.at[i]) for i, (s, rr) in enumerate(zip(srcs, (g.r, g.rp, g.rx, g.rxp)))]
    return [pltpu.make_async_copy(land_all(g.oc, j), buf, sems.at[0])]


def attn_head(block, q_ref, k_ref, v_ref, o_ref):
    seq, size = q_ref.shape
    scale = size ** -0.5 * LOG2E
    tri = lax.broadcasted_iota(jnp.int32, (block, block), 0) >= lax.broadcasted_iota(jnp.int32, (block, block), 1)

    def scores(i):
        q = q_ref[i * block:(i + 1) * block, :]
        dot = lambda k: lax.dot_general(q, k, (((1,), (1,)), ((), ())), preferred_element_type=F32)
        diag = jnp.where(tri, dot(k_ref[i * block:(i + 1) * block, :]), -1e30)
        return [dot(k_ref[:i * block, :]), diag] if i else [diag]

    def probs(parts):
        top = functools.reduce(jnp.maximum, [jnp.max(s, axis=1, keepdims=True) for s in parts])
        parts = [jnp.exp2((s - top) * scale) for s in parts]
        inv = 1.0 / sum(jnp.sum(e, axis=1, keepdims=True) for e in parts)
        return jnp.concatenate([(e * inv).astype(BF) for e in parts], axis=1)

    def finish(i, p):
        o_ref[i * block:(i + 1) * block, :] = jnp.dot(p, v_ref[:(i + 1) * block, :], preferred_element_type=F32).astype(BF)

    count = seq // block
    ahead, before = scores(0), None
    for i in range(count):
        now, ahead = ahead, scores(i + 1) if i + 1 < count else None
        now = probs(now)
        if i:
            finish(i - 1, before)
        before = now
    finish(count - 1, before)


BEGIN, FINISH = (lambda d: d.start()), (lambda d: d.wait())
WIDE, SLIM, LANES, PIECE = 512, 256, 128, 512
DOWN_X, EARLY, SHARE = 2, 4, 128


def aligned(start, size):
    return pl.ds(pl.multiple_of(start, size), size)


def layer_kernel(offs, g1, s1, g2, s2, bo, bd, bq, bu, hid, wq, wo, wu, wd, out, xland, qkv, qland, oland, uland, dland, hb, pk, pk2,
                 qs, qr, os, oo, us, ur, ds, dr, hs, hr, ts, tr, vs, ps, pr, ls, ws, st, al, gs, gr, ks):
    g = Grid()
    g.barrier()
    seqs, seq, half = hid.shape
    mine = seqs // 2
    tokens = mine * seq
    units = WIDE // LANES
    qgat = Gather(g, lambda j: wq.at[pl.ds(j * units, units)], lambda cc, rr, j: qland.at[cc, rr, pl.ds(j * units, units)], qs, qr, lambda j: True)
    ogat = Gather(g, *columns(wo, oland, WIDE), os, oo, lambda j: j == 0)
    ugat = Gather(g, *columns(wu, uland, WIDE), us, ur, lambda j: j >= 5, (4, SHARE, vs))
    dgat = Gather(g, *columns(wd, dland, SLIM), ds, dr, lambda j: True)
    deep = wd.shape[0] // 2
    cut = lambda j: (pl.ds(j % 2 * deep, deep), aligned((DOWN_X + j // 2) * SLIM, SLIM))
    tgat = Gather(g, lambda j: wd.at[cut(j)], lambda cc, rr, j: dland.at[(cc, rr) + cut(j)], ts, tr, None)
    nq, no, nu, nd = wq.shape[0] // units, wo.shape[1] // WIDE, wu.shape[1] // WIDE, wd.shape[1] // SLIM
    per = seq // PIECE
    pieces = mine * per

    def vec(name, cc, size, start=0):
        return pk2[cc, :, pl.ds(offs[name] + start, size)]

    def small():
        return remote(pk, pk2.at[g.c], ps, pr, g.Y)

    def span(p):
        return p // per, pl.ds(p % per * PIECE, PIECE)

    def hidden(p):
        s, rows = span(p)
        return remote(hid.at[g.oc * mine + s, rows], xland.at[s, rows], hs.at[p], hr.at[p], g.Y)

    hidden(0).start()

    @functools.partial(chunked, nq)
    def _(j):
        qgat.start(0, j)

    ogat.start(0, 0)
    for ref, start in zip((g1, s1, g2, s2, bo, bd, bq, bu), offs.values()):
        if len(ref.shape) == 1:
            pk[0, pl.ds(start, ref.shape[0])] = ref[...].astype(F32)
            continue
        for i in range(ref.shape[0]):
            for j in range(ref.shape[1]):
                pk[0, pl.ds(start + (i * ref.shape[1] + j) * LANES, LANES)] = ref[i, j, :].astype(F32)
    small().start()
    for p in range(1, pieces):
        hidden(p).start()
    for kind in (2, 1):
        @functools.partial(chunked, nq)
        def _(j):
            qgat.start(kind, j)
    for j in range(no):
        ogat.start(1, j)
    for j in range(EARLY):
        ugat.start(1, j)

    def qkv_phase(xbuf, wbuf, obuf, ab):
        pk2[g.c] = pk[...]
        small().wait_recv()
        gains = [vec('g1', cc, half) for cc in (g.c, g.oc)]
        shifts = [vec('s1', cc, half) for cc in (g.c, g.oc)]
        for p in range(pieces):
            s, rows = span(p)
            loads = [pltpu.make_async_copy(src, xbuf.at[i], ls.at[i]) for i, src in enumerate((hid.at[g.c * mine + s, rows], xland.at[s, rows]))]
            loads[0].start()
            hidden(p).wait_recv()
            loads[1].start()
            for load in loads:
                load.wait()
            sub = 64

            @functools.partial(chunked, PIECE // sub)
            def _(i):
                rows = aligned(i * sub, sub)
                res = norm_rows([xbuf[0, rows, :], xbuf[1, rows, :]], gains, shifts)
                for cc, val in zip((g.c, g.oc), res):
                    ab[aligned(p * PIECE + i * sub, sub), aligned(cc * half, half)] = val

        def load_own(j, act_on):
            for i in range(units):
                for idx, rr in enumerate((g.r, g.rp, g.rx, g.rxp)):
                    src = qland.at[g.c, rr, j * units + i] if idx else wq.at[j * units + i]
                    act_on(pltpu.make_async_copy(src, wbuf.at[0, rr, :, pl.ds(i * LANES, LANES)], ws.at[0, i, idx]))

        def load_other(j, act_on):
            for i in range(units):
                act_on(pltpu.make_async_copy(qland.at[g.oc, :, j * units + i], wbuf.at[1, :, :, pl.ds(i * LANES, LANES)], ws.at[1, i, 0]))

        def save(slot, cc, j):
            return pltpu.make_async_copy(obuf.at[slot], qkv.at[:, aligned((cc * nq + j) * WIDE, WIDE)], st.at[slot])

        def compute(slot, cc, j):
            @pl.when(j > 0)
            def _():
                save(slot, cc, j - 1).wait()

            bias = vec('bq', cc, WIDE, pl.multiple_of(j * WIDE, WIDE))

            def emit(rows, val):
                obuf[slot, rows, :] = (val + bias).astype(BF)

            matmul_rows(ab, wbuf.at[slot], 1024, emit)
            save(slot, cc, j).start()

        @functools.partial(chunked, nq + 3)
        def _(t):
            @pl.when(t < nq)
            def _():
                qgat.relay(t)

            @pl.when(t == nq - 1)
            def _():
                for j in range(1, no):
                    ogat.start(0, j)
                for j in range(2):
                    ugat.start(0, j)

            @pl.when((t >= 1) & (t <= nq))
            def _():
                qgat.push(t - 1)

            @pl.when(t < nq)
            def _():
                qgat.arrive(2, t)
                qgat.arrive(3, t)
                load_own(t, BEGIN)

            @pl.when(t >= 3)
            def _():
                load_other(t - 3, FINISH)
                compute(1, g.oc, t - 3)

            @pl.when((t >= 2) & (t < nq + 2))
            def _():
                qgat.arrive(4, t - 2)
                qgat.arrive(5, t - 2)
                load_other(t - 2, BEGIN)

            @pl.when(t < nq)
            def _():
                load_own(t, FINISH)
                compute(0, g.c, t)

        for slot, cc in enumerate((g.c, g.oc)):
            save(slot, cc, nq - 1).wait()

    pl.run_scoped(
        qkv_phase,
        pltpu.VMEM((2, PIECE, half), BF),
        pltpu.VMEM((2, 4, wq.shape[1], WIDE), BF),
        pltpu.VMEM((2, tokens, WIDE), BF),
        pltpu.VMEM((tokens, 2 * half), BF),
    )

    heads = wq.shape[0] // 3

    def attend(ob, abuf, wob, xb):
        def first():
            for j in range(no):
                ogat.start(2, j)
                ogat.relay(j)
            for j in range(nu):
                ugat.start(2, j)
            for j in range(2, nu):
                ugat.start(0, j)
            for j in range(EARLY, nu):
                ugat.start(1, j)

        events = {0: first, 34: lambda: ogat.push(0), 46: lambda: ogat.push(1)}
        for j, at in enumerate((10, 18)):
            events[at] = functools.partial(ugat.relay, j)
        steps = mine * 2 * heads

        def block(step, act_on):
            s, h = step // (2 * heads), step % (2 * heads)
            base = (h // heads) * 3 * heads + h % heads
            for i in range(3):
                src = qkv.at[aligned(s * seq, seq), aligned((base + i * heads) * LANES, LANES)]
                act_on(pltpu.make_async_copy(src, abuf.at[step % 2, i], al.at[step % 2, i]))

        block(0, BEGIN)

        @functools.partial(chunked, steps)
        def _(step):
            for at, act in events.items():
                pl.when(step == at)(act)

            @pl.when(step + 1 < steps)
            def _():
                block(step + 1, BEGIN)

            block(step, FINISH)
            s, h = step // (2 * heads), step % (2 * heads)
            attn_head(256, *(abuf.at[step % 2, i] for i in range(3)), ob.at[aligned(s * seq, seq), aligned(h * LANES, LANES)])

        for j in range(no):
            for kind in range(2, 6):
                ogat.arrive(kind, j)
        parts = half // WIDE

        def fetch(i, act_on):
            slot, rel, j = i % 2, i // parts, i % parts
            at = pl.ds(j * WIDE, WIDE)
            copies = shard_loads(g, ogat.own, lambda cc, j: oland.at[cc, :, :, at], ogat.land, wob.at[slot], ws.at[slot, 0], rel, j)
            for s in range(mine):
                src = xland.at[s, :, at] if rel else hid.at[g.c * mine + s, :, at]
                copies.append(pltpu.make_async_copy(src, xb.at[slot, pl.ds(s * seq, seq)], ws.at[slot, 1, s]))
            for copy in copies:
                act_on(copy)

        fetch(0, BEGIN)
        for i in range(2 * parts):
            slot = i % 2
            if i + 1 < 2 * parts:
                fetch(i + 1, BEGIN)
            fetch(i, FINISH)
            cc = g.oc if i >= parts else g.c
            bias = vec('bo', cc, WIDE, i % parts * WIDE)
            at = aligned(cc * half + i % parts * WIDE, WIDE)

            def emit(rows, val):
                hb[rows, at] = (xb[slot, rows, :].astype(F32) + val + bias).astype(BF)

            matmul_rows(ob, wob.at[slot], 512, emit)
            ugat.relay(2 + i)

    pl.run_scoped(
        attend,
        pltpu.VMEM((tokens, 2 * heads * LANES), BF),
        pltpu.VMEM((2, 3, seq, LANES), BF),
        pltpu.VMEM((2, 4, wo.shape[0], WIDE), BF),
        pltpu.VMEM((2, tokens, WIDE), BF),
    )

    def mlp(act):
        def load(gat, land, width, wbuf, rel, j, act_on):
            whole = lambda cc, j: land.at[cc, :, :, aligned(j * width, width)]
            for copy in shard_loads(g, gat.own, whole, gat.land, wbuf.at[rel], ws.at[rel, 0], rel, j):
                act_on(copy)

        def up(wbuf, ab):
            gains = [vec('g2', cc, half) for cc in range(2)]
            shifts = [vec('s2', cc, half) for cc in range(2)]

            @functools.partial(chunked, tokens // 64)
            def _(i):
                rows = aligned(i * 64, 64)
                ab[rows, :half], ab[rows, half:] = norm_rows([hb[rows, :half], hb[rows, half:]], gains, shifts)

            fetch = functools.partial(load, ugat, uland, WIDE, wbuf)

            def compute(rel, j):
                cc = g.oc if rel else g.c
                bias = vec('bu', cc, WIDE, pl.multiple_of(j * WIDE, WIDE))
                at = aligned((cc * nu + j) * WIDE, WIDE)

                def emit(rows, val):
                    act[rows, at] = jax.nn.gelu(val + bias, approximate=True).astype(BF)

                fetch(rel, j, FINISH)
                matmul_rows(ab, wbuf.at[rel], 1024, emit)

            def ready(rel, j):
                for kind in ((4, 5) if rel else (2, 3)):
                    ugat.arrive(kind, j)
                fetch(rel, j, BEGIN)

            ugat.relay(nu - 2)
            ready(0, 0)

            @functools.partial(chunked, nu + 1)
            def _(t):
                @pl.when(t < nu)
                def _():
                    compute(0, t)

                @pl.when(t == 0)
                def _():
                    ugat.push(0)
                    ugat.relay(nu - 1)
                    for j in range(nd):
                        dgat.start(1, j)
                        dgat.start(2, j)
                    for j in range(DOWN_X):
                        dgat.start(0, j)

                @pl.when(t + 1 < nu)
                def _():
                    ready(0, t + 1)

                @pl.when((t >= 1) & (t < nu))
                def _():
                    ugat.push(t)

                @pl.when(t == 1)
                def _():
                    ready(1, 0)

                @pl.when((t == 6) | (t == 8))
                def _():
                    dgat.relay((t - 6) // 2)

                @pl.when(t >= 1)
                def _():
                    compute(1, t - 1)

                @pl.when((t >= 1) & (t < nu))
                def _():
                    ready(1, t)

        pl.run_scoped(up, pltpu.VMEM((2, 4, wu.shape[0], WIDE), BF), pltpu.VMEM((tokens, 2 * half), BF))

        def down(wbuf, acc):
            depth = wd.shape[0]
            fetch = functools.partial(load, dgat, dland, SLIM, wbuf, 1)

            def spot(rel, j):
                return aligned((g.oc if rel else g.c) * half + j * SLIM, SLIM)

            def place(rel, s, j):
                src = hb.at[pl.ds(s * seq, seq), spot(rel, j)]
                dst = out.at[g.c * mine + s, :, aligned(j * SLIM, SLIM)]
                return remote(src, dst, gs.at[s, j], gr.at[s, j], g.Y) if rel else pltpu.make_async_copy(src, dst, ks.at[s, j])

            def finish(rel, j):
                cc = g.oc if rel else g.c
                bias = vec('bd', cc, SLIM, pl.multiple_of(j * SLIM, SLIM))

                def emit(rows, val):
                    hb[rows, spot(rel, j)] = (hb[rows, spot(rel, j)].astype(F32) + val + bias).astype(BF)

                return emit

            def send(rel, j):
                for s in range(mine):
                    place(rel, s, j).start()

            def other(j):
                fetch(j, FINISH)
                matmul_rows(act, wbuf.at[1], 1024, finish(1, j))
                send(1, j)

            def shard(rr, j, act_on):
                src = dland.at[g.c, rr, :, aligned(j * SLIM, SLIM)]
                act_on(pltpu.make_async_copy(src, wbuf.at[0, rr], ws.at[0, 1, rr]))

            def mine_shard(j, act_on):
                act_on(pltpu.make_async_copy(dgat.own(j), wbuf.at[0, g.r], ws.at[0, 1, g.r]))
                shard(g.rp, j, act_on)

            def product(rr, count, emit):
                matmul_rows(act.at[:, aligned(rr * depth, count * depth)], wbuf.at[0, pl.ds(rr, count)], 1024, emit)

            def near(j):
                mine_shard(j, FINISH)

                def emit(rows, val):
                    acc[rows, :] = val

                product(g.r // 2 * 2, 2, emit)

                @pl.when(j + 1 < nd)
                def _():
                    dgat.arrive(2, j + 1)
                    mine_shard(j + 1, BEGIN)

            def add(rows, val):
                acc[rows, :] += val

            def far(j):
                shard(g.rx, j, BEGIN)
                dgat.arrive(3, j)
                shard(g.rxp, j, BEGIN)
                shard(g.rx, j, FINISH)
                product(g.rx, 1, add)
                shard(g.rxp, j, FINISH)
                last = finish(0, j)
                product(g.rxp, 1, lambda rows, val: last(rows, acc[rows, :] + val))
                send(0, j)

            def far_late(j):
                last = finish(0, j)
                for i in range(2):
                    piece = 2 * (j - DOWN_X) + i
                    rows_in = pl.ds(i * deep, deep)

                    def block(rr, act_on):
                        act_on(pltpu.make_async_copy(tgat.land(g.c, rr, piece), wbuf.at[0, rr, rows_in], ws.at[0, 1, rr]))

                    def block_product(rr, emit):
                        matmul_rows(act.at[:, aligned(rr * depth + i * deep, deep)], wbuf.at[0, pl.ds(rr, 1), rows_in], 1024, emit)

                    tgat.arrive(0, piece)
                    tgat.start(3, piece)
                    block(g.rx, BEGIN)
                    block(g.rx, FINISH)
                    block_product(g.rx, add)
                    tgat.arrive(3, piece)
                    block(g.rxp, BEGIN)
                    block(g.rxp, FINISH)
                    block_product(g.rxp, (lambda rows, val: last(rows, acc[rows, :] + val)) if i else add)
                send(0, j)

            def pass_on(j):
                dgat.arrive(1, j)
                dgat.start(4, j)
                dgat.start(6, j)

            dgat.arrive(2, 0)
            mine_shard(0, BEGIN)

            @functools.partial(chunked, nd + 1)
            def _(t):
                @pl.when(t < nd)
                def _():
                    dgat.push(t)

                @pl.when(t < DOWN_X)
                def _():
                    pass_on(t + DOWN_X)

                @pl.when(t == 1)
                def _():
                    for j in range(2 * (nd - DOWN_X)):
                        tgat.start(0, j)

                @pl.when(t < nd)
                def _():
                    for kind in (4, 5):
                        dgat.arrive(kind, t)
                    fetch(t, BEGIN)
                    other(t)

                @pl.when(t <= DOWN_X)
                def _():
                    near(t)

                @pl.when(t < DOWN_X)
                def _():
                    far(t)

                @pl.when(t > DOWN_X)
                def _():
                    far_late(t - 1)

                @pl.when(t == nd - 1)
                def _():
                    near(nd - 1)

            for s in range(mine):
                for j in range(nd):
                    place(0, s, j).wait()
                    place(1, s, j).wait_send()
                    got = out.at[g.oc * mine + s, :, aligned(j * SLIM, SLIM)]
                    remote(got, got, gs.at[s, j], gr.at[s, j], g.Y).wait_recv()

        pl.run_scoped(down, pltpu.VMEM((2, 4, wd.shape[0], SLIM), BF), pltpu.VMEM((tokens, SLIM), F32))

    pl.run_scoped(mlp, pltpu.VMEM((tokens, 2 * wu.shape[1]), BF))
    small().wait_send()
    for p in range(pieces):
        hidden(p).wait_send()
    for gat, count in ((qgat, nq), (ogat, no), (ugat, nu), (dgat, DOWN_X)):
        gat.drain(range(7), 0, count)
    dgat.drain((1, 2, 4, 5, 6), DOWN_X, nd)
    tgat.drain((0, 3), 0, 2 * (nd - DOWN_X))


def layer_call(small, hidden, wq, wo, wu, wd, offs):
    seqs, seq, half = hidden.shape
    mine = seqs // 2
    tokens = mine * seq
    nq, no, nu, nd = wq.shape[0] * LANES // WIDE, wo.shape[1] // WIDE, wu.shape[1] // WIDE, wd.shape[1] // SLIM
    total = sum(a.size for a in small)
    dma = pltpu.SemaphoreType.DMA
    shape = lambda *dims: jax.ShapeDtypeStruct(dims, BF)
    sems = [dma((7, n)) for n in (nq, no, nu, nd) for _ in 'sr']
    sems += [dma((tokens // PIECE,))] * 2 + [dma((4, 4))] * 2 + [dma((2, 2)), dma, dma, dma((2,)), dma((2, 4, 4)), dma((2,)), dma((2, 3))] + [dma((mine, nd))] * 3
    return pl.pallas_call(
        functools.partial(layer_kernel, offs),
        in_specs=[pl.BlockSpec(memory_space=pltpu.VMEM)] * len(small) + [ANY] * 5,
        out_specs=[ANY] * 7,
        out_shape=[shape(*hidden.shape), shape(mine, seq, half), shape(tokens, 2 * wq.shape[0] * LANES)] + [shape(2, 4, *w.shape) for w in (wq, wo, wu, wd)],
        scratch_shapes=[pltpu.VMEM((tokens, 2 * half), BF), pltpu.VMEM((1, total), F32), pltpu.VMEM((2, 1, total), F32)] + sems,
        compiler_params=pltpu.CompilerParams(collective_id=1, has_side_effects=True, vmem_limit_bytes=VMEM_LIMIT),
        name='layer',
    )(*small, hidden, wq, wo, wu, wd)[0]


def tidy_kernel(src, dst, buf, ins, outs):
    count = src.shape[0] * 2
    rows = src.shape[1] // 2
    at = lambda ref, i: ref.at[i // 2, pl.ds(i % 2 * rows, rows)]
    loads = [pltpu.make_async_copy(at(src, i), buf.at[i], ins.at[i]) for i in range(count)]
    stores = [pltpu.make_async_copy(buf.at[i], at(dst, i), outs.at[i]) for i in range(count)]
    for load in loads:
        load.start()
    for load, store in zip(loads, stores):
        load.wait()
        store.start()
    for store in stores:
        store.wait()


def tidy(out):
    count = out.shape[0] * 2
    dma = pltpu.SemaphoreType.DMA
    return pl.pallas_call(
        tidy_kernel,
        in_specs=[ANY],
        out_specs=ANY,
        out_shape=jax.ShapeDtypeStruct(out.shape, BF),
        scratch_shapes=[pltpu.VMEM((count, out.shape[1] // 2, out.shape[2]), BF), dma((count,)), dma((count,))],
        compiler_params=pltpu.CompilerParams(vmem_limit_bytes=VMEM_LIMIT),
        name='tidy',
    )(out)


def solution(mesh):
    act_spec = P(('dp', 'row'), None, 'col')
    arg_specs = (act_spec, P('col'), P('col'), P('row', None, 'col', None), P(None, 'col', None), P('row', None, 'col'), P('col'), P('col'), P('col'), P('row', 'col'), P('col'), P('row', 'col'), P('col'))

    def local_layer(hidden, ln1_gain, ln1_bias, w_qkv, b_qkv, w_out, b_out, ln2_gain, ln2_bias, w_up, b_up, w_down, b_down):
        seqs, _, half = hidden.shape
        heads, size = w_qkv.shape[2], w_qkv.shape[3]
        small = {'g1': ln1_gain, 's1': ln1_bias, 'g2': ln2_gain, 's2': ln2_bias, 'bo': b_out, 'bd': b_down, 'bq': b_qkv, 'bu': b_up}
        offs, at = {}, 0
        for name, a in small.items():
            offs[name], at = at, at + a.size
        wq = jnp.transpose(w_qkv, (1, 2, 0, 3)).reshape(3 * heads, w_qkv.shape[0], size)
        wo = w_out.reshape(-1, half)
        return tidy(layer_call(list(small.values()), hidden, wq, wo, w_up, w_down, offs))

    return jax.shard_map(local_layer, mesh=mesh, in_specs=arg_specs, out_specs=act_spec, check_vma=False)
```

```python
import functools

import jax
import jax.numpy as jnp
from jax import lax
from jax.experimental import pallas as pl
from jax.experimental.pallas import tpu as pltpu
from jax.sharding import PartitionSpec as P

LN_EPS = 1e-5
BF = jnp.bfloat16
F32 = jnp.float32
LOG2E = 1.4426950408889634
MESH = pl.DeviceIdType.MESH
ANY = pl.BlockSpec(memory_space=pl.ANY)
VMEM_LIMIT = 63 * 1024 * 1024


class Grid:
    def __init__(self):
        self.c = lax.axis_index('col')
        self.r = lax.axis_index('row')
        self.oc = 1 - self.c
        x = self.r // 2
        k = self.r - 2 * x
        self.rp = 2 * x + 1 - k
        self.rx = 2 * (1 - x) + k
        self.rxp = 2 * (1 - x) + 1 - k
        self.P, self.X, self.Y = {'row': self.rp}, {'row': self.rx}, {'col': self.oc}

    def barrier(self):
        sem = pltpu.get_barrier_semaphore()
        for dev in (self.P, self.X, self.Y):
            pl.semaphore_signal(sem, inc=1, device_id=dev, device_id_type=MESH)
        pl.semaphore_wait(sem, 3)


def remote(src, dst, send, recv, dev):
    return pltpu.make_async_remote_copy(src_ref=src, dst_ref=dst, send_sem=send, recv_sem=recv, device_id=dev, device_id_type=MESH)


class Gather:
    def __init__(self, g, own, land, send, recv, via_x, split=None):
        self.split = split
        self.g, self.own, self.land, self.send_sem, self.recv_sem, self.via_x = g, own, land, send, recv, via_x

    def desc(self, kind, j, via_x=True):
        g = self.g
        if kind < 3:
            src, dst = self.own(j), self.land(g.c, g.r, j)
            dev = (g.X, g.Y, g.P)[kind]
        else:
            at = {3: (g.c, g.rx), 4: (g.oc, g.r), 5: (g.oc, g.rx), 6: (g.oc, g.r) if via_x else (g.c, g.rx)}[kind]
            src = dst = self.land(*at, j)
            dev = g.P if kind < 6 else (g.X if via_x else g.Y)
        return remote(src, dst, self.send_sem.at[kind, j], self.recv_sem.at[kind, j], dev)

    def routed(self, j, act):
        via = self.via_x(j)
        if isinstance(via, bool) and self.split is None:
            act(self.desc(6, j, via))
            return

        @pl.when(via)
        def _():
            act(self.desc(6, j))

        @pl.when(jnp.logical_not(via) & (j != self.split[0]) if self.split else jnp.logical_not(via))
        def _():
            act(self.desc(6, j, False))

        if self.split:
            @pl.when(j == self.split[0])
            def _():
                for copy in self.shares():
                    act(copy)

    def shares(self, arriving=False):
        g, (j, rows, sems) = self.g, self.split
        copies = []
        for i, dev in enumerate((g.X, g.Y)):
            cut = pl.ds(0, rows) if i == 0 else pl.ds(rows, self.own(j).shape[0] - rows)
            at = (g.oc, g.rx) if arriving else ((g.oc, g.r) if i == 0 else (g.c, g.rx))
            ref = self.land(*at, j).at[cut]
            copies.append(remote(ref, ref, sems.at[0, i], sems.at[1, i], dev))
        return copies

    def start(self, kind, j):
        if kind == 6:
            self.routed(j, lambda d: d.start())
        else:
            self.desc(kind, j).start()

    def arrive(self, kind, j):
        g = self.g
        at = [(g.c, g.rx), (g.oc, g.r), (g.c, g.rp), (g.c, g.rxp), (g.oc, g.rp), (g.oc, g.rxp), (g.oc, g.rx)][kind]
        ref = self.land(*at, j)
        copy = remote(ref, ref, self.send_sem.at[kind, j], self.recv_sem.at[kind, j], g.P)
        if kind < 6 or not self.split:
            copy.wait_recv()
            return

        @pl.when(j != self.split[0])
        def _():
            copy.wait_recv()

        @pl.when(j == self.split[0])
        def _():
            for part in self.shares(True):
                part.wait_recv()

    def drain(self, kinds, lo, hi):
        @functools.partial(chunked, hi - lo)
        def _(i):
            for kind in kinds:
                if kind == 6:
                    self.routed(lo + i, lambda d: d.wait_send())
                else:
                    self.desc(kind, lo + i).wait_send()

    def relay(self, j):
        self.arrive(0, j)
        self.start(3, j)
        self.arrive(1, j)
        self.start(4, j)
        self.start(6, j)

    def push(self, j):
        self.arrive(6, j)
        self.start(5, j)


def chunked(total, body):
    lax.fori_loop(0, total, lambda j, carry: (body(j), carry)[1], 0)


def matmul_rows(a_ref, w_ref, tile, emit):
    depth = w_ref.shape[0] * w_ref.shape[1]

    def body(m):
        rows = pl.ds(pl.multiple_of(m * tile, tile), tile)
        w = w_ref[...].reshape(depth, w_ref.shape[2])
        emit(rows, jnp.dot(a_ref[rows, :], w, preferred_element_type=F32))

    chunked(a_ref.shape[0] // tile, body)


def norm_rows(parts, gains, shifts):
    parts = [p.astype(F32) for p in parts]
    width = sum(p.shape[1] for p in parts)
    mean = sum(jnp.sum(p, axis=1, keepdims=True) for p in parts) / width
    parts = [p - mean for p in parts]
    var = sum(jnp.sum(p * p, axis=1, keepdims=True) for p in parts) / width
    inv = lax.rsqrt(var + LN_EPS)
    return [(p * inv * gn + sh).astype(BF) for p, gn, sh in zip(parts, gains, shifts)]


def columns(own_ref, wland, width):
    def cols(j):
        return pl.ds(pl.multiple_of(j * width, width), width)

    return (lambda j: own_ref.at[:, cols(j)]), (lambda cc, rr, j: wland.at[cc, rr, :, cols(j)])


def shard_loads(g, own, land_all, land, buf, sems, rel, j):
    if rel == 0:
        srcs = [own(j)] + [land(g.c, rr, j) for rr in (g.rp, g.rx, g.rxp)]
        return [pltpu.make_async_copy(s, buf.at[rr], sems.at[i]) for i, (s, rr) in enumerate(zip(srcs, (g.r, g.rp, g.rx, g.rxp)))]
    return [pltpu.make_async_copy(land_all(g.oc, j), buf, sems.at[0])]


def attn_head(block, q_ref, k_ref, v_ref, o_ref):
    seq, size = q_ref.shape
    scale = size ** -0.5 * LOG2E
    tri = lax.broadcasted_iota(jnp.int32, (block, block), 0) >= lax.broadcasted_iota(jnp.int32, (block, block), 1)

    def scores(i):
        q = q_ref[i * block:(i + 1) * block, :]
        dot = lambda k: lax.dot_general(q, k, (((1,), (1,)), ((), ())), preferred_element_type=F32)
        diag = jnp.where(tri, dot(k_ref[i * block:(i + 1) * block, :]), -1e30 * size ** 0.5)
        return [dot(k_ref[:i * block, :]), diag] if i else [diag]

    def probs(parts):
        top = functools.reduce(jnp.maximum, [jnp.max(s, axis=1, keepdims=True) for s in parts])
        parts = [jnp.exp2((s - top) * scale) for s in parts]
        inv = 1.0 / sum(jnp.sum(e, axis=1, keepdims=True) for e in parts)
        return jnp.concatenate([(e * inv).astype(BF) for e in parts], axis=1)

    def finish(i, p):
        o_ref[i * block:(i + 1) * block, :] = jnp.dot(p, v_ref[:(i + 1) * block, :], preferred_element_type=F32).astype(BF)

    count = seq // block
    ahead, before = scores(0), None
    for i in range(count):
        now, ahead = ahead, scores(i + 1) if i + 1 < count else None
        now = probs(now)
        if i:
            finish(i - 1, before)
        before = now
    finish(count - 1, before)


BEGIN, FINISH = (lambda d: d.start()), (lambda d: d.wait())
WIDE, SLIM, LANES, PIECE = 512, 256, 128, 512
DOWN_X, EARLY, SHARE = 2, 4, 128


def aligned(start, size):
    return pl.ds(pl.multiple_of(start, size), size)


def layer_kernel(offs, g1, s1, g2, s2, bo, bd, bq, bu, hid, wq, wo, wu, wd, out, xland, qkv, qland, oland, uland, dland, hb, pk, pk2,
                 qs, qr, os, oo, us, ur, ds, dr, hs, hr, ts, tr, vs, ps, pr, ls, ws, st, al, gs, gr, ks):
    g = Grid()
    g.barrier()
    seqs, seq, half = hid.shape
    mine = seqs // 2
    tokens = mine * seq
    units = WIDE // LANES
    qgat = Gather(g, lambda j: wq.at[pl.ds(j * units, units)], lambda cc, rr, j: qland.at[cc, rr, pl.ds(j * units, units)], qs, qr, lambda j: True)
    ogat = Gather(g, *columns(wo, oland, WIDE), os, oo, lambda j: j == 0)
    ugat = Gather(g, *columns(wu, uland, WIDE), us, ur, lambda j: j >= 5, (4, SHARE, vs))
    dgat = Gather(g, *columns(wd, dland, SLIM), ds, dr, lambda j: True)
    deep = wd.shape[0] // 2
    cut = lambda j: (pl.ds(j % 2 * deep, deep), aligned((DOWN_X + j // 2) * SLIM, SLIM))
    tgat = Gather(g, lambda j: wd.at[cut(j)], lambda cc, rr, j: dland.at[(cc, rr) + cut(j)], ts, tr, None)
    nq, no, nu, nd = wq.shape[0] // units, wo.shape[1] // WIDE, wu.shape[1] // WIDE, wd.shape[1] // SLIM
    per = seq // PIECE
    pieces = mine * per

    def vec(name, cc, size, start=0):
        return pk2[cc, :, pl.ds(offs[name] + start, size)]

    def small():
        return remote(pk, pk2.at[g.c], ps, pr, g.Y)

    def span(p):
        return p // per, pl.ds(p % per * PIECE, PIECE)

    def hidden(p):
        s, rows = span(p)
        return remote(hid.at[g.oc * mine + s, rows], xland.at[s, rows], hs.at[p], hr.at[p], g.Y)

    hidden(0).start()

    @functools.partial(chunked, nq)
    def _(j):
        qgat.start(0, j)

    ogat.start(0, 0)
    for ref, start in zip((g1, s1, g2, s2, bo, bd, bq, bu), offs.values()):
        if len(ref.shape) == 1:
            pk[0, pl.ds(start, ref.shape[0])] = ref[...].astype(F32)
            continue
        for i in range(ref.shape[0]):
            for j in range(ref.shape[1]):
                pk[0, pl.ds(start + (i * ref.shape[1] + j) * LANES, LANES)] = ref[i, j, :].astype(F32)
    small().start()
    for p in range(1, pieces):
        hidden(p).start()
    for kind in (2, 1):
        @functools.partial(chunked, nq)
        def _(j):
            qgat.start(kind, j)
    for j in range(no):
        ogat.start(1, j)
    for j in range(EARLY):
        ugat.start(1, j)

    def qkv_phase(xbuf, wbuf, obuf, ab):
        pk2[g.c] = pk[...]
        small().wait_recv()
        gains = [vec('g1', cc, half) for cc in (g.c, g.oc)]
        shifts = [vec('s1', cc, half) for cc in (g.c, g.oc)]
        for p in range(pieces):
            s, rows = span(p)
            loads = [pltpu.make_async_copy(src, xbuf.at[i], ls.at[i]) for i, src in enumerate((hid.at[g.c * mine + s, rows], xland.at[s, rows]))]
            loads[0].start()
            hidden(p).wait_recv()
            loads[1].start()
            for load in loads:
                load.wait()
            sub = 64

            @functools.partial(chunked, PIECE // sub)
            def _(i):
                rows = aligned(i * sub, sub)
                res = norm_rows([xbuf[0, rows, :], xbuf[1, rows, :]], gains, shifts)
                for cc, val in zip((g.c, g.oc), res):
                    ab[aligned(p * PIECE + i * sub, sub), aligned(cc * half, half)] = val

        def load_own(j, act_on):
            for i in range(units):
                for idx, rr in enumerate((g.r, g.rp, g.rx, g.rxp)):
                    src = qland.at[g.c, rr, j * units + i] if idx else wq.at[j * units + i]
                    act_on(pltpu.make_async_copy(src, wbuf.at[0, rr, :, pl.ds(i * LANES, LANES)], ws.at[0, i, idx]))

        def load_other(j, act_on):
            for i in range(units):
                act_on(pltpu.make_async_copy(qland.at[g.oc, :, j * units + i], wbuf.at[1, :, :, pl.ds(i * LANES, LANES)], ws.at[1, i, 0]))

        def save(slot, cc, j):
            return pltpu.make_async_copy(obuf.at[slot], qkv.at[:, aligned((cc * nq + j) * WIDE, WIDE)], st.at[slot])

        def compute(slot, cc, j):
            @pl.when(j > 0)
            def _():
                save(slot, cc, j - 1).wait()

            bias = vec('bq', cc, WIDE, pl.multiple_of(j * WIDE, WIDE))

            def emit(rows, val):
                obuf[slot, rows, :] = (val + bias).astype(BF)

            matmul_rows(ab, wbuf.at[slot], 1024, emit)
            save(slot, cc, j).start()

        @functools.partial(chunked, nq + 3)
        def _(t):
            @pl.when(t < nq)
            def _():
                qgat.relay(t)

            @pl.when(t == nq - 1)
            def _():
                for j in range(1, no):
                    ogat.start(0, j)
                for j in range(2):
                    ugat.start(0, j)

            @pl.when((t >= 1) & (t <= nq))
            def _():
                qgat.push(t - 1)

            @pl.when(t < nq)
            def _():
                qgat.arrive(2, t)
                qgat.arrive(3, t)
                load_own(t, BEGIN)

            @pl.when(t >= 3)
            def _():
                load_other(t - 3, FINISH)
                compute(1, g.oc, t - 3)

            @pl.when((t >= 2) & (t < nq + 2))
            def _():
                qgat.arrive(4, t - 2)
                qgat.arrive(5, t - 2)
                load_other(t - 2, BEGIN)

            @pl.when(t < nq)
            def _():
                load_own(t, FINISH)
                compute(0, g.c, t)

        for slot, cc in enumerate((g.c, g.oc)):
            save(slot, cc, nq - 1).wait()

    pl.run_scoped(
        qkv_phase,
        pltpu.VMEM((2, PIECE, half), BF),
        pltpu.VMEM((2, 4, wq.shape[1], WIDE), BF),
        pltpu.VMEM((2, tokens, WIDE), BF),
        pltpu.VMEM((tokens, 2 * half), BF),
    )

    heads = wq.shape[0] // 3

    def attend(ob, abuf, wob, xb):
        def first():
            for j in range(no):
                ogat.start(2, j)
                ogat.relay(j)
            for j in range(nu):
                ugat.start(2, j)
            for j in range(2, nu):
                ugat.start(0, j)
            for j in range(EARLY, nu):
                ugat.start(1, j)

        events = {0: first, 34: lambda: ogat.push(0), 46: lambda: ogat.push(1)}
        for j, at in enumerate((10, 18)):
            events[at] = functools.partial(ugat.relay, j)
        steps = mine * 2 * heads

        def block(step, act_on):
            s, h = step // (2 * heads), step % (2 * heads)
            base = (h // heads) * 3 * heads + h % heads
            for i in range(3):
                src = qkv.at[aligned(s * seq, seq), aligned((base + i * heads) * LANES, LANES)]
                act_on(pltpu.make_async_copy(src, abuf.at[step % 2, i], al.at[step % 2, i]))

        block(0, BEGIN)

        @functools.partial(chunked, steps)
        def _(step):
            for at, act in events.items():
                pl.when(step == at)(act)

            @pl.when(step + 1 < steps)
            def _():
                block(step + 1, BEGIN)

            block(step, FINISH)
            s, h = step // (2 * heads), step % (2 * heads)
            attn_head(256, *(abuf.at[step % 2, i] for i in range(3)), ob.at[aligned(s * seq, seq), aligned(h * LANES, LANES)])

        for j in range(no):
            for kind in range(2, 6):
                ogat.arrive(kind, j)
        parts = half // WIDE

        def fetch(i, act_on):
            slot, rel, j = i % 2, i // parts, i % parts
            at = pl.ds(j * WIDE, WIDE)
            copies = shard_loads(g, ogat.own, lambda cc, j: oland.at[cc, :, :, at], ogat.land, wob.at[slot], ws.at[slot, 0], rel, j)
            for s in range(mine):
                src = xland.at[s, :, at] if rel else hid.at[g.c * mine + s, :, at]
                copies.append(pltpu.make_async_copy(src, xb.at[slot, pl.ds(s * seq, seq)], ws.at[slot, 1, s]))
            for copy in copies:
                act_on(copy)

        fetch(0, BEGIN)
        for i in range(2 * parts):
            slot = i % 2
            if i + 1 < 2 * parts:
                fetch(i + 1, BEGIN)
            fetch(i, FINISH)
            cc = g.oc if i >= parts else g.c
            bias = vec('bo', cc, WIDE, i % parts * WIDE)
            at = aligned(cc * half + i % parts * WIDE, WIDE)

            def emit(rows, val):
                hb[rows, at] = (xb[slot, rows, :].astype(F32) + val + bias).astype(BF)

            matmul_rows(ob, wob.at[slot], 512, emit)
            ugat.relay(2 + i)

    pl.run_scoped(
        attend,
        pltpu.VMEM((tokens, 2 * heads * LANES), BF),
        pltpu.VMEM((2, 3, seq, LANES), BF),
        pltpu.VMEM((2, 4, wo.shape[0], WIDE), BF),
        pltpu.VMEM((2, tokens, WIDE), BF),
    )

    small().wait_send()
    for p in range(pieces):
        hidden(p).wait_send()
    qgat.drain(range(7), 0, nq)
    ogat.drain(range(7), 0, no)

    def mlp(act):
        def load(gat, land, width, wbuf, rel, j, act_on):
            whole = lambda cc, j: land.at[cc, :, :, aligned(j * width, width)]
            for copy in shard_loads(g, gat.own, whole, gat.land, wbuf.at[rel], ws.at[rel, 0], rel, j):
                act_on(copy)

        def up(wbuf, ab):
            gains = [vec('g2', cc, half) for cc in range(2)]
            shifts = [vec('s2', cc, half) for cc in range(2)]

            @functools.partial(chunked, tokens // 64)
            def _(i):
                rows = aligned(i * 64, 64)
                ab[rows, :half], ab[rows, half:] = norm_rows([hb[rows, :half], hb[rows, half:]], gains, shifts)

            fetch = functools.partial(load, ugat, uland, WIDE, wbuf)

            def compute(rel, j):
                cc = g.oc if rel else g.c
                bias = vec('bu', cc, WIDE, pl.multiple_of(j * WIDE, WIDE))
                at = aligned((cc * nu + j) * WIDE, WIDE)

                def emit(rows, val):
                    act[rows, at] = jax.nn.gelu(val + bias, approximate=True).astype(BF)

                fetch(rel, j, FINISH)
                matmul_rows(ab, wbuf.at[rel], 1024, emit)

            def ready(rel, j):
                for kind in ((4, 5) if rel else (2, 3)):
                    ugat.arrive(kind, j)
                fetch(rel, j, BEGIN)

            ugat.relay(nu - 2)
            ready(0, 0)

            @functools.partial(chunked, nu + 1)
            def _(t):
                @pl.when(t < nu)
                def _():
                    compute(0, t)

                @pl.when(t == 0)
                def _():
                    ugat.push(0)
                    ugat.relay(nu - 1)
                    for j in range(nd):
                        dgat.start(1, j)
                        dgat.start(2, j)
                    for j in range(DOWN_X):
                        dgat.start(0, j)

                @pl.when(t + 1 < nu)
                def _():
                    ready(0, t + 1)

                @pl.when((t >= 1) & (t < nu))
                def _():
                    ugat.push(t)

                @pl.when(t == 1)
                def _():
                    ready(1, 0)

                @pl.when((t == 6) | (t == 8))
                def _():
                    dgat.relay((t - 6) // 2)

                @pl.when(t >= 1)
                def _():
                    compute(1, t - 1)

                @pl.when((t >= 1) & (t < nu))
                def _():
                    ready(1, t)

        pl.run_scoped(up, pltpu.VMEM((2, 4, wu.shape[0], WIDE), BF), pltpu.VMEM((tokens, 2 * half), BF))

        def down(wbuf, acc):
            depth = wd.shape[0]
            fetch = functools.partial(load, dgat, dland, SLIM, wbuf, 1)

            def spot(rel, j):
                return aligned((g.oc if rel else g.c) * half + j * SLIM, SLIM)

            def place(rel, s, j):
                src = hb.at[pl.ds(s * seq, seq), spot(rel, j)]
                dst = out.at[g.c * mine + s, :, aligned(j * SLIM, SLIM)]
                return remote(src, dst, gs.at[s, j], gr.at[s, j], g.Y) if rel else pltpu.make_async_copy(src, dst, ks.at[s, j])

            def finish(rel, j):
                cc = g.oc if rel else g.c
                bias = vec('bd', cc, SLIM, pl.multiple_of(j * SLIM, SLIM))

                def emit(rows, val):
                    hb[rows, spot(rel, j)] = (hb[rows, spot(rel, j)].astype(F32) + val + bias).astype(BF)

                return emit

            def send(rel, j):
                for s in range(mine):
                    place(rel, s, j).start()

            def other(j):
                fetch(j, FINISH)
                matmul_rows(act, wbuf.at[1], 1024, finish(1, j))
                send(1, j)

            def shard(rr, j, act_on):
                src = dland.at[g.c, rr, :, aligned(j * SLIM, SLIM)]
                act_on(pltpu.make_async_copy(src, wbuf.at[0, rr], ws.at[0, 1, rr]))

            def mine_shard(j, act_on):
                act_on(pltpu.make_async_copy(dgat.own(j), wbuf.at[0, g.r], ws.at[0, 1, g.r]))
                shard(g.rp, j, act_on)

            def product(rr, count, emit):
                matmul_rows(act.at[:, aligned(rr * depth, count * depth)], wbuf.at[0, pl.ds(rr, count)], 1024, emit)

            def near(j):
                mine_shard(j, FINISH)

                def emit(rows, val):
                    acc[rows, :] = val

                product(g.r // 2 * 2, 2, emit)

                @pl.when(j + 1 < nd)
                def _():
                    dgat.arrive(2, j + 1)
                    mine_shard(j + 1, BEGIN)

            def add(rows, val):
                acc[rows, :] += val

            def far(j):
                shard(g.rx, j, BEGIN)
                dgat.arrive(3, j)
                shard(g.rxp, j, BEGIN)
                shard(g.rx, j, FINISH)
                product(g.rx, 1, add)
                shard(g.rxp, j, FINISH)
                last = finish(0, j)
                product(g.rxp, 1, lambda rows, val: last(rows, acc[rows, :] + val))
                send(0, j)

            def far_late(j):
                last = finish(0, j)
                for i in range(2):
                    piece = 2 * (j - DOWN_X) + i
                    rows_in = pl.ds(i * deep, deep)

                    def block(rr, act_on):
                        act_on(pltpu.make_async_copy(tgat.land(g.c, rr, piece), wbuf.at[0, rr, rows_in], ws.at[0, 1, rr]))

                    def block_product(rr, emit):
                        matmul_rows(act.at[:, aligned(rr * depth + i * deep, deep)], wbuf.at[0, pl.ds(rr, 1), rows_in], 1024, emit)

                    tgat.arrive(0, piece)
                    tgat.start(3, piece)
                    block(g.rx, BEGIN)
                    block(g.rx, FINISH)
                    block_product(g.rx, add)
                    tgat.arrive(3, piece)
                    block(g.rxp, BEGIN)
                    block(g.rxp, FINISH)
                    block_product(g.rxp, (lambda rows, val: last(rows, acc[rows, :] + val)) if i else add)
                send(0, j)

            def pass_on(j):
                dgat.arrive(1, j)
                dgat.start(4, j)
                dgat.start(6, j)

            dgat.arrive(2, 0)
            mine_shard(0, BEGIN)

            @functools.partial(chunked, nd + 1)
            def _(t):
                @pl.when(t < nd)
                def _():
                    dgat.push(t)

                @pl.when(t < DOWN_X)
                def _():
                    pass_on(t + DOWN_X)

                @pl.when(t == 1)
                def _():
                    for j in range(2 * (nd - DOWN_X)):
                        tgat.start(0, j)

                @pl.when(t < nd)
                def _():
                    for kind in (4, 5):
                        dgat.arrive(kind, t)
                    fetch(t, BEGIN)
                    other(t)

                @pl.when(t <= DOWN_X)
                def _():
                    near(t)

                @pl.when(t == DOWN_X)
                def _():
                    ugat.drain(range(7), 0, nu)

                @pl.when(t < DOWN_X)
                def _():
                    far(t)

                @pl.when(t > DOWN_X)
                def _():
                    far_late(t - 1)

                @pl.when(t == nd - 1)
                def _():
                    near(nd - 1)

            for s in range(mine):
                for j in range(nd):
                    place(0, s, j).wait()
                    place(1, s, j).wait_send()
                    got = out.at[g.oc * mine + s, :, aligned(j * SLIM, SLIM)]
                    remote(got, got, gs.at[s, j], gr.at[s, j], g.Y).wait_recv()

        pl.run_scoped(down, pltpu.VMEM((2, 4, wd.shape[0], SLIM), BF), pltpu.VMEM((tokens, SLIM), F32))

    pl.run_scoped(mlp, pltpu.VMEM((tokens, 2 * wu.shape[1]), BF))
    dgat.drain(range(7), 0, DOWN_X)
    dgat.drain((1, 2, 4, 5, 6), DOWN_X, nd)
    tgat.drain((0, 3), 0, 2 * (nd - DOWN_X))


def layer_call(small, hidden, wq, wo, wu, wd, offs):
    seqs, seq, half = hidden.shape
    mine = seqs // 2
    tokens = mine * seq
    nq, no, nu, nd = wq.shape[0] * LANES // WIDE, wo.shape[1] // WIDE, wu.shape[1] // WIDE, wd.shape[1] // SLIM
    total = sum(a.size for a in small)
    dma = pltpu.SemaphoreType.DMA
    shape = lambda *dims: jax.ShapeDtypeStruct(dims, BF)
    sems = [dma((7, n)) for n in (nq, no, nu, nd) for _ in 'sr']
    sems += [dma((tokens // PIECE,))] * 2 + [dma((4, 4))] * 2 + [dma((2, 2)), dma, dma, dma((2,)), dma((2, 4, 4)), dma((2,)), dma((2, 3))] + [dma((mine, nd))] * 3
    return pl.pallas_call(
        functools.partial(layer_kernel, offs),
        in_specs=[pl.BlockSpec(memory_space=pltpu.VMEM)] * len(small) + [ANY] * 5,
        out_specs=[ANY] * 7,
        out_shape=[shape(*hidden.shape), shape(mine, seq, half), shape(tokens, 2 * wq.shape[0] * LANES)] + [shape(2, 4, *w.shape) for w in (wq, wo, wu, wd)],
        scratch_shapes=[pltpu.VMEM((tokens, 2 * half), BF), pltpu.VMEM((1, total), F32), pltpu.VMEM((2, 1, total), F32)] + sems,
        compiler_params=pltpu.CompilerParams(collective_id=1, has_side_effects=True, vmem_limit_bytes=VMEM_LIMIT),
        name='layer',
    )(*small, hidden, wq, wo, wu, wd)[0]


def tidy_kernel(src, dst, buf, ins, outs):
    count = src.shape[0] * 2
    rows = src.shape[1] // 2
    at = lambda ref, i: ref.at[i // 2, pl.ds(i % 2 * rows, rows)]
    loads = [pltpu.make_async_copy(at(src, i), buf.at[i], ins.at[i]) for i in range(count)]
    stores = [pltpu.make_async_copy(buf.at[i], at(dst, i), outs.at[i]) for i in range(count)]
    for load in loads:
        load.start()
    for load, store in zip(loads, stores):
        load.wait()
        store.start()
    for store in stores:
        store.wait()


def tidy(out):
    count = out.shape[0] * 2
    dma = pltpu.SemaphoreType.DMA
    return pl.pallas_call(
        tidy_kernel,
        in_specs=[ANY],
        out_specs=ANY,
        out_shape=jax.ShapeDtypeStruct(out.shape, BF),
        scratch_shapes=[pltpu.VMEM((count, out.shape[1] // 2, out.shape[2]), BF), dma((count,)), dma((count,))],
        compiler_params=pltpu.CompilerParams(vmem_limit_bytes=VMEM_LIMIT),
        name='tidy',
    )(out)


def solution(mesh):
    act_spec = P(('dp', 'row'), None, 'col')
    arg_specs = (act_spec, P('col'), P('col'), P('row', None, 'col', None), P(None, 'col', None), P('row', None, 'col'), P('col'), P('col'), P('col'), P('row', 'col'), P('col'), P('row', 'col'), P('col'))

    def local_layer(hidden, ln1_gain, ln1_bias, w_qkv, b_qkv, w_out, b_out, ln2_gain, ln2_bias, w_up, b_up, w_down, b_down):
        seqs, _, half = hidden.shape
        heads, size = w_qkv.shape[2], w_qkv.shape[3]
        small = {'g1': ln1_gain, 's1': ln1_bias, 'g2': ln2_gain, 's2': ln2_bias, 'bo': b_out, 'bd': b_down, 'bq': b_qkv, 'bu': b_up}
        offs, at = {}, 0
        for name, a in small.items():
            offs[name], at = at, at + a.size
        wq = jnp.transpose(w_qkv, (1, 2, 0, 3)).reshape(3 * heads, w_qkv.shape[0], size)
        wo = w_out.reshape(-1, half)
        return tidy(layer_call(list(small.values()), hidden, wq, wo, w_up, w_down, offs))

    return jax.shard_map(local_layer, mesh=mesh, in_specs=arg_specs, out_specs=act_spec, check_vma=False)
```

```python
import functools

import jax
import jax.numpy as jnp
from jax import lax
from jax.experimental import pallas as pl
from jax.experimental.pallas import tpu as pltpu
from jax.sharding import PartitionSpec as P

LN_EPS = 1e-5
BF = jnp.bfloat16
F32 = jnp.float32
LOG2E = 1.4426950408889634
MESH = pl.DeviceIdType.MESH
ANY = pl.BlockSpec(memory_space=pl.ANY)
VMEM_LIMIT = 63 * 1024 * 1024


class Grid:
    def __init__(self):
        self.c = lax.axis_index('col')
        self.r = lax.axis_index('row')
        self.oc = 1 - self.c
        x = self.r // 2
        k = self.r - 2 * x
        self.rp = 2 * x + 1 - k
        self.rx = 2 * (1 - x) + k
        self.rxp = 2 * (1 - x) + 1 - k
        self.P, self.X, self.Y = {'row': self.rp}, {'row': self.rx}, {'col': self.oc}

    def barrier(self):
        sem = pltpu.get_barrier_semaphore()
        for dev in (self.P, self.X, self.Y):
            pl.semaphore_signal(sem, inc=1, device_id=dev, device_id_type=MESH)
        pl.semaphore_wait(sem, 3)


def remote(src, dst, send, recv, dev):
    return pltpu.make_async_remote_copy(src_ref=src, dst_ref=dst, send_sem=send, recv_sem=recv, device_id=dev, device_id_type=MESH)


class Gather:
    def __init__(self, g, own, land, send, recv, via_x, split=None):
        self.split = split
        self.g, self.own, self.land, self.send_sem, self.recv_sem, self.via_x = g, own, land, send, recv, via_x

    def desc(self, kind, j, via_x=True):
        g = self.g
        if kind < 3:
            src, dst = self.own(j), self.land(g.c, g.r, j)
            dev = (g.X, g.Y, g.P)[kind]
        else:
            at = {3: (g.c, g.rx), 4: (g.oc, g.r), 5: (g.oc, g.rx), 6: (g.oc, g.r) if via_x else (g.c, g.rx)}[kind]
            src = dst = self.land(*at, j)
            dev = g.P if kind < 6 else (g.X if via_x else g.Y)
        return remote(src, dst, self.send_sem.at[kind, j], self.recv_sem.at[kind, j], dev)

    def routed(self, j, act):
        via = self.via_x(j)
        if isinstance(via, bool) and self.split is None:
            act(self.desc(6, j, via))
            return

        @pl.when(via)
        def _():
            act(self.desc(6, j))

        @pl.when(jnp.logical_not(via) & (j != self.split[0]) if self.split else jnp.logical_not(via))
        def _():
            act(self.desc(6, j, False))

        if self.split:
            @pl.when(j == self.split[0])
            def _():
                for copy in self.shares():
                    act(copy)

    def shares(self, arriving=False):
        g, (j, rows, sems) = self.g, self.split
        copies = []
        for i, dev in enumerate((g.X, g.Y)):
            cut = pl.ds(0, rows) if i == 0 else pl.ds(rows, self.own(j).shape[0] - rows)
            at = (g.oc, g.rx) if arriving else ((g.oc, g.r) if i == 0 else (g.c, g.rx))
            ref = self.land(*at, j).at[cut]
            copies.append(remote(ref, ref, sems.at[0, i], sems.at[1, i], dev))
        return copies

    def start(self, kind, j):
        if kind == 6:
            self.routed(j, lambda d: d.start())
        else:
            self.desc(kind, j).start()

    def arrive(self, kind, j):
        g = self.g
        at = [(g.c, g.rx), (g.oc, g.r), (g.c, g.rp), (g.c, g.rxp), (g.oc, g.rp), (g.oc, g.rxp), (g.oc, g.rx)][kind]
        ref = self.land(*at, j)
        copy = remote(ref, ref, self.send_sem.at[kind, j], self.recv_sem.at[kind, j], g.P)
        if kind < 6 or not self.split:
            copy.wait_recv()
            return

        @pl.when(j != self.split[0])
        def _():
            copy.wait_recv()

        @pl.when(j == self.split[0])
        def _():
            for part in self.shares(True):
                part.wait_recv()

    def drain(self, kinds, lo, hi):
        @functools.partial(chunked, hi - lo)
        def _(i):
            for kind in kinds:
                if kind == 6:
                    self.routed(lo + i, lambda d: d.wait_send())
                else:
                    self.desc(kind, lo + i).wait_send()

    def relay(self, j):
        self.arrive(0, j)
        self.start(3, j)
        self.arrive(1, j)
        self.start(4, j)
        self.start(6, j)

    def push(self, j):
        self.arrive(6, j)
        self.start(5, j)


def chunked(total, body):
    lax.fori_loop(0, total, lambda j, carry: (body(j), carry)[1], 0)


def matmul_rows(a_ref, w_ref, tile, emit):
    depth = w_ref.shape[0] * w_ref.shape[1]

    def body(m):
        rows = pl.ds(pl.multiple_of(m * tile, tile), tile)
        w = w_ref[...].reshape(depth, w_ref.shape[2])
        emit(rows, jnp.dot(a_ref[rows, :], w, preferred_element_type=F32))

    chunked(a_ref.shape[0] // tile, body)


def norm_rows(parts, gains, shifts):
    parts = [p.astype(F32) for p in parts]
    width = sum(p.shape[1] for p in parts)
    mean = sum(jnp.sum(p, axis=1, keepdims=True) for p in parts) / width
    parts = [p - mean for p in parts]
    var = sum(jnp.sum(p * p, axis=1, keepdims=True) for p in parts) / width
    inv = lax.rsqrt(var + LN_EPS)
    return [(p * inv * gn + sh).astype(BF) for p, gn, sh in zip(parts, gains, shifts)]


def columns(own_ref, wland, width):
    def cols(j):
        return pl.ds(pl.multiple_of(j * width, width), width)

    return (lambda j: own_ref.at[:, cols(j)]), (lambda cc, rr, j: wland.at[cc, rr, :, cols(j)])


def shard_loads(g, own, land_all, land, buf, sems, rel, j):
    if rel == 0:
        srcs = [own(j)] + [land(g.c, rr, j) for rr in (g.rp, g.rx, g.rxp)]
        return [pltpu.make_async_copy(s, buf.at[rr], sems.at[i]) for i, (s, rr) in enumerate(zip(srcs, (g.r, g.rp, g.rx, g.rxp)))]
    return [pltpu.make_async_copy(land_all(g.oc, j), buf, sems.at[0])]


def attn_head(block, q_ref, k_ref, v_ref, o_ref):
    seq, size = q_ref.shape
    scale = size ** -0.5 * LOG2E
    tri = lax.broadcasted_iota(jnp.int32, (block, block), 0) >= lax.broadcasted_iota(jnp.int32, (block, block), 1)

    def scores(i):
        q = q_ref[i * block:(i + 1) * block, :]
        dot = lambda k: lax.dot_general(q, k, (((1,), (1,)), ((), ())), preferred_element_type=F32)
        diag = jnp.where(tri, dot(k_ref[i * block:(i + 1) * block, :]), -1e30 * size ** 0.5)
        return [dot(k_ref[:i * block, :]), diag] if i else [diag]

    def probs(parts):
        top = functools.reduce(jnp.maximum, [jnp.max(s, axis=1, keepdims=True) for s in parts])
        parts = [jnp.exp2((s - top) * scale) for s in parts]
        inv = 1.0 / sum(jnp.sum(e, axis=1, keepdims=True) for e in parts)
        return jnp.concatenate([(e * inv).astype(BF) for e in parts], axis=1)

    def finish(i, p):
        o_ref[i * block:(i + 1) * block, :] = jnp.dot(p, v_ref[:(i + 1) * block, :], preferred_element_type=F32).astype(BF)

    count = seq // block
    ahead, before = scores(0), None
    for i in range(count):
        now, ahead = ahead, scores(i + 1) if i + 1 < count else None
        now = probs(now)
        if i:
            finish(i - 1, before)
        before = now
    finish(count - 1, before)


BEGIN, FINISH = (lambda d: d.start()), (lambda d: d.wait())
WIDE, SLIM, LANES, PIECE = 512, 256, 128, 512
DOWN_X, EARLY, SHARE = 2, 4, 128


def aligned(start, size):
    return pl.ds(pl.multiple_of(start, size), size)


def layer_kernel(offs, g1, s1, g2, s2, bo, bd, bq, bu, hid, wq, wo, wu, wd, out, xland, qkv, qland, oland, uland, dland, hb, pk, pk2,
                 qs, qr, os, oo, us, ur, ds, dr, hs, hr, ts, tr, vs, ps, pr, ls, ws, st, al, gs, gr, ks):
    g = Grid()
    g.barrier()
    seqs, seq, half = hid.shape
    mine = seqs // 2
    tokens = mine * seq
    units = WIDE // LANES
    qgat = Gather(g, lambda j: wq.at[pl.ds(j * units, units)], lambda cc, rr, j: qland.at[cc, rr, pl.ds(j * units, units)], qs, qr, lambda j: True)
    ogat = Gather(g, *columns(wo, oland, WIDE), os, oo, lambda j: j == 0)
    ugat = Gather(g, *columns(wu, uland, WIDE), us, ur, lambda j: j >= 5, (4, SHARE, vs))
    dgat = Gather(g, *columns(wd, dland, SLIM), ds, dr, lambda j: True)
    deep = wd.shape[0] // 2
    cut = lambda j: (pl.ds(j % 2 * deep, deep), aligned((DOWN_X + j // 2) * SLIM, SLIM))
    tgat = Gather(g, lambda j: wd.at[cut(j)], lambda cc, rr, j: dland.at[(cc, rr) + cut(j)], ts, tr, None)
    nq, no, nu, nd = wq.shape[0] // units, wo.shape[1] // WIDE, wu.shape[1] // WIDE, wd.shape[1] // SLIM
    per = seq // PIECE
    pieces = mine * per

    def vec(name, cc, size, start=0):
        return pk2[cc, :, pl.ds(offs[name] + start, size)]

    def small():
        return remote(pk, pk2.at[g.c], ps, pr, g.Y)

    def span(p):
        return p // per, pl.ds(p % per * PIECE, PIECE)

    def hidden(p):
        s, rows = span(p)
        return remote(hid.at[g.oc * mine + s, rows], xland.at[s, rows], hs.at[p], hr.at[p], g.Y)

    hidden(0).start()

    @functools.partial(chunked, nq)
    def _(j):
        qgat.start(0, j)

    ogat.start(0, 0)
    for ref, start in zip((g1, s1, g2, s2, bo, bd, bq, bu), offs.values()):
        if len(ref.shape) == 1:
            pk[0, pl.ds(start, ref.shape[0])] = ref[...].astype(F32)
            continue
        for i in range(ref.shape[0]):
            for j in range(ref.shape[1]):
                pk[0, pl.ds(start + (i * ref.shape[1] + j) * LANES, LANES)] = ref[i, j, :].astype(F32)
    small().start()
    for p in range(1, pieces):
        hidden(p).start()
    for kind in (2, 1):
        @functools.partial(chunked, nq)
        def _(j):
            qgat.start(kind, j)
    for j in range(no):
        ogat.start(1, j)
    for j in range(EARLY):
        ugat.start(1, j)

    def qkv_phase(xbuf, wbuf, obuf, ab):
        pk2[g.c] = pk[...]
        small().wait_recv()
        gains = [vec('g1', cc, half) for cc in (g.c, g.oc)]
        shifts = [vec('s1', cc, half) for cc in (g.c, g.oc)]
        for p in range(pieces):
            s, rows = span(p)
            loads = [pltpu.make_async_copy(src, xbuf.at[i], ls.at[i]) for i, src in enumerate((hid.at[g.c * mine + s, rows], xland.at[s, rows]))]
            loads[0].start()
            hidden(p).wait_recv()
            loads[1].start()
            for load in loads:
                load.wait()
            sub = 64

            @functools.partial(chunked, PIECE // sub)
            def _(i):
                rows = aligned(i * sub, sub)
                res = norm_rows([xbuf[0, rows, :], xbuf[1, rows, :]], gains, shifts)
                for cc, val in zip((g.c, g.oc), res):
                    ab[aligned(p * PIECE + i * sub, sub), aligned(cc * half, half)] = val

        def load_own(j, act_on):
            for i in range(units):
                for idx, rr in enumerate((g.r, g.rp, g.rx, g.rxp)):
                    src = qland.at[g.c, rr, j * units + i] if idx else wq.at[j * units + i]
                    act_on(pltpu.make_async_copy(src, wbuf.at[0, rr, :, pl.ds(i * LANES, LANES)], ws.at[0, i, idx]))

        def load_other(j, act_on):
            for i in range(units):
                act_on(pltpu.make_async_copy(qland.at[g.oc, :, j * units + i], wbuf.at[1, :, :, pl.ds(i * LANES, LANES)], ws.at[1, i, 0]))

        def save(slot, cc, j):
            return pltpu.make_async_copy(obuf.at[slot], qkv.at[:, aligned((cc * nq + j) * WIDE, WIDE)], st.at[slot])

        def compute(slot, cc, j):
            @pl.when(j > 0)
            def _():
                save(slot, cc, j - 1).wait()

            bias = vec('bq', cc, WIDE, pl.multiple_of(j * WIDE, WIDE))

            def emit(rows, val):
                obuf[slot, rows, :] = (val + bias).astype(BF)

            matmul_rows(ab, wbuf.at[slot], 1024, emit)
            save(slot, cc, j).start()

        @functools.partial(chunked, nq + 3)
        def _(t):
            @pl.when(t < nq)
            def _():
                qgat.relay(t)

            @pl.when(t == nq - 1)
            def _():
                for j in range(1, no):
                    ogat.start(0, j)
                for j in range(2):
                    ugat.start(0, j)

            @pl.when((t >= 1) & (t <= nq))
            def _():
                qgat.push(t - 1)

            @pl.when(t < nq)
            def _():
                qgat.arrive(2, t)
                qgat.arrive(3, t)
                load_own(t, BEGIN)

            @pl.when(t >= 3)
            def _():
                load_other(t - 3, FINISH)
                compute(1, g.oc, t - 3)

            @pl.when((t >= 2) & (t < nq + 2))
            def _():
                qgat.arrive(4, t - 2)
                qgat.arrive(5, t - 2)
                load_other(t - 2, BEGIN)

            @pl.when(t < nq)
            def _():
                load_own(t, FINISH)
                compute(0, g.c, t)

        for slot, cc in enumerate((g.c, g.oc)):
            save(slot, cc, nq - 1).wait()

    pl.run_scoped(
        qkv_phase,
        pltpu.VMEM((2, PIECE, half), BF),
        pltpu.VMEM((2, 4, wq.shape[1], WIDE), BF),
        pltpu.VMEM((2, tokens, WIDE), BF),
        pltpu.VMEM((tokens, 2 * half), BF),
    )

    heads = wq.shape[0] // 3

    def attend(ob, abuf, wob, xb):
        def first():
            for j in range(no):
                ogat.start(2, j)
                ogat.relay(j)
            for j in range(nu):
                ugat.start(2, j)
            for j in range(2, nu):
                ugat.start(0, j)
            for j in range(EARLY, nu):
                ugat.start(1, j)

        events = {0: first, 34: lambda: ogat.push(0), 46: lambda: ogat.push(1)}
        for j, at in enumerate((10, 18)):
            events[at] = functools.partial(ugat.relay, j)
        steps = mine * 2 * heads

        def block(step, act_on):
            s, h = step // (2 * heads), step % (2 * heads)
            base = (h // heads) * 3 * heads + h % heads
            for i in range(3):
                src = qkv.at[aligned(s * seq, seq), aligned((base + i * heads) * LANES, LANES)]
                act_on(pltpu.make_async_copy(src, abuf.at[step % 2, i], al.at[step % 2, i]))

        block(0, BEGIN)

        @functools.partial(chunked, steps)
        def _(step):
            for at, act in events.items():
                pl.when(step == at)(act)

            @pl.when(step + 1 < steps)
            def _():
                block(step + 1, BEGIN)

            block(step, FINISH)
            s, h = step // (2 * heads), step % (2 * heads)
            attn_head(256, *(abuf.at[step % 2, i] for i in range(3)), ob.at[aligned(s * seq, seq), aligned(h * LANES, LANES)])

        for j in range(no):
            for kind in range(2, 6):
                ogat.arrive(kind, j)
        parts = half // WIDE

        def fetch(i, act_on):
            slot, rel, j = i % 2, i // parts, i % parts
            at = pl.ds(j * WIDE, WIDE)
            copies = shard_loads(g, ogat.own, lambda cc, j: oland.at[cc, :, :, at], ogat.land, wob.at[slot], ws.at[slot, 0], rel, j)
            for s in range(mine):
                src = xland.at[s, :, at] if rel else hid.at[g.c * mine + s, :, at]
                copies.append(pltpu.make_async_copy(src, xb.at[slot, pl.ds(s * seq, seq)], ws.at[slot, 1, s]))
            for copy in copies:
                act_on(copy)

        fetch(0, BEGIN)
        for i in range(2 * parts):
            slot = i % 2
            if i + 1 < 2 * parts:
                fetch(i + 1, BEGIN)
            fetch(i, FINISH)
            cc = g.oc if i >= parts else g.c
            bias = vec('bo', cc, WIDE, i % parts * WIDE)
            at = aligned(cc * half + i % parts * WIDE, WIDE)

            def emit(rows, val):
                hb[rows, at] = (xb[slot, rows, :].astype(F32) + val + bias).astype(BF)

            matmul_rows(ob, wob.at[slot], 512, emit)
            ugat.relay(2 + i)

    pl.run_scoped(
        attend,
        pltpu.VMEM((tokens, 2 * heads * LANES), BF),
        pltpu.VMEM((2, 3, seq, LANES), BF),
        pltpu.VMEM((2, 4, wo.shape[0], WIDE), BF),
        pltpu.VMEM((2, tokens, WIDE), BF),
    )

    small().wait_send()
    for p in range(pieces):
        hidden(p).wait_send()
    qgat.drain(range(7), 0, nq)
    ogat.drain(range(7), 0, no)

    def mlp(act):
        def load(gat, land, width, wbuf, rel, j, act_on):
            whole = lambda cc, j: land.at[cc, :, :, aligned(j * width, width)]
            for copy in shard_loads(g, gat.own, whole, gat.land, wbuf.at[rel], ws.at[rel, 0], rel, j):
                act_on(copy)

        def up(wbuf, ab):
            gains = [vec('g2', cc, half) for cc in range(2)]
            shifts = [vec('s2', cc, half) for cc in range(2)]

            @functools.partial(chunked, tokens // 64)
            def _(i):
                rows = aligned(i * 64, 64)
                ab[rows, :half], ab[rows, half:] = norm_rows([hb[rows, :half], hb[rows, half:]], gains, shifts)

            fetch = functools.partial(load, ugat, uland, WIDE, wbuf)

            def compute(rel, j):
                cc = g.oc if rel else g.c
                bias = vec('bu', cc, WIDE, pl.multiple_of(j * WIDE, WIDE))
                at = aligned((cc * nu + j) * WIDE, WIDE)

                def emit(rows, val):
                    act[rows, at] = jax.nn.gelu(val + bias, approximate=True).astype(BF)

                fetch(rel, j, FINISH)
                matmul_rows(ab, wbuf.at[rel], 1024, emit)

            def ready(rel, j):
                for kind in ((4, 5) if rel else (2, 3)):
                    ugat.arrive(kind, j)
                fetch(rel, j, BEGIN)

            ugat.relay(nu - 2)
            ready(0, 0)

            @functools.partial(chunked, nu + 1)
            def _(t):
                @pl.when(t < nu)
                def _():
                    compute(0, t)

                @pl.when(t == 0)
                def _():
                    ugat.push(0)
                    ugat.relay(nu - 1)
                    for j in range(nd):
                        dgat.start(1, j)
                        dgat.start(2, j)
                    for j in range(DOWN_X):
                        dgat.start(0, j)

                @pl.when(t + 1 < nu)
                def _():
                    ready(0, t + 1)

                @pl.when((t >= 1) & (t < nu))
                def _():
                    ugat.push(t)

                @pl.when(t == 1)
                def _():
                    ready(1, 0)

                @pl.when((t == 6) | (t == 8))
                def _():
                    dgat.relay((t - 6) // 2)

                @pl.when(t >= 1)
                def _():
                    compute(1, t - 1)

                @pl.when((t >= 1) & (t < nu))
                def _():
                    ready(1, t)

        pl.run_scoped(up, pltpu.VMEM((2, 4, wu.shape[0], WIDE), BF), pltpu.VMEM((tokens, 2 * half), BF))

        def down(wbuf, acc):
            depth = wd.shape[0]
            fetch = functools.partial(load, dgat, dland, SLIM, wbuf, 1)

            def spot(rel, j):
                return aligned((g.oc if rel else g.c) * half + j * SLIM, SLIM)

            def place(rel, s, j):
                src = hb.at[pl.ds(s * seq, seq), spot(rel, j)]
                dst = out.at[g.c * mine + s, :, aligned(j * SLIM, SLIM)]
                return remote(src, dst, gs.at[s, j], gr.at[s, j], g.Y) if rel else pltpu.make_async_copy(src, dst, ks.at[s, j])

            def finish(rel, j):
                cc = g.oc if rel else g.c
                bias = vec('bd', cc, SLIM, pl.multiple_of(j * SLIM, SLIM))

                def emit(rows, val):
                    hb[rows, spot(rel, j)] = (hb[rows, spot(rel, j)].astype(F32) + val + bias).astype(BF)

                return emit

            def send(rel, j):
                for s in range(mine):
                    place(rel, s, j).start()

            def other(j):
                fetch(j, FINISH)
                matmul_rows(act, wbuf.at[1], 1024, finish(1, j))
                send(1, j)

            def shard(rr, j, act_on):
                src = dland.at[g.c, rr, :, aligned(j * SLIM, SLIM)]
                act_on(pltpu.make_async_copy(src, wbuf.at[0, rr], ws.at[0, 1, rr]))

            def mine_shard(j, act_on):
                act_on(pltpu.make_async_copy(dgat.own(j), wbuf.at[0, g.r], ws.at[0, 1, g.r]))
                shard(g.rp, j, act_on)

            def product(rr, count, emit):
                matmul_rows(act.at[:, aligned(rr * depth, count * depth)], wbuf.at[0, pl.ds(rr, count)], 1024, emit)

            def near(j):
                mine_shard(j, FINISH)

                def emit(rows, val):
                    acc[rows, :] = val

                product(g.r // 2 * 2, 2, emit)

                @pl.when(j + 1 < nd)
                def _():
                    dgat.arrive(2, j + 1)
                    mine_shard(j + 1, BEGIN)

            def add(rows, val):
                acc[rows, :] += val

            def far(j):
                shard(g.rx, j, BEGIN)
                dgat.arrive(3, j)
                shard(g.rxp, j, BEGIN)
                shard(g.rx, j, FINISH)
                product(g.rx, 1, add)
                shard(g.rxp, j, FINISH)
                last = finish(0, j)
                product(g.rxp, 1, lambda rows, val: last(rows, acc[rows, :] + val))
                send(0, j)

            def far_late(j):
                last = finish(0, j)
                for i in range(2):
                    piece = 2 * (j - DOWN_X) + i
                    rows_in = pl.ds(i * deep, deep)

                    def block(rr, act_on):
                        act_on(pltpu.make_async_copy(tgat.land(g.c, rr, piece), wbuf.at[0, rr, rows_in], ws.at[0, 1, rr]))

                    def block_product(rr, emit):
                        matmul_rows(act.at[:, aligned(rr * depth + i * deep, deep)], wbuf.at[0, pl.ds(rr, 1), rows_in], 1024, emit)

                    tgat.arrive(0, piece)
                    tgat.start(3, piece)
                    block(g.rx, BEGIN)
                    block(g.rx, FINISH)
                    block_product(g.rx, add)
                    tgat.arrive(3, piece)
                    block(g.rxp, BEGIN)
                    block(g.rxp, FINISH)
                    if i == 0:
                        block_product(g.rxp, add)
                        continue
                    for s in range(mine):
                        here = pl.ds(s * seq, seq)

                        def close(rows, val):
                            last(here, acc[here, :] + val)

                        matmul_rows(act.at[here, aligned(g.rxp * depth + i * deep, deep)], wbuf.at[0, pl.ds(g.rxp, 1), rows_in], seq, close)
                        place(0, s, j).start()

            def pass_on(j):
                dgat.arrive(1, j)
                dgat.start(4, j)
                dgat.start(6, j)

            dgat.arrive(2, 0)
            mine_shard(0, BEGIN)

            @functools.partial(chunked, nd + 1)
            def _(t):
                @pl.when(t < nd)
                def _():
                    dgat.push(t)

                @pl.when(t < DOWN_X)
                def _():
                    pass_on(t + DOWN_X)

                @pl.when(t == 1)
                def _():
                    for j in range(2 * (nd - DOWN_X)):
                        tgat.start(0, j)

                @pl.when(t < nd)
                def _():
                    for kind in (4, 5):
                        dgat.arrive(kind, t)
                    fetch(t, BEGIN)
                    other(t)

                @pl.when(t <= DOWN_X)
                def _():
                    near(t)

                @pl.when(t == DOWN_X)
                def _():
                    ugat.drain(range(7), 0, nu)

                @pl.when(t < DOWN_X)
                def _():
                    far(t)

                @pl.when(t > DOWN_X)
                def _():
                    far_late(t - 1)

                @pl.when(t == nd - 1)
                def _():
                    near(nd - 1)

            for s in range(mine):
                for j in range(nd):
                    place(0, s, j).wait()
                    place(1, s, j).wait_send()
                    got = out.at[g.oc * mine + s, :, aligned(j * SLIM, SLIM)]
                    remote(got, got, gs.at[s, j], gr.at[s, j], g.Y).wait_recv()

        pl.run_scoped(down, pltpu.VMEM((2, 4, wd.shape[0], SLIM), BF), pltpu.VMEM((tokens, SLIM), F32))

    pl.run_scoped(mlp, pltpu.VMEM((tokens, 2 * wu.shape[1]), BF))
    dgat.drain(range(7), 0, DOWN_X)
    dgat.drain((1, 2, 4, 5, 6), DOWN_X, nd)
    tgat.drain((0, 3), 0, 2 * (nd - DOWN_X))


def layer_call(small, hidden, wq, wo, wu, wd, offs):
    seqs, seq, half = hidden.shape
    mine = seqs // 2
    tokens = mine * seq
    nq, no, nu, nd = wq.shape[0] * LANES // WIDE, wo.shape[1] // WIDE, wu.shape[1] // WIDE, wd.shape[1] // SLIM
    total = sum(a.size for a in small)
    dma = pltpu.SemaphoreType.DMA
    shape = lambda *dims: jax.ShapeDtypeStruct(dims, BF)
    sems = [dma((7, n)) for n in (nq, no, nu, nd) for _ in 'sr']
    sems += [dma((tokens // PIECE,))] * 2 + [dma((4, 4))] * 2 + [dma((2, 2)), dma, dma, dma((2,)), dma((2, 4, 4)), dma((2,)), dma((2, 3))] + [dma((mine, nd))] * 3
    return pl.pallas_call(
        functools.partial(layer_kernel, offs),
        in_specs=[pl.BlockSpec(memory_space=pltpu.VMEM)] * len(small) + [ANY] * 5,
        out_specs=[ANY] * 7,
        out_shape=[shape(*hidden.shape), shape(mine, seq, half), shape(tokens, 2 * wq.shape[0] * LANES)] + [shape(2, 4, *w.shape) for w in (wq, wo, wu, wd)],
        scratch_shapes=[pltpu.VMEM((tokens, 2 * half), BF), pltpu.VMEM((1, total), F32), pltpu.VMEM((2, 1, total), F32)] + sems,
        compiler_params=pltpu.CompilerParams(collective_id=1, has_side_effects=True, vmem_limit_bytes=VMEM_LIMIT),
        name='layer',
    )(*small, hidden, wq, wo, wu, wd)[0]


def tidy_kernel(src, dst, buf, ins, outs):
    count = src.shape[0] * 2
    rows = src.shape[1] // 2
    at = lambda ref, i: ref.at[i // 2, pl.ds(i % 2 * rows, rows)]
    loads = [pltpu.make_async_copy(at(src, i), buf.at[i], ins.at[i]) for i in range(count)]
    stores = [pltpu.make_async_copy(buf.at[i], at(dst, i), outs.at[i]) for i in range(count)]
    for load in loads:
        load.start()
    for load, store in zip(loads, stores):
        load.wait()
        store.start()
    for store in stores:
        store.wait()


def tidy(out):
    count = out.shape[0] * 2
    dma = pltpu.SemaphoreType.DMA
    return pl.pallas_call(
        tidy_kernel,
        in_specs=[ANY],
        out_specs=ANY,
        out_shape=jax.ShapeDtypeStruct(out.shape, BF),
        scratch_shapes=[pltpu.VMEM((count, out.shape[1] // 2, out.shape[2]), BF), dma((count,)), dma((count,))],
        compiler_params=pltpu.CompilerParams(vmem_limit_bytes=VMEM_LIMIT),
        name='tidy',
    )(out)


def solution(mesh):
    act_spec = P(('dp', 'row'), None, 'col')
    arg_specs = (act_spec, P('col'), P('col'), P('row', None, 'col', None), P(None, 'col', None), P('row', None, 'col'), P('col'), P('col'), P('col'), P('row', 'col'), P('col'), P('row', 'col'), P('col'))

    def local_layer(hidden, ln1_gain, ln1_bias, w_qkv, b_qkv, w_out, b_out, ln2_gain, ln2_bias, w_up, b_up, w_down, b_down):
        seqs, _, half = hidden.shape
        heads, size = w_qkv.shape[2], w_qkv.shape[3]
        small = {'g1': ln1_gain, 's1': ln1_bias, 'g2': ln2_gain, 's2': ln2_bias, 'bo': b_out, 'bd': b_down, 'bq': b_qkv, 'bu': b_up}
        offs, at = {}, 0
        for name, a in small.items():
            offs[name], at = at, at + a.size
        wq = jnp.transpose(w_qkv, (1, 2, 0, 3)).reshape(3 * heads, w_qkv.shape[0], size)
        wo = w_out.reshape(-1, half)
        return tidy(layer_call(list(small.values()), hidden, wq, wo, w_up, w_down, offs))

    return jax.shard_map(local_layer, mesh=mesh, in_specs=arg_specs, out_specs=act_spec, check_vma=False)
```
